256 devices in a mesh: row: 32 (over z_lo, y, core), col: 8 (over x, z_hi).
Axes of the slice: x: 4, y: 4, z: 8 (z_hi: 2, z_lo: 4; z = z_hi * 4 + z_lo), core: 2. Of those that a mesh axis runs over, the one named last changes fastest.
Arguments:
- pair_rep: bfloat16 [2048, 2048, 128], P('row', 'col'), may hold values from -6 to 6
- bias_weight: bfloat16 [128, 12], replicated, may hold values from -0.5 to 0.5
- head_weight: float32 [12], replicated, may hold values from -1 to 1
- queries: float32 [192, 2048], P(None, 'row'), may hold values from -48 to 48, as said below
- key_vectors: float32 [192, 2048], P(None, 'col'), may hold values from -48 to 48, as said below
- values: float32 [192, 2048], P(None, 'col'), may hold values from -6 to 6
- query_points: float32 [3, 48, 2048], P(None, None, 'row'), may hold values from -6 to 6
- key_points: float32 [3, 48, 2048], P(None, None, 'col'), may hold values from -6 to 6
- value_points: float32 [3, 96, 2048], P(None, None, 'col'), may hold values from -6 to 6
- rotations: float32 [3, 3, 2048], replicated, may hold values from -1 to 1, as said below
- translations: float32 [3, 2048], replicated, may hold values from -12 to 12
- residue_count: int32 [1], replicated, may hold values from 1024 to 2048
- grad_output: float32 [192, 2048], P(None, 'row'), may hold values from -6 to 6
- grad_points: float32 [3, 96, 2048], P(None, None, 'row'), may hold values from -6 to 6
- grad_pair: bfloat16 [2048, 12, 128], P('row'), may hold values from -2 to 2
Outputs:
- pair_grad: bfloat16 [2048, 2048, 128], P('row', 'col')
- query_grad: float32 [192, 2048], P(None, ('row', 'col'))
- query_point_grad: float32 [3, 48, 2048], P(None, None, ('row', 'col'))
- query_frame_grad: float32 [3, 4, 2048], P(None, None, ('row', 'col'))
- key_grad: float32 [192, 2048], P(None, ('col', 'row'))
- value_grad: float32 [192, 2048], P(None, ('col', 'row'))
- key_point_grad: float32 [3, 48, 2048], P(None, None, ('col', 'row'))
- value_point_grad: float32 [3, 96, 2048], P(None, None, ('col', 'row'))
- key_frame_grad: float32 [3, 4, 2048], P(None, None, ('col', 'row'))
- bias_weight_grad: float32 [128, 12], replicated
- head_weight_grad: float32 [12], replicated
The draws below stay inside these ranges and needn't reach their ends.
Inputs may be any that keep to these rules, and one draw needn't show every extreme that they name: `queries`: entries of order one, except a few residues whose vectors are much larger. `key_vectors`: entries of order one, except a few residues whose vectors are much larger. `rotations`: each residue's 3 x 3 matrix is a rotation: orthonormal with determinant one.
All inputs are finite; a program needn't handle non-finite values.
Results may differ from the reference program's by a relative error of at most 0.0049.
Values sent between devices are 32-bit elements; how exact they have to be, the bound alone decides.
No kernel may reach another device: no remote copies, remote signals or barrier semaphores. Data moves between devices by JAX's collectives and lax.ppermute only.
A program may use at most 128 MiB of HBM per device.

```python
import math
import jax
import jax.numpy as jnp
from jax import lax

N = 2048
H = 12
C = 16
PQ = 4
PV = 8
CZ = 128


def drawn_vectors(key):
    base_key = jax.random.fold_in(key, 11)
    first, second = jax.random.split(base_key, 2)
    query_draw = jnp.clip(jax.random.normal(first, (H * C, N), jnp.float32), -4.0, 4.0)
    key_draw = jnp.clip(jax.random.normal(second, (H * C, N), jnp.float32), -4.0, 4.0)
    return (query_draw, key_draw)


def draw_queries(key, part):
    return drawn_vectors(key)[0]


def draw_key_vectors(key, part):
    return drawn_vectors(key)[1]


def draw_rotations(key, part):
    base_key = jax.random.fold_in(key, 23)
    first, second = jax.random.split(base_key)
    scalar = jax.random.uniform(first, (N,), jnp.float32, 0.5, 1.5)
    vector = jax.random.normal(second, (3, N), jnp.float32)
    length = jnp.sqrt(scalar ** 2 + jnp.sum(vector ** 2, axis=0))
    qw = scalar / length
    qx = vector[0] / length
    qy = vector[1] / length
    qz = vector[2] / length
    first_row = jnp.stack([1 - 2 * (qy * qy + qz * qz), 2 * (qx * qy - qw * qz), 2 * (qx * qz + qw * qy)])
    second_row = jnp.stack([2 * (qx * qy + qw * qz), 1 - 2 * (qx * qx + qz * qz), 2 * (qy * qz - qw * qx)])
    third_row = jnp.stack([2 * (qx * qz - qw * qy), 2 * (qy * qz + qw * qx), 1 - 2 * (qx * qx + qy * qy)])
    return jnp.stack([first_row, second_row, third_row])


def levels(stream_key, dims, shards, least, high):
    factor_of, own = 1.0, jax.random.fold_in(stream_key, 6)
    for position, parts in shards:
        heights = jnp.exp(jax.random.uniform(jax.random.fold_in(own, position), (parts,), jnp.float32, least / len(shards), high / len(shards)))
        factor_of = factor_of * jnp.repeat(heights, dims[position] // parts).reshape([-1 if axis == position else 1 for axis in range(len(dims))])
    return factor_of


def gaussian(own_key, shape, deviation, most, pieces=(), kind=jnp.bfloat16):
    loudness = levels(own_key, shape, pieces, -0.22, 0.18) if pieces else 1.0
    drawn = jax.random.normal(own_key, shape, jnp.float32) * deviation * loudness
    return jnp.minimum(jnp.maximum(drawn, -most), most).astype(kind)


def setup_inputs(seed: int = 0) -> dict:
    key_list = jax.random.split(jax.random.key(seed), 16)
    return {
        "pair_rep": gaussian(key_list[0], (N, N, CZ), 1.0, 6.0, ((0, 32), (1, 8))),
        "bias_weight": gaussian(key_list[1], (CZ, H), CZ ** -0.5, 0.5),
        "head_weight": jnp.clip(jax.random.uniform(key_list[2], (H,), jnp.float32, -1.0, 1.0), -1.0, 1.0),
        "queries": draw_queries(jax.random.fold_in(key_list[15], 71), 0),
        "key_vectors": draw_key_vectors(jax.random.fold_in(key_list[15], 71), 0),
        "values": gaussian(key_list[5], (H * C, N), 1.0, 6.0, ((1, 8),), jnp.float32),
        "query_points": gaussian(key_list[6], (3, H * PQ, N), 1.0, 6.0, ((2, 32),), jnp.float32),
        "key_points": gaussian(key_list[7], (3, H * PQ, N), 1.0, 6.0, ((2, 8),), jnp.float32),
        "value_points": gaussian(key_list[8], (3, H * PV, N), 1.0, 6.0, ((2, 8),), jnp.float32),
        "rotations": draw_rotations(jax.random.fold_in(key_list[15], 71), 0),
        "translations": gaussian(key_list[10], (3, N), 2.0, 12.0, (), jnp.float32),
        "residue_count": jax.random.randint(key_list[11], (1,), N // 2, N + 1).astype(jnp.int32),
        "grad_output": gaussian(key_list[12], (H * C, N), 1.0, 6.0, ((1, 32),), jnp.float32),
        "grad_points": gaussian(key_list[13], (3, H * PV, N), 1.0, 6.0, ((2, 32),), jnp.float32),
        "grad_pair": gaussian(key_list[14], (N, H, CZ), 0.3, 2.0, ((0, 32),)),
    }


HIGHEST = lax.Precision.HIGHEST

def globalize(rotation, offset, local):
    return jnp.einsum('xym,ykm->xkm', rotation, local, precision=HIGHEST) + offset[:, None, :]

def rotate_back(rotation, vector):
    return jnp.einsum('xym,xkm->ykm', rotation, vector, precision=HIGHEST)

def frame_terms(grad_global, local):
    rotation_part = jnp.einsum('xkm,ykm->xym', grad_global, local, precision=HIGHEST)
    return jnp.concatenate([rotation_part, lax.optimization_barrier(jnp.sum(grad_global, axis=1))[:, None, :]], axis=1)

def output_frame_terms(point_out, offset, cotan_local, grad_rotated):
    rotation_part = jnp.einsum('xkm,ykm->xym', point_out - offset[:, None, :], cotan_local, precision=HIGHEST)
    return jnp.concatenate([rotation_part, -lax.optimization_barrier(jnp.sum(grad_rotated, axis=1))[:, None, :]], axis=1)

def reference(pair_rep, bias_weight, head_weight, queries, key_vectors, values, query_points, key_points, value_points, rotations, translations, residue_count, grad_output, grad_points, grad_pair):
    logit_scale = math.sqrt(1.0 / 3.0)
    point_scale = math.sqrt(2.0 / (9.0 * PQ))
    inner_scale = 1.0 / math.sqrt(C)
    distance_coef = 0.5 * logit_scale * point_scale * jax.nn.softplus(head_weight)
    query_global = globalize(rotations, translations, query_points).reshape(3, H, PQ, N)
    key_global = globalize(rotations, translations, key_points).reshape(3, H, PQ, N)
    value_global = globalize(rotations, translations, value_points).reshape(3, H, PV, N)
    grad_global = jnp.einsum('xym,ykm->xkm', rotations, grad_points, precision=HIGHEST)
    grad_heads = grad_global.reshape(3, H, PV, N)
    key_heads = key_vectors.reshape(H, C, N)
    value_heads = values.reshape(H, C, N)
    query_heads = queries.reshape(H, C, N)
    out_heads = grad_output.reshape(H, C, N)
    valid = jnp.arange(N) < residue_count[0]
    pair_weight = bias_weight.astype(jnp.float32)
    block = min(128, N)

    def step(carry, start):
        pair_block = lax.dynamic_slice_in_dim(pair_rep, start, block, 0).astype(jnp.float32)
        cotan_pair = lax.dynamic_slice_in_dim(grad_pair, start, block, 0).astype(jnp.float32)
        query_block = lax.dynamic_slice_in_dim(query_heads, start, block, 2)
        out_block = lax.dynamic_slice_in_dim(out_heads, start, block, 2)
        qglobal_block = lax.dynamic_slice_in_dim(query_global, start, block, 3)
        gglobal_block = lax.dynamic_slice_in_dim(grad_heads, start, block, 3)
        inner = jnp.einsum('hci,hcj->hij', query_block, key_heads, precision=HIGHEST)
        cross = jnp.einsum('xhpi,xhpj->hij', qglobal_block, key_global, precision=HIGHEST)
        distance = lax.optimization_barrier(jnp.sum(qglobal_block ** 2, axis=(0, 2)))[:, :, None] + lax.optimization_barrier(jnp.sum(key_global ** 2, axis=(0, 2)))[:, None, :] - 2.0 * cross
        bias = jnp.einsum('ijc,ch->hij', pair_block, pair_weight, precision=HIGHEST)
        logits = logit_scale * (inner_scale * inner + bias) - distance_coef[:, None, None] * distance
        logits = jnp.where(valid[None, None, :], logits, jnp.float32(-1000000000.0))
        row_peak = lax.optimization_barrier(jnp.max(logits, axis=2, keepdims=True))
        exponent = jnp.exp(logits - row_peak)
        attention = exponent / lax.optimization_barrier(jnp.sum(exponent, axis=2, keepdims=True))
        product = jnp.einsum('hci,hcj->hij', out_block, value_heads, precision=HIGHEST) + jnp.einsum('xhvi,xhvj->hij', gglobal_block, value_global, precision=HIGHEST) + jnp.einsum('ijc,ihc->hij', pair_block, cotan_pair, precision=HIGHEST)
        delta = lax.optimization_barrier(jnp.sum(attention * product, axis=2, keepdims=True))
        logit_grad = attention * (product - delta)
        query_grad = logit_scale * inner_scale * jnp.einsum('hij,hcj->hci', logit_grad, key_heads, precision=HIGHEST)
        row_sum = lax.optimization_barrier(jnp.sum(logit_grad, axis=2))
        qpoint_grad = -2.0 * distance_coef[None, :, None, None] * (qglobal_block * row_sum[None, :, None, :] - jnp.einsum('hij,xhpj->xhpi', logit_grad, key_global, precision=HIGHEST))
        qpoint_flat = qpoint_grad.reshape(3, H * PQ, block)
        point_out = jnp.einsum('hij,xhvj->xhvi', attention, value_global, precision=HIGHEST).reshape(3, H * PV, block)
        rot_block = lax.dynamic_slice_in_dim(rotations, start, block, 2)
        shift_block = lax.dynamic_slice_in_dim(translations, start, block, 1)
        local_block = lax.dynamic_slice_in_dim(query_points, start, block, 2)
        cotan_local = lax.dynamic_slice_in_dim(grad_points, start, block, 2)
        gflat_block = gglobal_block.reshape(3, H * PV, block)
        qlocal_grad = rotate_back(rot_block, qpoint_flat)
        qframe = frame_terms(qpoint_flat, local_block) + output_frame_terms(point_out, shift_block, cotan_local, gflat_block)
        key_part = logit_scale * inner_scale * jnp.einsum('hij,hci->hcj', logit_grad, query_block, precision=HIGHEST)
        value_part = jnp.einsum('hij,hci->hcj', attention, out_block, precision=HIGHEST)
        col_sum = lax.optimization_barrier(jnp.sum(logit_grad, axis=1))
        kpoint_part = 2.0 * distance_coef[None, :, None, None] * (jnp.einsum('hij,xhpi->xhpj', logit_grad, qglobal_block, precision=HIGHEST) - key_global * col_sum[None, :, None, :])
        vpoint_part = jnp.einsum('hij,xhvi->xhvj', attention, gglobal_block, precision=HIGHEST)
        grad_rounded = lax.optimization_barrier(logit_grad.astype(jnp.bfloat16)).astype(jnp.float32)
        attn_rounded = lax.optimization_barrier(attention.astype(jnp.bfloat16)).astype(jnp.float32)
        weight_part = logit_scale * jnp.einsum('ijc,hij->ch', pair_block, grad_rounded, precision=HIGHEST)
        distance_part = lax.optimization_barrier(jnp.sum(logit_grad * distance, axis=(1, 2)))
        pair_grad = (logit_scale * jnp.einsum('hij,ch->ijc', grad_rounded, pair_weight, precision=HIGHEST) + jnp.einsum('hij,ihc->ijc', attn_rounded, cotan_pair, precision=HIGHEST)).astype(jnp.bfloat16)
        new_carry = (carry[0] + key_part, carry[1] + value_part, carry[2] + kpoint_part, carry[3] + vpoint_part, carry[4] + weight_part, carry[5] + distance_part)
        return (new_carry, (pair_grad, query_grad.reshape(H * C, block), qlocal_grad, qframe))
    initial = (jnp.zeros((H, C, N), jnp.float32), jnp.zeros((H, C, N), jnp.float32), jnp.zeros((3, H, PQ, N), jnp.float32), jnp.zeros((3, H, PV, N), jnp.float32), jnp.zeros((CZ, H), jnp.float32), jnp.zeros((H,), jnp.float32))
    starts = jnp.arange(N // block, dtype=jnp.int32) * block
    carry, stacked = lax.scan(step, initial, starts)
    pair_grad = stacked[0].reshape(N, N, CZ)
    query_grad = jnp.transpose(stacked[1], (1, 0, 2)).reshape(H * C, N)
    query_point_grad = jnp.transpose(stacked[2], (1, 2, 0, 3)).reshape(3, H * PQ, N)
    query_frame_grad = jnp.transpose(stacked[3], (1, 2, 0, 3)).reshape(3, 4, N)
    kpoint_flat = carry[2].reshape(3, H * PQ, N)
    vpoint_flat = carry[3].reshape(3, H * PV, N)
    key_point_grad = rotate_back(rotations, kpoint_flat)
    value_point_grad = rotate_back(rotations, vpoint_flat)
    key_frame_grad = frame_terms(kpoint_flat, key_points) + frame_terms(vpoint_flat, value_points)
    head_weight_grad = carry[5] * (-0.5 * logit_scale * point_scale) * jax.nn.sigmoid(head_weight)
    return (pair_grad, query_grad, query_point_grad, query_frame_grad, carry[0].reshape(H * C, N), carry[1].reshape(H * C, N), key_point_grad, value_point_grad, key_frame_grad, carry[4], head_weight_grad)
```

```python
import functools
import math

import jax
import jax.numpy as jnp
from jax import lax
from jax.experimental import pallas as pl
from jax.experimental.pallas import tpu as pltpu
from jax.sharding import Mesh
from jax.sharding import PartitionSpec as P

ROW = ("row_0", "row_1", "row_2")
COL = ("col_0", "col_1")
ROW_COL = ROW + COL
COL_ROW = COL + ROW
CHIPS = ("row_0", "row_1")

H, C, PQ, PV, CZ = 12, 16, 4, 8, 128
IQ, JK = 64, 256
NCOL, NROW, NCHIP = 8, 32, 16
WL = math.sqrt(1.0 / 3.0)
WC = math.sqrt(2.0 / (9.0 * PQ))
WS = 1.0 / math.sqrt(C)
MASKED = -1000000000.0

KEY0, VAL0, KPT0, VPT0, KEND = 0, 192, 384, 528, 816
QRY0, QPT0, OPT0, QEND = 0, 192, 336, 624
KW, QW = 1024, 640
QB = 8

F32, BF16 = jnp.float32, jnp.bfloat16
VMEM_SPEC = pl.BlockSpec(memory_space=pltpu.VMEM)
SMEM_SPEC = pl.BlockSpec(memory_space=pltpu.SMEM)
TN = (((0,), (0,)), ((), ()))
NT = (((1,), (1,)), ((), ()))
NN = (((1,), (0,)), ((), ()))


def mm(a, b, dims):
    return lax.dot_general(a, b, dims, preferred_element_type=F32)


def split2(x):
    hi = x.astype(BF16)
    return hi, (x - hi.astype(F32)).astype(BF16)


def split3(x):
    hi = x.astype(BF16)
    rest = x - hi.astype(F32)
    mid = rest.astype(BF16)
    return hi, mid, (rest - mid.astype(F32)).astype(BF16)


def row_index():
    return (lax.axis_index("row_0") * 4 + lax.axis_index("row_1")) * 2 + lax.axis_index("row_2")


def col_index():
    return lax.axis_index("col_0") * 2 + lax.axis_index("col_1")


def soft(hw_ref, h, lanes):
    w = jnp.full((1, lanes), hw_ref[h], F32)
    return jnp.maximum(w, 0.0) + jnp.log1p(jnp.exp(-jnp.abs(w)))


def coef_row(hw_ref, h, lanes):
    return (0.5 * WL * WC) * soft(hw_ref, h, lanes)


def rotate(rot, shift, local):
    out = []
    for x in range(3):
        g = rot[x][0] * local[0] + rot[x][1] * local[1] + rot[x][2] * local[2]
        out.append(g if shift is None else g + shift[x])
    return out


def col_frames(rot_ref, tr_ref):
    start = pl.multiple_of(col_index() * JK, JK)
    rot = [[rot_ref[x, y : y + 1, pl.ds(start, JK)] for y in range(3)] for x in range(3)]
    tr = [tr_ref[x : x + 1, pl.ds(start, JK)] for x in range(3)]
    return rot, tr


def lanes_at(block, offset, count):
    return pltpu.roll(block, lax.rem(128 - offset, 128), block.ndim - 1)[..., :count]


def row_frames(rot_ref, tr_ref, offset, count):
    at = row_index() * IQ + offset
    base = pl.multiple_of(lax.div(at, 128) * 128, 128)
    off = lax.rem(at, 128)
    rot = []
    for x in range(3):
        block = lanes_at(
            jnp.concatenate([rot_ref[x, :, pl.ds(base, 128)], jnp.zeros((5, 128), F32)], 0),
            off,
            count,
        )
        rot.append([block[y : y + 1] for y in range(3)])
    block = lanes_at(
        jnp.concatenate([tr_ref[:, pl.ds(base, 128)], jnp.zeros((5, 128), F32)], 0), off, count
    )
    return rot, [block[x : x + 1] for x in range(3)]


def logits_kernel(
    hw_ref, rc_ref, pair_ref, gp_ref, bw_ref, q_ref, k_ref, v_ref, qp_ref, kp_ref, vp_ref,
    rot_ref, tr_ref, go_ref, gpt_ref,
    e_ref, p_ref, st_ref, qg_ref, kg_ref, vg_ref, gg_ref,
    bp_ref, wt_ref,
):
    step = pl.program_id(0)

    @pl.when(step == 0)
    def _():
        wide = jnp.concatenate([bw_ref[...].astype(F32), jnp.zeros((CZ, 128 - H), F32)], 1)
        wt_ref[...] = wide.T[:16].astype(BF16)

    wt = wt_ref[...]
    for n in range(QB):
        lhs = jnp.concatenate([wt, gp_ref[n]], 0)
        res = mm(lhs, pair_ref[n], NT)
        for half in range(2):
            bp_ref[half, pl.ds(step * QB + n, 16 + H, stride=IQ), :] = res[
                :, half * 128 : half * 128 + 128
            ]

    @pl.when(step == IQ // QB - 1)
    def _():
        crot, ctr = col_frames(rot_ref, tr_ref)
        rrot, rtr = row_frames(rot_ref, tr_ref, 0, IQ)
        kg = rotate(crot, ctr, [kp_ref[y] for y in range(3)])
        vg = rotate(crot, ctr, [vp_ref[y] for y in range(3)])
        qg = rotate(rrot, rtr, [qp_ref[y] for y in range(3)])
        gg = rotate(rrot, None, [gpt_ref[y] for y in range(3)])
        for x in range(3):
            kg_ref[x], vg_ref[x], qg_ref[x], gg_ref[x] = kg[x], vg[x], qg[x], gg[x]
        real = (
            lax.broadcasted_iota(jnp.int32, (IQ, JK), 1) + col_index() * JK < rc_ref[0]
        )
        lane = lax.broadcasted_iota(jnp.int32, (IQ, 128), 1)
        stats = [jnp.zeros((IQ, 128), F32), jnp.zeros((IQ, 128), F32)]
        row4q = lax.broadcasted_iota(jnp.int32, (4, IQ), 0)
        row4k = lax.broadcasted_iota(jnp.int32, (4, JK), 0)
        for h in range(H):
            cf = coef_row(hw_ref, h, IQ)
            qgh = [qg_ref[x, 4 * h : 4 * h + 4] for x in range(3)]
            kgh = [kg_ref[x, 4 * h : 4 * h + 4] for x in range(3)]
            qn = sum(jnp.sum(t * t, axis=0, keepdims=True) for t in qgh)
            kn = sum(jnp.sum(t * t, axis=0, keepdims=True) for t in kgh)
            qtail = jnp.where(row4q == 0, -cf, jnp.where(row4q == 1, -cf * qn, 0.0))
            ktail = jnp.where(row4k == 0, kn, jnp.where(row4k == 1, 1.0, 0.0))
            qf = jnp.concatenate(
                [q_ref[C * h : C * h + C] * (WL * WS)] + [2.0 * cf * t for t in qgh] + [qtail], 0
            )
            kf = jnp.concatenate([k_ref[C * h : C * h + C]] + kgh + [ktail], 0)
            a1, a2, a3 = split3(qf)
            b1, b2, b3 = split3(kf)
            core = mm(
                jnp.concatenate([a1, a1, a2, a1, a2, a3], 0),
                jnp.concatenate([b1, b2, b1, b3, b2, b1], 0),
                TN,
            )
            gf = jnp.concatenate(
                [go_ref[C * h : C * h + C]] + [gg_ref[x, 8 * h : 8 * h + 8] for x in range(3)]
                + [jnp.zeros((8, IQ), F32)], 0
            )
            vf = jnp.concatenate(
                [v_ref[C * h : C * h + C]] + [vg_ref[x, 8 * h : 8 * h + 8] for x in range(3)]
                + [jnp.zeros((8, JK), F32)], 0
            )
            g1, g2 = split2(gf)
            v1, v2 = split2(vf)
            prod = mm(
                jnp.concatenate([g1, g1, g2], 0), jnp.concatenate([v1, v2, v1], 0), TN
            )

            def planes(base):
                return jnp.concatenate(
                    [bp_ref[half, base * IQ : base * IQ + IQ, :] for half in range(2)], 1
                )

            logit = jnp.where(real, core + WL * planes(h), MASKED)
            prod = prod + planes(16 + h)
            peak = jnp.max(logit, axis=1, keepdims=True)
            e = jnp.exp(logit - peak)
            e_ref[h] = e
            p_ref[h] = prod
            total = jnp.sum(e, axis=1, keepdims=True)
            upper = jnp.sum(e * prod, axis=1, keepdims=True)
            g, r = divmod(h, 6)
            acc = jnp.where(lane == r, peak, stats[g])
            acc = jnp.where(lane == 8 + r, total, acc)
            stats[g] = jnp.where(lane == 16 + r, upper, acc)
        packed = jnp.concatenate(stats, 0).T[:24]
        for c in range(NCOL):
            st_ref[c] = packed


def grads_kernel(
    hw_ref, e_ref, p_ref, own_ref, all_ref, q_ref, k_ref, go_ref, qg_ref, kg_ref, vg_ref, gg_ref,
    pair_ref,
    d_ref, key_ref, qry_ref,
    da_ref, kp_ref, qp_ref, w_ref, hs_ref,
):
    step = pl.program_id(0)

    @pl.when(step == 0)
    def _():
        peaks = all_ref[:, 0:8]
        top = jnp.max(peaks, axis=0)
        grow = jnp.exp(peaks - top[None])
        total = jnp.sum(all_ref[:, 8:16] * grow, axis=0)
        upper = jnp.sum(all_ref[:, 16:24] * grow, axis=0)
        scale = jnp.exp(own_ref[0, 0:8] - top) / total
        delta = upper / total
        cols = jnp.concatenate([scale, delta, jnp.zeros((112, 128), F32)], 0).T
        w_ref[...] = jnp.zeros_like(w_ref)
        for half in range(2):
            da_ref[half, H * IQ : 16 * IQ, :] = jnp.zeros((4 * IQ, 128), F32)
            da_ref[half, 28 * IQ : 32 * IQ, :] = jnp.zeros((4 * IQ, 128), F32)
        row4q = lax.broadcasted_iota(jnp.int32, (4, IQ), 0)
        row4k = lax.broadcasted_iota(jnp.int32, (4, JK), 0)
        lane = lax.broadcasted_iota(jnp.int32, (8, 128), 1)
        hs = jnp.zeros((8, 128), F32)
        for h in range(H):
            g, r = divmod(h, 6)
            sc = cols[IQ * g : IQ * g + IQ, r : r + 1]
            dl = cols[IQ * g : IQ * g + IQ, 8 + r : 9 + r]
            a = e_ref[h] * sc
            d = a * (p_ref[h] - dl)
            for half in range(2):
                piece = slice(half * 128, half * 128 + 128)
                da_ref[half, h * IQ : h * IQ + IQ, :] = d[:, piece]
                da_ref[half, (16 + h) * IQ : (17 + h) * IQ, :] = a[:, piece]
            d1, d2 = split2(d)
            a1, a2 = split2(a)
            cfq = coef_row(hw_ref, h, IQ)
            cfk = coef_row(hw_ref, h, JK)
            qgh = [qg_ref[x, 4 * h : 4 * h + 4] for x in range(3)]
            kgh = [kg_ref[x, 4 * h : 4 * h + 4] for x in range(3)]
            qf = jnp.concatenate(
                [q_ref[C * h : C * h + C] * (WL * WS)] + qgh + [jnp.where(row4q == 0, 1.0, 0.0)], 0
            )
            kf = jnp.concatenate(
                [k_ref[C * h : C * h + C] * (WL * WS)] + kgh + [jnp.where(row4k == 0, 1.0, 0.0)], 0
            )
            gf = jnp.concatenate(
                [go_ref[C * h : C * h + C]] + [gg_ref[x, 8 * h : 8 * h + 8] for x in range(3)], 0
            )
            vf = jnp.concatenate([vg_ref[x, 8 * h : 8 * h + 8] for x in range(3)], 0)

            def three(left, n, right1, right2, dims):
                hi, lo = split2(left)
                both = mm(jnp.concatenate([hi, lo], 0), right1, dims)
                return both[:n] + both[n:] + mm(hi, right2, dims)

            kside = three(qf, 32, d1, d2, NN)
            vside = three(gf, 40, a1, a2, NN)
            qside = three(kf, 32, d1, d2, NT)
            oside = three(vf, 24, a1, a2, NT)
            csum, rsum = kside[28:29], qside[28:29]
            kp_ref[KEY0 + C * h : KEY0 + C * h + C] = kside[0:16]
            kp_ref[VAL0 + C * h : VAL0 + C * h + C] = vside[0:16]
            qp_ref[QRY0 + C * h : QRY0 + C * h + C] = qside[0:16]
            tk = jnp.zeros((1, JK), F32)
            tq = jnp.zeros((1, IQ), F32)
            for x in range(3):
                kq = kside[16 + 4 * x : 20 + 4 * x]
                qk = qside[16 + 4 * x : 20 + 4 * x]
                kp_ref[KPT0 + 48 * x + 4 * h : KPT0 + 48 * x + 4 * h + 4] = (2.0 * cfk) * (
                    kq - kgh[x] * csum
                )
                qp_ref[QPT0 + 48 * x + 4 * h : QPT0 + 48 * x + 4 * h + 4] = (-2.0 * cfq) * (
                    qgh[x] * rsum - qk
                )
                kp_ref[VPT0 + 96 * x + 8 * h : VPT0 + 96 * x + 8 * h + 8] = vside[
                    16 + 8 * x : 24 + 8 * x
                ]
                qp_ref[OPT0 + 96 * x + 8 * h : OPT0 + 96 * x + 8 * h + 8] = oside[
                    8 * x : 8 * x + 8
                ]
                tk = tk + jnp.sum(kgh[x] * (kgh[x] * csum - 2.0 * kq), axis=0, keepdims=True)
                tq = tq + jnp.sum(qgh[x] * qgh[x], axis=0, keepdims=True)
            part = jnp.sum(tk, axis=1, keepdims=True) + jnp.sum(tq * rsum, axis=1, keepdims=True)
            hs = jnp.where(lane == 48 + h, part, hs)
        hs_ref[...] = hs

    dlogs = []
    for n in range(QB):
        rows = jnp.concatenate(
            [da_ref[half, pl.ds(step * QB + n, 32, stride=IQ), :] for half in range(2)], 1
        ).astype(BF16)
        d_ref[n] = rows
        dlogs.append(rows[:16])
    w_ref[...] += mm(
        jnp.concatenate(dlogs, 1), pair_ref[...].reshape(QB * JK, CZ), NN
    )

    @pl.when(step == IQ // QB - 1)
    def _():
        core = lax.axis_index("row_2")
        w0 = w_ref[0:8]
        w1 = w_ref[8:16]
        lane = lax.broadcasted_iota(jnp.int32, (8, 128), 1)
        sub = lax.broadcasted_iota(jnp.int32, (8, 128), 0)
        fold = jnp.where(sub < 4, pltpu.roll(w1, 64, 1), pltpu.roll(w1, 4, 0))
        extra = jnp.where(lane < 64, hs_ref[...], fold)
        keys = [
            [kp_ref[128 * t : 128 * t + 128, 128 * b : 128 * b + 128].T for t in range(7)]
            for b in range(2)
        ]
        for b in range(2):
            for s in range(16):
                zone, parity = divmod(16 * b + s, 2)
                spot = core if parity else 1 - core
                spot = jnp.abs(parity - core)
                for t in range(6):
                    key_ref[spot, zone, :, 128 * t : 128 * t + 128] = keys[b][t][8 * s : 8 * s + 8]
                key_ref[spot, zone, :, 768:896] = jnp.where(
                    lane < 48, keys[b][6][8 * s : 8 * s + 8], extra
                )
                key_ref[spot, zone, :, 896:1024] = w0
        for t in range(5):
            block = qp_ref[128 * t : 128 * t + 128]
            turned = jnp.concatenate([block, jnp.zeros((128, 64), F32)], 1).T
            for c in range(NCOL):
                qry_ref[c, :, 128 * t : 128 * t + 128] = turned[8 * c : 8 * c + 8]


def pair_kernel(d_ref, gp_ref, bw_ref, out_ref, wt_ref):
    @pl.when(pl.program_id(0) == 0)
    def _():
        wide = jnp.concatenate([bw_ref[...].astype(F32), jnp.zeros((CZ, 128 - H), F32)], 1)
        hi, lo = split2(wide.T[:16] * WL)
        wt_ref[0:16] = hi
        wt_ref[16:32] = lo

    pad = jnp.zeros((4, CZ), BF16)
    for n in range(QB):
        rows = d_ref[n]
        lhs = jnp.concatenate([rows[:16], rows], 0)
        rhs = jnp.concatenate([wt_ref[...], jnp.concatenate([gp_ref[n], pad], 0)], 0)
        out_ref[n] = mm(lhs, rhs, TN).astype(BF16)


def mid_kernel(parts_ref, qry_ref, keys_ref, send_ref):
    total = jnp.sum(parts_ref[...], axis=0)
    keys_ref[...] = total
    for c in range(NCOL):
        send_ref[c, :, 0:QW] = qry_ref[c]
        send_ref[c, :, QW : QW + 128] = total[:, 896:1024]
        send_ref[c, :, QW + 128 : QW + 256] = total[:, 768:896]


def turn(block):
    return jnp.concatenate([block, jnp.zeros((120, 128), F32)], 0).T[:, :8]


def own_lanes(ref, offset):
    base = pl.multiple_of(lax.div(offset, 128) * 128, 128)
    off = lax.rem(offset, 128)
    return [lanes_at(ref[y, :, pl.ds(base, 128)], off, 8) for y in range(3)]


def sum0(x):
    return jnp.sum(x, axis=0, keepdims=True)


def key_kernel(keys_ref, kp_ref, vp_ref, rot_ref, kgr_ref, vgr_ref, kpg_ref, vpg_ref, kfr_ref):
    flat = jnp.concatenate([turn(keys_ref[:, 128 * t : 128 * t + 128]) for t in range(7)], 0)
    kgr_ref[...] = flat[KEY0:VAL0]
    vgr_ref[...] = flat[VAL0:KPT0]
    dk = [flat[KPT0 + 48 * x : KPT0 + 48 * x + 48] for x in range(3)]
    dv = [flat[VPT0 + 96 * x : VPT0 + 96 * x + 96] for x in range(3)]
    offset = row_index() * 8
    kp = own_lanes(kp_ref, offset)
    vp = own_lanes(vp_ref, offset)
    base = pl.multiple_of(col_index() * JK + lax.div(offset, 128) * 128, 128)
    rot = []
    for x in range(3):
        block = lanes_at(
            jnp.concatenate([rot_ref[x, :, pl.ds(base, 128)], jnp.zeros((5, 128), F32)], 0),
            lax.rem(offset, 128),
            8,
        )
        rot.append([block[y : y + 1] for y in range(3)])
    for y in range(3):
        kpg_ref[y] = rot[0][y] * dk[0] + rot[1][y] * dk[1] + rot[2][y] * dk[2]
        vpg_ref[y] = rot[0][y] * dv[0] + rot[1][y] * dv[1] + rot[2][y] * dv[2]
    for x in range(3):
        for y in range(3):
            kfr_ref[x, y : y + 1] = sum0(dk[x] * kp[y]) + sum0(dv[x] * vp[y])
        kfr_ref[x, 3:4] = sum0(dk[x]) + sum0(dv[x])


def last_kernel(
    hw_ref, parts_ref, qp_ref, gpt_ref, gg_ref, rot_ref, tr_ref,
    qgr_ref, qpg_ref, qfr_ref, wg_ref, hg_ref,
):
    total = jnp.sum(parts_ref[...], axis=0)
    flat = jnp.concatenate([turn(total[:, 128 * t : 128 * t + 128]) for t in range(5)], 0)
    qgr_ref[...] = flat[QRY0:QPT0]
    dq = [flat[QPT0 + 48 * x : QPT0 + 48 * x + 48] for x in range(3)]
    opt = [flat[OPT0 + 96 * x : OPT0 + 96 * x + 96] for x in range(3)]
    offset = col_index() * 8
    rot, tr = row_frames(rot_ref, tr_ref, offset, 8)

    def own(ref):
        return [
            lanes_at(jnp.concatenate([ref[y], ref[y]], 1), offset, 8) for y in range(3)
        ]

    qp, gpt, gg = own(qp_ref), own(gpt_ref), own(gg_ref)
    for y in range(3):
        qpg_ref[y] = rot[0][y] * dq[0] + rot[1][y] * dq[1] + rot[2][y] * dq[2]
    for x in range(3):
        away = opt[x] - tr[x]
        for y in range(3):
            qfr_ref[x, y : y + 1] = sum0(dq[x] * qp[y]) + sum0(away * gpt[y])
        qfr_ref[x, 3:4] = sum0(dq[x]) - sum0(gg[x])
    w0 = total[:, QW : QW + 128]
    extra = total[:, QW + 128 : QW + 256]
    lane4 = lax.broadcasted_iota(jnp.int32, (4, 128), 1)
    w1 = jnp.where(lane4 < 64, pltpu.roll(extra, 64, 1)[0:4], extra[4:8])
    wide = jnp.concatenate([w0, w1, jnp.zeros((116, 128), F32)], 0).T
    wg_ref[...] = (WL * wide)[:, :H]
    lane = lax.broadcasted_iota(jnp.int32, (1, 128), 1)
    raw = jnp.zeros((1, 128), F32)
    for h in range(H):
        raw = jnp.where(lane == h, hw_ref[h], raw)
    sig = 1.0 / (1.0 + jnp.exp(-raw))
    sums = pltpu.roll(extra, 128 - 48, 1)[0:1]
    hg_ref[...] = ((-0.5 * WL * WC) * sums * sig)[:, :H]


def struct(shape, dtype=F32):
    return jax.ShapeDtypeStruct(shape, dtype)


def cost(us, nbytes):
    return pl.CostEstimate(flops=int(us * 4e6), bytes_accessed=int(nbytes), transcendentals=0)


def per_device(
    pair_rep, bias_weight, head_weight, queries, key_vectors, values, query_points, key_points,
    value_points, rotations, translations, residue_count, grad_output, grad_points, grad_pair,
):
    steps = IQ // QB
    pair_spec = pl.BlockSpec((QB, JK, CZ), lambda i: (i, 0, 0))
    gp_spec = pl.BlockSpec((QB, H, CZ), lambda i: (i, 0, 0))
    e, p, st, qg, kg, vg, gg = pl.pallas_call(
        logits_kernel,
        name="logits",
        grid=(steps,),
        in_specs=[SMEM_SPEC, SMEM_SPEC, pair_spec, gp_spec] + [VMEM_SPEC] * 11,
        out_specs=[VMEM_SPEC] * 7,
        out_shape=[
            struct((H, IQ, JK)), struct((H, IQ, JK)), struct((NCOL, 24, 128)),
            struct((3, 48, IQ)), struct((3, 48, JK)), struct((3, 96, JK)), struct((3, 96, IQ)),
        ],
        scratch_shapes=[pltpu.VMEM((2, 32 * IQ, 128), F32), pltpu.VMEM((16, CZ), BF16)],
        cost_estimate=cost(8, 6e6),
    )(
        head_weight, residue_count, pair_rep, grad_pair, bias_weight, queries, key_vectors, values,
        query_points, key_points, value_points, rotations, translations, grad_output, grad_points,
    )
    everyone = lax.all_to_all(st, COL, 0, 0, tiled=True)
    d, keys, qry = pl.pallas_call(
        grads_kernel,
        name="grads",
        grid=(steps,),
        in_specs=[SMEM_SPEC] + [VMEM_SPEC] * 11 + [pair_spec],
        out_specs=[pl.BlockSpec((QB, 32, JK), lambda i: (i, 0, 0)), VMEM_SPEC, VMEM_SPEC],
        out_shape=[
            struct((IQ, 32, JK), BF16), struct((2, NCHIP, 8, KW)), struct((NCOL, 8, QW)),
        ],
        scratch_shapes=[
            pltpu.VMEM((2, 32 * IQ, 128), F32), pltpu.VMEM((896, JK), F32),
            pltpu.VMEM((QW, IQ), F32), pltpu.VMEM((16, CZ), F32), pltpu.VMEM((8, 128), F32),
        ],
        cost_estimate=cost(8, 8e6),
    )(
        head_weight, e, p, st, everyone, queries, key_vectors, grad_output, qg, kg, vg, gg, pair_rep,
    )
    swapped = lax.ppermute(keys[1], "row_2", [(0, 1), (1, 0)])
    parts = lax.all_to_all(keys[0] + swapped, CHIPS, 0, 0, tiled=True)
    pair_grad = pl.pallas_call(
        pair_kernel,
        name="pair",
        grid=(steps,),
        in_specs=[pl.BlockSpec((QB, 32, JK), lambda i: (i, 0, 0)), gp_spec, VMEM_SPEC],
        out_specs=pair_spec,
        out_shape=struct((IQ, JK, CZ), BF16),
        scratch_shapes=[pltpu.VMEM((32, CZ), BF16)],
        cost_estimate=cost(6, 6e6),
    )(d, grad_pair, bias_weight)
    keysum, send = pl.pallas_call(
        mid_kernel,
        name="mid",
        in_specs=[VMEM_SPEC] * 2,
        out_specs=[VMEM_SPEC] * 2,
        out_shape=[struct((8, KW)), struct((NCOL, 8, QW + 256))],
        cost_estimate=cost(1, 1e6),
    )(parts, qry)
    last = lax.all_to_all(send, COL, 0, 0, tiled=True)
    key_grad, value_grad, key_point_grad, value_point_grad, key_frame_grad = pl.pallas_call(
        key_kernel,
        name="keyout",
        in_specs=[VMEM_SPEC] * 4,
        out_specs=[VMEM_SPEC] * 5,
        out_shape=[
            struct((192, 8)), struct((192, 8)), struct((3, 48, 8)), struct((3, 96, 8)),
            struct((3, 4, 8)),
        ],
        cost_estimate=cost(2, 1e6),
    )(keysum, key_points, value_points, rotations)
    query_grad, query_point_grad, query_frame_grad, weight_grad, head_grad = pl.pallas_call(
        last_kernel,
        name="last",
        in_specs=[SMEM_SPEC] + [VMEM_SPEC] * 6,
        out_specs=[VMEM_SPEC] * 5,
        out_shape=[
            struct((192, 8)), struct((3, 48, 8)), struct((3, 4, 8)), struct((CZ, H)),
            struct((1, H)),
        ],
        cost_estimate=cost(2, 1e6),
    )(head_weight, last, query_points, grad_points, gg, rotations, translations)
    return (
        pair_grad, query_grad, query_point_grad, query_frame_grad, key_grad, value_grad,
        key_point_grad, value_point_grad, key_frame_grad, weight_grad, head_grad.reshape(H),
    )


def solution(mesh):
    finer = Mesh(mesh.devices.reshape(4, 4, 2, 4, 2), ROW_COL)
    in_specs = (
        P(ROW, COL, None), P(), P(), P(None, ROW), P(None, COL), P(None, COL),
        P(None, None, ROW), P(None, None, COL), P(None, None, COL), P(), P(), P(),
        P(None, ROW), P(None, None, ROW), P(ROW, None, None),
    )
    out_specs = (
        P(ROW, COL, None), P(None, ROW_COL), P(None, None, ROW_COL), P(None, None, ROW_COL),
        P(None, COL_ROW), P(None, COL_ROW), P(None, None, COL_ROW), P(None, None, COL_ROW),
        P(None, None, COL_ROW), P(), P(),
    )
    return jax.shard_map(
        per_device, mesh=finer, in_specs=in_specs, out_specs=out_specs, check_vma=False
    )
```

```python
import functools
import math

import jax
import jax.numpy as jnp
from jax import lax
from jax.experimental import pallas as pl
from jax.experimental.pallas import tpu as pltpu
from jax.sharding import Mesh
from jax.sharding import PartitionSpec as P

ROW = ("row_0", "row_1", "row_2")
COL = ("col_0", "col_1")
ROW_COL = ROW + COL
COL_ROW = COL + ROW
CHIPS = ("row_0", "row_1")

H, C, PQ, PV, CZ = 12, 16, 4, 8, 128
IQ, JK = 64, 256
NCOL, NROW, NCHIP = 8, 32, 16
WL = math.sqrt(1.0 / 3.0)
WC = math.sqrt(2.0 / (9.0 * PQ))
WS = 1.0 / math.sqrt(C)
MASKED = -1000000000.0

KEY0, VAL0, KPT0, VPT0, KEND = 0, 192, 384, 528, 816
QRY0, QPT0, OPT0, QEND = 0, 192, 336, 624
KW, QW = 1024, 640
QB = 8

F32, BF16 = jnp.float32, jnp.bfloat16
VMEM_SPEC = pl.BlockSpec(memory_space=pltpu.VMEM)
SMEM_SPEC = pl.BlockSpec(memory_space=pltpu.SMEM)
TN = (((0,), (0,)), ((), ()))
NT = (((1,), (1,)), ((), ()))
NN = (((1,), (0,)), ((), ()))


def mm(a, b, dims):
    return lax.dot_general(a, b, dims, preferred_element_type=F32)


def split2(x):
    hi = x.astype(BF16)
    return hi, (x - hi.astype(F32)).astype(BF16)


def split3(x):
    hi = x.astype(BF16)
    rest = x - hi.astype(F32)
    mid = rest.astype(BF16)
    return hi, mid, (rest - mid.astype(F32)).astype(BF16)


def row_index():
    return (lax.axis_index("row_0") * 4 + lax.axis_index("row_1")) * 2 + lax.axis_index("row_2")


def col_index():
    return lax.axis_index("col_0") * 2 + lax.axis_index("col_1")


def soft(hw_ref, h, lanes):
    w = jnp.full((1, lanes), hw_ref[h], F32)
    return jnp.maximum(w, 0.0) + jnp.log1p(jnp.exp(-jnp.abs(w)))


def coef_row(hw_ref, h, lanes):
    return (0.5 * WL * WC) * soft(hw_ref, h, lanes)


def rotate(rot, shift, local):
    out = []
    for x in range(3):
        g = rot[x][0] * local[0] + rot[x][1] * local[1] + rot[x][2] * local[2]
        out.append(g if shift is None else g + shift[x])
    return out


def flip(x):
    rows, lanes = x.shape
    full = -(-lanes // 128) * 128
    if full > lanes:
        x = jnp.concatenate([x, jnp.zeros((rows, full - lanes), F32)], 1)
    x = jnp.concatenate([x, jnp.zeros((128 - rows, full), F32)], 0)
    return jnp.concatenate(
        [x[:, t : t + 128].T for t in range(0, full, 128)], 0
    )[:, :rows]


def col_frames(rot_ref, tr_ref):
    start = pl.multiple_of(col_index() * JK, JK)
    rot = [[rot_ref[x, y : y + 1, pl.ds(start, JK)] for y in range(3)] for x in range(3)]
    tr = [tr_ref[x : x + 1, pl.ds(start, JK)] for x in range(3)]
    return rot, tr


def lanes_at(block, offset, count):
    return pltpu.roll(block, lax.rem(128 - offset, 128), block.ndim - 1)[..., :count]


def row_frames(rot_ref, tr_ref, offset, count):
    at = row_index() * IQ + offset
    base = pl.multiple_of(lax.div(at, 128) * 128, 128)
    off = lax.rem(at, 128)
    rot = []
    for x in range(3):
        block = lanes_at(
            jnp.concatenate([rot_ref[x, :, pl.ds(base, 128)], jnp.zeros((5, 128), F32)], 0),
            off,
            count,
        )
        rot.append([block[y : y + 1] for y in range(3)])
    block = lanes_at(
        jnp.concatenate([tr_ref[:, pl.ds(base, 128)], jnp.zeros((5, 128), F32)], 0), off, count
    )
    return rot, [block[x : x + 1] for x in range(3)]


def logits_kernel(
    hw_ref, rc_ref, pair_ref, gp_ref, bw_ref, qt_ref, k_ref, v_ref, qp_ref, kp_ref, vp_ref,
    rot_ref, tr_ref, got_ref, gpt_ref,
    e_ref, p_ref, st_ref, q_ref, go_ref, qg_ref, kg_ref, vg_ref, gg_ref,
    bp_ref, gs_ref,
):
    step = pl.program_id(0)
    wt = jnp.concatenate([bw_ref[...].astype(F32), jnp.zeros((4, CZ), F32)], 0)
    gs_ref[...] = gp_ref[...].astype(F32).reshape(H * QB, CZ)
    for n in range(QB):
        lhs = jnp.concatenate([wt, gs_ref[pl.ds(n, H, stride=QB), :]], 0).astype(BF16)
        res = mm(lhs, pair_ref[n], NT)
        for half in range(2):
            bp_ref[half, pl.ds(step * QB + n, 16 + H, stride=IQ), :] = res[
                :, half * 128 : half * 128 + 128
            ]

    @pl.when(step == IQ // QB - 1)
    def _():
        crot, ctr = col_frames(rot_ref, tr_ref)
        rrot, rtr = row_frames(rot_ref, tr_ref, 0, IQ)
        kg = rotate(crot, ctr, [kp_ref[y] for y in range(3)])
        vg = rotate(crot, ctr, [vp_ref[y] for y in range(3)])
        qg = rotate(rrot, rtr, [qp_ref[y] for y in range(3)])
        gg = rotate(rrot, None, [flip(gpt_ref[y])[: H * PV] for y in range(3)])
        q_ref[...] = flip(qt_ref[...])[: H * C]
        go_ref[...] = flip(got_ref[...])[: H * C]
        for x in range(3):
            kg_ref[x], vg_ref[x], qg_ref[x], gg_ref[x] = kg[x], vg[x], qg[x], gg[x]
        real = (
            lax.broadcasted_iota(jnp.int32, (IQ, JK), 1) + col_index() * JK < rc_ref[0]
        )
        lane = lax.broadcasted_iota(jnp.int32, (IQ, 128), 1)
        stats = [jnp.zeros((IQ, 128), F32), jnp.zeros((IQ, 128), F32)]
        row4q = lax.broadcasted_iota(jnp.int32, (4, IQ), 0)
        row4k = lax.broadcasted_iota(jnp.int32, (4, JK), 0)
        for h in range(H):
            cf = coef_row(hw_ref, h, IQ)
            qgh = [qg_ref[x, 4 * h : 4 * h + 4] for x in range(3)]
            kgh = [kg_ref[x, 4 * h : 4 * h + 4] for x in range(3)]
            qn = sum(jnp.sum(t * t, axis=0, keepdims=True) for t in qgh)
            kn = sum(jnp.sum(t * t, axis=0, keepdims=True) for t in kgh)
            qtail = jnp.where(row4q == 0, -cf, jnp.where(row4q == 1, -cf * qn, 0.0))
            ktail = jnp.where(row4k == 0, kn, jnp.where(row4k == 1, 1.0, 0.0))
            qf = jnp.concatenate(
                [q_ref[C * h : C * h + C] * (WL * WS)] + [2.0 * cf * t for t in qgh] + [qtail], 0
            )
            kf = jnp.concatenate([k_ref[C * h : C * h + C]] + kgh + [ktail], 0)
            a1, a2, a3 = split3(qf)
            b1, b2, b3 = split3(kf)
            core = mm(
                jnp.concatenate([a1, a1, a2, a1, a2, a3], 0),
                jnp.concatenate([b1, b2, b1, b3, b2, b1], 0),
                TN,
            )
            gf = jnp.concatenate(
                [go_ref[C * h : C * h + C]] + [gg_ref[x, 8 * h : 8 * h + 8] for x in range(3)]
                + [jnp.zeros((8, IQ), F32)], 0
            )
            vf = jnp.concatenate(
                [v_ref[C * h : C * h + C]] + [vg_ref[x, 8 * h : 8 * h + 8] for x in range(3)]
                + [jnp.zeros((8, JK), F32)], 0
            )
            g1, g2 = split2(gf)
            v1, v2 = split2(vf)
            prod = mm(
                jnp.concatenate([g1, g1, g2], 0), jnp.concatenate([v1, v2, v1], 0), TN
            )

            def planes(base):
                return jnp.concatenate(
                    [bp_ref[half, base * IQ : base * IQ + IQ, :] for half in range(2)], 1
                )

            logit = jnp.where(real, core + WL * planes(h), MASKED)
            prod = prod + planes(16 + h)
            peak = jnp.max(logit, axis=1, keepdims=True)
            e = jnp.exp(logit - peak)
            e_ref[h] = e
            p_ref[h] = prod
            total = jnp.sum(e, axis=1, keepdims=True)
            upper = jnp.sum(e * prod, axis=1, keepdims=True)
            g, r = divmod(h, 6)
            acc = jnp.where(lane == r, peak, stats[g])
            acc = jnp.where(lane == 8 + r, total, acc)
            stats[g] = jnp.where(lane == 16 + r, upper, acc)
        packed = jnp.concatenate(stats, 0).T[:24]
        for c in range(NCOL):
            st_ref[c] = packed


def grads_kernel(
    hw_ref, e_ref, p_ref, own_ref, all_ref, q_ref, k_ref, go_ref, qg_ref, kg_ref, vg_ref, gg_ref,
    pair_ref,
    d_ref, keep_ref, give_ref, qry_ref,
    da_ref, kp_ref, qp_ref, w_ref, hs_ref,
):
    step = pl.program_id(0)

    @pl.when(step == 0)
    def _():
        peaks = all_ref[:, 0:8]
        top = jnp.max(peaks, axis=0)
        grow = jnp.exp(peaks - top[None])
        total = jnp.sum(all_ref[:, 8:16] * grow, axis=0)
        upper = jnp.sum(all_ref[:, 16:24] * grow, axis=0)
        scale = jnp.exp(own_ref[0, 0:8] - top) / total
        delta = upper / total
        cols = jnp.concatenate([scale, delta, jnp.zeros((112, 128), F32)], 0).T
        w_ref[...] = jnp.zeros_like(w_ref)
        for half in range(2):
            da_ref[half, H * IQ : 16 * IQ, :] = jnp.zeros((4 * IQ, 128), F32)
            da_ref[half, 28 * IQ : 32 * IQ, :] = jnp.zeros((4 * IQ, 128), F32)
        row4q = lax.broadcasted_iota(jnp.int32, (4, IQ), 0)
        row4k = lax.broadcasted_iota(jnp.int32, (4, JK), 0)
        lane = lax.broadcasted_iota(jnp.int32, (8, 128), 1)
        hs = jnp.zeros((8, 128), F32)
        for h in range(H):
            g, r = divmod(h, 6)
            sc = cols[IQ * g : IQ * g + IQ, r : r + 1]
            dl = cols[IQ * g : IQ * g + IQ, 8 + r : 9 + r]
            a = e_ref[h] * sc
            d = a * (p_ref[h] - dl)
            for half in range(2):
                piece = slice(half * 128, half * 128 + 128)
                da_ref[half, h * IQ : h * IQ + IQ, :] = d[:, piece]
                da_ref[half, (16 + h) * IQ : (17 + h) * IQ, :] = a[:, piece]
            d1, d2 = split2(d)
            a1, a2 = split2(a)
            cfq = coef_row(hw_ref, h, IQ)
            cfk = coef_row(hw_ref, h, JK)
            qgh = [qg_ref[x, 4 * h : 4 * h + 4] for x in range(3)]
            kgh = [kg_ref[x, 4 * h : 4 * h + 4] for x in range(3)]
            qf = jnp.concatenate(
                [q_ref[C * h : C * h + C] * (WL * WS)] + qgh + [jnp.where(row4q == 0, 1.0, 0.0)], 0
            )
            kf = jnp.concatenate(
                [k_ref[C * h : C * h + C] * (WL * WS)] + kgh + [jnp.where(row4k == 0, 1.0, 0.0)], 0
            )
            gf = jnp.concatenate(
                [go_ref[C * h : C * h + C]] + [gg_ref[x, 8 * h : 8 * h + 8] for x in range(3)], 0
            )
            vf = jnp.concatenate([vg_ref[x, 8 * h : 8 * h + 8] for x in range(3)], 0)

            def three(left, n, right1, right2, dims):
                hi, lo = split2(left)
                both = mm(jnp.concatenate([hi, lo], 0), right1, dims)
                return both[:n] + both[n:] + mm(hi, right2, dims)

            kside = three(qf, 32, d1, d2, NN)
            vside = three(gf, 40, a1, a2, NN)
            qside = three(kf, 32, d1, d2, NT)
            oside = three(vf, 24, a1, a2, NT)
            csum, rsum = kside[28:29], qside[28:29]
            kp_ref[KEY0 + C * h : KEY0 + C * h + C] = kside[0:16]
            kp_ref[VAL0 + C * h : VAL0 + C * h + C] = vside[0:16]
            qp_ref[QRY0 + C * h : QRY0 + C * h + C] = qside[0:16]
            tk = jnp.zeros((1, JK), F32)
            tq = jnp.zeros((1, IQ), F32)
            for x in range(3):
                kq = kside[16 + 4 * x : 20 + 4 * x]
                qk = qside[16 + 4 * x : 20 + 4 * x]
                kp_ref[KPT0 + 48 * x + 4 * h : KPT0 + 48 * x + 4 * h + 4] = (2.0 * cfk) * (
                    kq - kgh[x] * csum
                )
                qp_ref[QPT0 + 48 * x + 4 * h : QPT0 + 48 * x + 4 * h + 4] = (-2.0 * cfq) * (
                    qgh[x] * rsum - qk
                )
                kp_ref[VPT0 + 96 * x + 8 * h : VPT0 + 96 * x + 8 * h + 8] = vside[
                    16 + 8 * x : 24 + 8 * x
                ]
                qp_ref[OPT0 + 96 * x + 8 * h : OPT0 + 96 * x + 8 * h + 8] = oside[
                    8 * x : 8 * x + 8
                ]
                tk = tk + jnp.sum(kgh[x] * (kgh[x] * csum - 2.0 * kq), axis=0, keepdims=True)
                tq = tq + jnp.sum(qgh[x] * qgh[x], axis=0, keepdims=True)
            part = jnp.sum(tk, axis=1, keepdims=True) + jnp.sum(tq * rsum, axis=1, keepdims=True)
            hs = jnp.where(lane == 48 + h, part, hs)
        hs_ref[...] = hs

    dlogs = []
    for n in range(QB):
        rows = jnp.concatenate(
            [da_ref[half, pl.ds(step * QB + n, 32, stride=IQ), :] for half in range(2)], 1
        ).astype(BF16)
        d_ref[n] = rows
        dlogs.append(rows[:16])
    w_ref[...] += mm(
        jnp.concatenate(dlogs, 1), pair_ref[...].reshape(QB * JK, CZ), NN
    )

    @pl.when(step == IQ // QB - 1)
    def _():
        core = lax.axis_index("row_2")
        w0 = w_ref[0:8]
        w1 = w_ref[8:16]
        lane = lax.broadcasted_iota(jnp.int32, (8, 128), 1)
        sub = lax.broadcasted_iota(jnp.int32, (8, 128), 0)
        fold = jnp.where(sub < 4, pltpu.roll(w1, 64, 1), pltpu.roll(w1, 4, 0))
        extra = jnp.where(lane < 64, hs_ref[...], fold)
        keys = [
            [kp_ref[128 * t : 128 * t + 128, 128 * b : 128 * b + 128].T for t in range(7)]
            for b in range(2)
        ]
        def tile(j, t):
            b, r = divmod(j, 16)
            if t == 7:
                return w0
            piece = keys[b][t][8 * r : 8 * r + 8]
            return jnp.where(lane < 48, piece, extra) if t == 6 else piece

        first = core == 0
        for zone in range(NCHIP):
            for t in range(8):
                even, odd = tile(2 * zone, t), tile(2 * zone + 1, t)
                keep_ref[zone, :, 128 * t : 128 * t + 128] = jnp.where(first, even, odd)
                give_ref[zone, :, 128 * t : 128 * t + 128] = jnp.where(first, odd, even)
        for t in range(5):
            block = qp_ref[128 * t : 128 * t + 128]
            turned = jnp.concatenate([block, jnp.zeros((128, 64), F32)], 1).T
            for c in range(NCOL):
                qry_ref[c, :, 128 * t : 128 * t + 128] = turned[8 * c : 8 * c + 8]


def pair_kernel(d_ref, gp_ref, bw_ref, out_ref, gs_ref):
    wide = jnp.concatenate([bw_ref[...].astype(F32) * WL, jnp.zeros((4, CZ), F32)], 0)
    hi, lo = split2(wide)
    gs_ref[...] = gp_ref[...].astype(F32).reshape(H * QB, CZ)
    pad = jnp.zeros((4, CZ), F32)
    for n in range(QB):
        rows = d_ref[n]
        lhs = jnp.concatenate([rows[:16], rows], 0)
        part = jnp.concatenate([gs_ref[pl.ds(n, H, stride=QB), :], pad], 0).astype(BF16)
        rhs = jnp.concatenate([hi, lo, part], 0)
        out_ref[n] = mm(lhs, rhs, TN).astype(BF16)


def mid_kernel(parts_ref, qry_ref, keys_ref, send_ref):
    total = jnp.sum(parts_ref[...], axis=0)
    keys_ref[...] = total
    for c in range(NCOL):
        send_ref[c, :, 0:QW] = qry_ref[c]
        send_ref[c, :, QW : QW + 128] = total[:, 896:1024]
        send_ref[c, :, QW + 128 : QW + 256] = total[:, 768:896]


def own_lanes(ref, offset, rows):
    base = pl.multiple_of(lax.div(offset, 128) * 128, 128)
    off = lax.rem(offset, 128)
    return [lanes_at(ref[y, :, pl.ds(base, 128)], off, 128) for y in range(3)]


def sum1(x):
    return jnp.sum(x, axis=1, keepdims=True)


def frame_cols(rot_ref, tr_ref, at):
    base = pl.multiple_of(lax.div(at, 128) * 128, 128)
    rows = [rot_ref[x, :, pl.ds(base, 128)] for x in range(3)] + [tr_ref[:, pl.ds(base, 128)]]
    block = jnp.concatenate(rows + [jnp.zeros((116, 128), F32)], 0)
    return lanes_at(block, lax.rem(at, 128), 128).T[:8]


def tall(rows):
    x = jnp.concatenate(rows, 0)
    full = -(-x.shape[0] // 128) * 128
    if full > x.shape[0]:
        x = jnp.concatenate([x, jnp.zeros((full - x.shape[0], 128), F32)], 0)
    return jnp.concatenate([x[t : t + 128].T[:8] for t in range(0, full, 128)], 1)


def frame_out(ref, table):
    lane = lax.broadcasted_iota(jnp.int32, (8, 128), 1)
    block = jnp.zeros((8, 128), F32)
    for (x, y), column in table.items():
        block = jnp.where(lane == 4 * x + y, column, block)
    block = jnp.concatenate([block, jnp.zeros((120, 128), F32)], 0).T
    for x in range(3):
        ref[x] = block[4 * x : 4 * x + 4, :8]


def key_kernel(
    keys_ref, kp_ref, vp_ref, qp_ref, rot_ref, tr_ref,
    kgr_ref, vgr_ref, kpg_ref, vpg_ref, kfr_ref, qpo_ref, fr_ref,
):
    flat = keys_ref[...]
    kgr_ref[...] = flat[:, KEY0:VAL0]
    vgr_ref[...] = flat[:, VAL0:KPT0]
    dk = [flat[:, KPT0 + 48 * x : KPT0 + 48 * x + 48] for x in range(3)]
    dv = [flat[:, VPT0 + 96 * x : VPT0 + 96 * x + 96] for x in range(3)]
    offset = row_index() * 8
    local = tall(own_lanes(kp_ref, offset, 48) + own_lanes(vp_ref, offset, 96))
    kp = [local[:, 48 * y : 48 * y + 48] for y in range(3)]
    vp = [local[:, 144 + 96 * y : 240 + 96 * y] for y in range(3)]
    fr = frame_cols(rot_ref, tr_ref, col_index() * JK + offset)
    rot = [[fr[:, 3 * x + y : 3 * x + y + 1] for y in range(3)] for x in range(3)]
    table = {}
    for y in range(3):
        kpg_ref[y] = rot[0][y] * dk[0] + rot[1][y] * dk[1] + rot[2][y] * dk[2]
        vpg_ref[y] = rot[0][y] * dv[0] + rot[1][y] * dv[1] + rot[2][y] * dv[2]
    for x in range(3):
        for y in range(3):
            table[x, y] = sum1(dk[x] * kp[y]) + sum1(dv[x] * vp[y])
        table[x, 3] = sum1(dk[x]) + sum1(dv[x])
    frame_out(kfr_ref, table)
    off = col_index() * 8
    qpo_ref[...] = tall(
        [lanes_at(jnp.concatenate([qp_ref[y], qp_ref[y]], 1), off, 128) for y in range(3)]
    )
    fr_ref[...] = frame_cols(rot_ref, tr_ref, row_index() * IQ + off)


def last_kernel(
    hw_ref, parts_ref, qpo_ref, fr_ref, gpt_ref, qgr_ref, qpg_ref, qfr_ref, wg_ref, hg_ref,
):
    total = jnp.sum(parts_ref[...], axis=0)
    qgr_ref[...] = total[:, QRY0:QPT0]
    dq = [total[:, QPT0 + 48 * x : QPT0 + 48 * x + 48] for x in range(3)]
    opt = [total[:, OPT0 + 96 * x : OPT0 + 96 * x + 96] for x in range(3)]
    fr = fr_ref[...]
    rot = [[fr[:, 3 * x + y : 3 * x + y + 1] for y in range(3)] for x in range(3)]
    at = pl.multiple_of(col_index() * 8, 8)
    gpt = [gpt_ref[y, pl.ds(at, 8), :] for y in range(3)]
    qp = [qpo_ref[:, 48 * y : 48 * y + 48] for y in range(3)]
    gsum = [sum1(g) for g in gpt]
    for y in range(3):
        qpg_ref[y] = rot[0][y] * dq[0] + rot[1][y] * dq[1] + rot[2][y] * dq[2]
    table = {}
    for x in range(3):
        away = opt[x] - fr[:, 9 + x : 10 + x]
        for y in range(3):
            table[x, y] = sum1(dq[x] * qp[y]) + sum1(away * gpt[y])
        back = rot[x][0] * gsum[0] + rot[x][1] * gsum[1] + rot[x][2] * gsum[2]
        table[x, 3] = sum1(dq[x]) - back
    frame_out(qfr_ref, table)
    w0 = total[:, QW : QW + 128]
    extra = total[:, QW + 128 : QW + 256]
    lane4 = lax.broadcasted_iota(jnp.int32, (4, 128), 1)
    wg_ref[0:8] = WL * w0
    wg_ref[8:12] = WL * jnp.where(lane4 < 64, pltpu.roll(extra, 64, 1)[0:4], extra[4:8])
    lane = lax.broadcasted_iota(jnp.int32, (1, 128), 1)
    raw = jnp.zeros((1, 128), F32)
    for h in range(H):
        raw = jnp.where(lane == h, hw_ref[h], raw)
    sig = 1.0 / (1.0 + jnp.exp(-raw))
    sums = pltpu.roll(extra, 128 - 48, 1)[0:1]
    hg_ref[...] = ((-0.5 * WL * WC) * sums * sig)[:, :H]


def struct(shape, dtype=F32):
    return jax.ShapeDtypeStruct(shape, dtype)


def cost(us, nbytes):
    return pl.CostEstimate(flops=int(us * 4e6), bytes_accessed=int(nbytes), transcendentals=0)


def per_device(
    pair_rep, bias_weight, head_weight, queries, key_vectors, values, query_points, key_points,
    value_points, rotations, translations, residue_count, grad_output, grad_points, grad_pair,
):
    steps = IQ // QB
    pair_spec = pl.BlockSpec((QB, JK, CZ), lambda i: (i, 0, 0))
    gp_spec = pl.BlockSpec((H, QB, CZ), lambda i: (0, i, 0))
    gp_heads = grad_pair.transpose(1, 0, 2)
    bw_heads = bias_weight.T
    gpt_rows = grad_points.transpose(0, 2, 1)
    e, p, st, q, go, qg, kg, vg, gg = pl.pallas_call(
        logits_kernel,
        name="logits",
        grid=(steps,),
        in_specs=[SMEM_SPEC, SMEM_SPEC, pair_spec, gp_spec] + [VMEM_SPEC] * 11,
        out_specs=[VMEM_SPEC] * 9,
        out_shape=[
            struct((H, IQ, JK)), struct((H, IQ, JK)), struct((NCOL, 24, 128)),
            struct((H * C, IQ)), struct((H * C, IQ)),
            struct((3, 48, IQ)), struct((3, 48, JK)), struct((3, 96, JK)), struct((3, 96, IQ)),
        ],
        scratch_shapes=[pltpu.VMEM((2, 32 * IQ, 128), F32), pltpu.VMEM((H * QB, CZ), F32)],
        cost_estimate=cost(8, 6e6),
    )(
        head_weight, residue_count, pair_rep, gp_heads, bw_heads, queries.T, key_vectors, values,
        query_points, key_points, value_points, rotations, translations, grad_output.T, gpt_rows,
    )
    everyone = lax.all_to_all(st, COL, 0, 0, tiled=True)
    d, keep, give, qry = pl.pallas_call(
        grads_kernel,
        name="grads",
        grid=(steps,),
        in_specs=[SMEM_SPEC] + [VMEM_SPEC] * 11 + [pair_spec],
        out_specs=[pl.BlockSpec((QB, 32, JK), lambda i: (i, 0, 0))] + [VMEM_SPEC] * 3,
        out_shape=[
            struct((IQ, 32, JK), BF16), struct((NCHIP, 8, KW)), struct((NCHIP, 8, KW)),
            struct((NCOL, 8, QW)),
        ],
        scratch_shapes=[
            pltpu.VMEM((2, 32 * IQ, 128), F32), pltpu.VMEM((896, JK), F32),
            pltpu.VMEM((QW, IQ), F32), pltpu.VMEM((16, CZ), F32), pltpu.VMEM((8, 128), F32),
        ],
        cost_estimate=cost(8, 8e6),
    )(head_weight, e, p, st, everyone, q, key_vectors, go, qg, kg, vg, gg, pair_rep)
    swapped = lax.ppermute(give, "row_2", [(0, 1), (1, 0)])
    parts = lax.all_to_all(keep + swapped, CHIPS, 0, 0, tiled=True)
    pair_grad = pl.pallas_call(
        pair_kernel,
        name="pair",
        grid=(steps,),
        in_specs=[pl.BlockSpec((QB, 32, JK), lambda i: (i, 0, 0)), gp_spec, VMEM_SPEC],
        out_specs=pair_spec,
        out_shape=struct((IQ, JK, CZ), BF16),
        scratch_shapes=[pltpu.VMEM((H * QB, CZ), F32)],
        cost_estimate=cost(6, 6e6),
    )(d, gp_heads, bw_heads)
    keysum, send = pl.pallas_call(
        mid_kernel,
        name="mid",
        in_specs=[VMEM_SPEC] * 2,
        out_specs=[VMEM_SPEC] * 2,
        out_shape=[struct((8, KW)), struct((NCOL, 8, QW + 256))],
        cost_estimate=cost(1, 1e6),
    )(parts, qry)
    last = lax.all_to_all(send, COL, 0, 0, tiled=True)
    key_grad, value_grad, key_point_grad, value_point_grad, key_frame_grad, qpo, fr = (
        pl.pallas_call(
            key_kernel,
            name="keyout",
            in_specs=[VMEM_SPEC] * 6,
            out_specs=[VMEM_SPEC] * 7,
            out_shape=[
                struct((8, 192)), struct((8, 192)), struct((3, 8, 48)), struct((3, 8, 96)),
                struct((3, 4, 8)), struct((8, 256)), struct((8, 128)),
            ],
            cost_estimate=cost(2, 1e6),
        )(keysum, key_points, value_points, query_points, rotations, translations)
    )
    query_grad, query_point_grad, query_frame_grad, weight_grad, head_grad = pl.pallas_call(
        last_kernel,
        name="last",
        in_specs=[SMEM_SPEC] + [VMEM_SPEC] * 4,
        out_specs=[VMEM_SPEC] * 5,
        out_shape=[
            struct((8, 192)), struct((3, 8, 48)), struct((3, 4, 8)), struct((H, CZ)),
            struct((1, H)),
        ],
        cost_estimate=cost(2, 1e6),
    )(head_weight, last, qpo, fr, gpt_rows)
    return (
        pair_grad, query_grad.T, query_point_grad.transpose(0, 2, 1), query_frame_grad, key_grad.T,
        value_grad.T, key_point_grad.transpose(0, 2, 1), value_point_grad.transpose(0, 2, 1),
        key_frame_grad, weight_grad.T, head_grad.reshape(H),
    )


def solution(mesh):
    finer = Mesh(mesh.devices.reshape(4, 4, 2, 4, 2), ROW_COL)
    in_specs = (
        P(ROW, COL, None), P(), P(), P(None, ROW), P(None, COL), P(None, COL),
        P(None, None, ROW), P(None, None, COL), P(None, None, COL), P(), P(), P(),
        P(None, ROW), P(None, None, ROW), P(ROW, None, None),
    )
    out_specs = (
        P(ROW, COL, None), P(None, ROW_COL), P(None, None, ROW_COL), P(None, None, ROW_COL),
        P(None, COL_ROW), P(None, COL_ROW), P(None, None, COL_ROW), P(None, None, COL_ROW),
        P(None, None, COL_ROW), P(), P(),
    )
    return jax.shard_map(
        per_device, mesh=finer, in_specs=in_specs, out_specs=out_specs, check_vma=False
    )
```

```python
import functools
import math

import jax
import jax.numpy as jnp
from jax import lax
from jax.experimental import pallas as pl
from jax.experimental.pallas import tpu as pltpu
from jax.sharding import Mesh
from jax.sharding import PartitionSpec as P

ROW = ("row_0", "row_1", "row_2")
COL = ("col_0", "col_1")
ROW_COL = ROW + COL
COL_ROW = COL + ROW
CHIPS = ("row_0", "row_1")

H, C, PQ, PV, CZ = 12, 16, 4, 8, 128
IQ, JK = 64, 256
NCOL, NROW, NCHIP = 8, 32, 16
WL = math.sqrt(1.0 / 3.0)
WC = math.sqrt(2.0 / (9.0 * PQ))
WS = 1.0 / math.sqrt(C)
MASKED = -1000000000.0

KEY0, VAL0, KPT0, VPT0, KEND = 0, 192, 384, 528, 816
QRY0, QPT0, OPT0, QEND = 0, 192, 336, 624
KW, QW = 1024, 640
LIMIT = 20 << 20
QB = 16
PB = 8

F32, BF16 = jnp.float32, jnp.bfloat16
VMEM_SPEC = pl.BlockSpec(memory_space=pltpu.VMEM)
SMEM_SPEC = pl.BlockSpec(memory_space=pltpu.SMEM)
TN = (((0,), (0,)), ((), ()))
NT = (((1,), (1,)), ((), ()))
NN = (((1,), (0,)), ((), ()))


def mm(a, b, dims):
    return lax.dot_general(a, b, dims, preferred_element_type=F32)


def split2(x):
    hi = x.astype(BF16)
    return hi, (x - hi.astype(F32)).astype(BF16)


def split3(x):
    hi = x.astype(BF16)
    rest = x - hi.astype(F32)
    mid = rest.astype(BF16)
    return hi, mid, (rest - mid.astype(F32)).astype(BF16)


def row_index():
    return (lax.axis_index("row_0") * 4 + lax.axis_index("row_1")) * 2 + lax.axis_index("row_2")


def col_index():
    return lax.axis_index("col_0") * 2 + lax.axis_index("col_1")


def soft(hw_ref, h, lanes):
    w = jnp.full((1, lanes), hw_ref[h], F32)
    return jnp.maximum(w, 0.0) + jnp.log1p(jnp.exp(-jnp.abs(w)))


def coef_row(hw_ref, h, lanes):
    return (0.5 * WL * WC) * soft(hw_ref, h, lanes)


def rotate(rot, shift, local):
    out = []
    for x in range(3):
        g = rot[x][0] * local[0] + rot[x][1] * local[1] + rot[x][2] * local[2]
        out.append(g if shift is None else g + shift[x])
    return out


def flip(x):
    rows, lanes = x.shape
    full = -(-lanes // 128) * 128
    if full > lanes:
        x = jnp.concatenate([x, jnp.zeros((rows, full - lanes), F32)], 1)
    x = jnp.concatenate([x, jnp.zeros((128 - rows, full), F32)], 0)
    return jnp.concatenate(
        [x[:, t : t + 128].T for t in range(0, full, 128)], 0
    )[:, :rows]


def col_frames(rot_ref, tr_ref):
    start = pl.multiple_of(col_index() * JK, JK)
    rot = [[rot_ref[x, y : y + 1, pl.ds(start, JK)] for y in range(3)] for x in range(3)]
    tr = [tr_ref[x : x + 1, pl.ds(start, JK)] for x in range(3)]
    return rot, tr


def lanes_at(block, offset, count):
    return pltpu.roll(block, lax.rem(128 - offset, 128), block.ndim - 1)[..., :count]


def row_frames(rot_ref, tr_ref, offset, count):
    at = row_index() * IQ + offset
    base = pl.multiple_of(lax.div(at, 128) * 128, 128)
    off = lax.rem(at, 128)
    rot = []
    for x in range(3):
        block = lanes_at(
            jnp.concatenate([rot_ref[x, :, pl.ds(base, 128)], jnp.zeros((5, 128), F32)], 0),
            off,
            count,
        )
        rot.append([block[y : y + 1] for y in range(3)])
    block = lanes_at(
        jnp.concatenate([tr_ref[:, pl.ds(base, 128)], jnp.zeros((5, 128), F32)], 0), off, count
    )
    return rot, [block[x : x + 1] for x in range(3)]


HBM_SPEC = pl.BlockSpec(memory_space=pltpu.HBM)


def logits_kernel(
    rc_ref, hw_hbm, pair_hbm, gp_hbm, bw_hbm, qt_hbm, k_hbm, v_hbm, qp_hbm, kp_hbm, vp_hbm,
    rot_hbm, tr_hbm, got_hbm, gpt_hbm,
    e_ref, p_ref, st_ref, q_ref, go_ref, qg_ref, kg_ref, vg_ref, gg_ref, pair_ref, k_ref,
    bp_ref, gs_ref, hw_ref, gp_ref, bw_ref, qt_ref, v_ref, qp_ref, kp_ref, vp_ref, rot_ref,
    tr_ref, got_ref, gpt_ref, sems, pair_sems,
):
    def pair_copy(b):
        part = pl.ds(b * PB, PB)
        return pltpu.make_async_copy(pair_hbm.at[part], pair_ref.at[part], pair_sems.at[b])

    moves = [
        (gp_hbm, gp_ref), (bw_hbm, bw_ref), (k_hbm, k_ref), (v_hbm, v_ref), (qt_hbm, qt_ref),
        (got_hbm, got_ref), (qp_hbm, qp_ref), (kp_hbm, kp_ref), (vp_hbm, vp_ref),
        (gpt_hbm, gpt_ref), (rot_hbm, rot_ref), (tr_hbm, tr_ref), (hw_hbm, hw_ref),
    ]
    copies = [pltpu.make_async_copy(a, b, sems.at[n]) for n, (a, b) in enumerate(moves)]
    for c in copies[:2]:
        c.start()
    pair_copy(0).start()
    for c in copies[2:]:
        c.start()
    for b in range(1, IQ // PB):
        pair_copy(b).start()
    for c in copies[:2]:
        c.wait()
    wt = jnp.concatenate([bw_ref[...].astype(F32), jnp.zeros((4, CZ), F32)], 0)
    gs_ref[...] = gp_ref[...].astype(F32).reshape(H * IQ, CZ)

    @pl.loop(0, IQ // PB)
    def _(b):
        pair_copy(b).wait()
        for n in range(PB):
            at = b * PB + n
            lhs = jnp.concatenate([wt, gs_ref[pl.ds(at, H, stride=IQ), :]], 0).astype(BF16)
            res = mm(lhs, pair_ref[at], NT)
            for half in range(2):
                bp_ref[half, pl.ds(at, 16 + H, stride=IQ), :] = res[
                    :, half * 128 : half * 128 + 128
                ]

    for c in copies[2:]:
        c.wait()
    crot, ctr = col_frames(rot_ref, tr_ref)
    rrot, rtr = row_frames(rot_ref, tr_ref, 0, IQ)
    kg = rotate(crot, ctr, [kp_ref[y] for y in range(3)])
    vg = rotate(crot, ctr, [vp_ref[y] for y in range(3)])
    qg = rotate(rrot, rtr, [qp_ref[y] for y in range(3)])
    gg = rotate(rrot, None, [flip(gpt_ref[y])[: H * PV] for y in range(3)])
    q_ref[...] = flip(qt_ref[...])[: H * C]
    go_ref[...] = flip(got_ref[...])[: H * C]
    for x in range(3):
        kg_ref[x], vg_ref[x], qg_ref[x], gg_ref[x] = kg[x], vg[x], qg[x], gg[x]
    real = (
        lax.broadcasted_iota(jnp.int32, (IQ, JK), 1) + col_index() * JK < rc_ref[0]
    )
    lane = lax.broadcasted_iota(jnp.int32, (IQ, 128), 1)
    stats = [jnp.zeros((IQ, 128), F32), jnp.zeros((IQ, 128), F32)]
    row4q = lax.broadcasted_iota(jnp.int32, (4, IQ), 0)
    row4k = lax.broadcasted_iota(jnp.int32, (4, JK), 0)
    for h in range(H):
        cf = coef_row(hw_ref, h, IQ)
        qgh = [qg_ref[x, 4 * h : 4 * h + 4] for x in range(3)]
        kgh = [kg_ref[x, 4 * h : 4 * h + 4] for x in range(3)]
        qn = sum(jnp.sum(t * t, axis=0, keepdims=True) for t in qgh)
        kn = sum(jnp.sum(t * t, axis=0, keepdims=True) for t in kgh)
        qtail = jnp.where(row4q == 0, -cf, jnp.where(row4q == 1, -cf * qn, 0.0))
        ktail = jnp.where(row4k == 0, kn, jnp.where(row4k == 1, 1.0, 0.0))
        qf = jnp.concatenate(
            [q_ref[C * h : C * h + C] * (WL * WS)] + [2.0 * cf * t for t in qgh] + [qtail], 0
        )
        kf = jnp.concatenate([k_ref[C * h : C * h + C]] + kgh + [ktail], 0)
        a1, a2, a3 = split3(qf)
        b1, b2, b3 = split3(kf)
        core = mm(
            jnp.concatenate([a1, a1, a2, a1, a2, a3], 0),
            jnp.concatenate([b1, b2, b1, b3, b2, b1], 0),
            TN,
        )
        gf = jnp.concatenate(
            [go_ref[C * h : C * h + C]] + [gg_ref[x, 8 * h : 8 * h + 8] for x in range(3)]
            + [jnp.zeros((8, IQ), F32)], 0
        )
        vf = jnp.concatenate(
            [v_ref[C * h : C * h + C]] + [vg_ref[x, 8 * h : 8 * h + 8] for x in range(3)]
            + [jnp.zeros((8, JK), F32)], 0
        )
        g1, g2 = split2(gf)
        v1, v2 = split2(vf)
        prod = mm(
            jnp.concatenate([g1, g1, g2], 0), jnp.concatenate([v1, v2, v1], 0), TN
        )

        def planes(base):
            return jnp.concatenate(
                [bp_ref[half, base * IQ : base * IQ + IQ, :] for half in range(2)], 1
            )

        logit = jnp.where(real, core + WL * planes(h), MASKED)
        prod = prod + planes(16 + h)
        peak = jnp.max(logit, axis=1, keepdims=True)
        e = jnp.exp(logit - peak)
        e_ref[h] = e
        p_ref[h] = prod
        total = jnp.sum(e, axis=1, keepdims=True)
        upper = jnp.sum(e * prod, axis=1, keepdims=True)
        g, r = divmod(h, 6)
        acc = jnp.where(lane == r, peak, stats[g])
        acc = jnp.where(lane == 8 + r, total, acc)
        stats[g] = jnp.where(lane == 16 + r, upper, acc)
    packed = jnp.concatenate(stats, 0).T[:24]
    for c in range(NCOL):
        st_ref[c] = packed


def grads_kernel(
    hw_ref, e_ref, p_ref, own_ref, all_ref, q_ref, k_ref, go_ref, qg_ref, kg_ref, vg_ref, gg_ref,
    pair_ref,
    d_ref, keep_ref, give_ref, qry_ref,
    da_ref, kp_ref, qp_ref, w_ref, hs_ref,
):
    if True:
        peaks = all_ref[:, 0:8]
        top = jnp.max(peaks, axis=0)
        grow = jnp.exp(peaks - top[None])
        total = jnp.sum(all_ref[:, 8:16] * grow, axis=0)
        upper = jnp.sum(all_ref[:, 16:24] * grow, axis=0)
        scale = jnp.exp(own_ref[0, 0:8] - top) / total
        delta = upper / total
        cols = jnp.concatenate([scale, delta, jnp.zeros((112, 128), F32)], 0).T
        w_ref[...] = jnp.zeros_like(w_ref)
        for half in range(2):
            da_ref[half, H * IQ : 16 * IQ, :] = jnp.zeros((4 * IQ, 128), F32)
            da_ref[half, 28 * IQ : 32 * IQ, :] = jnp.zeros((4 * IQ, 128), F32)
        row4q = lax.broadcasted_iota(jnp.int32, (4, IQ), 0)
        row4k = lax.broadcasted_iota(jnp.int32, (4, JK), 0)
        lane = lax.broadcasted_iota(jnp.int32, (8, 128), 1)
        hs = jnp.zeros((8, 128), F32)
        for h in range(H):
            g, r = divmod(h, 6)
            sc = cols[IQ * g : IQ * g + IQ, r : r + 1]
            dl = cols[IQ * g : IQ * g + IQ, 8 + r : 9 + r]
            a = e_ref[h] * sc
            d = a * (p_ref[h] - dl)
            for half in range(2):
                piece = slice(half * 128, half * 128 + 128)
                da_ref[half, h * IQ : h * IQ + IQ, :] = d[:, piece]
                da_ref[half, (16 + h) * IQ : (17 + h) * IQ, :] = a[:, piece]
            d1, d2 = split2(d)
            a1, a2 = split2(a)
            cfq = coef_row(hw_ref, h, IQ)
            cfk = coef_row(hw_ref, h, JK)
            qgh = [qg_ref[x, 4 * h : 4 * h + 4] for x in range(3)]
            kgh = [kg_ref[x, 4 * h : 4 * h + 4] for x in range(3)]
            qf = jnp.concatenate(
                [q_ref[C * h : C * h + C] * (WL * WS)] + qgh + [jnp.where(row4q == 0, 1.0, 0.0)], 0
            )
            kf = jnp.concatenate(
                [k_ref[C * h : C * h + C] * (WL * WS)] + kgh + [jnp.where(row4k == 0, 1.0, 0.0)], 0
            )
            gf = jnp.concatenate(
                [go_ref[C * h : C * h + C]] + [gg_ref[x, 8 * h : 8 * h + 8] for x in range(3)], 0
            )
            vf = jnp.concatenate([vg_ref[x, 8 * h : 8 * h + 8] for x in range(3)], 0)

            def three(left, n, right1, right2, dims):
                hi, lo = split2(left)
                both = mm(jnp.concatenate([hi, lo], 0), right1, dims)
                return both[:n] + both[n:] + mm(hi, right2, dims)

            kside = three(qf, 32, d1, d2, NN)
            vside = three(gf, 40, a1, a2, NN)
            qside = three(kf, 32, d1, d2, NT)
            oside = three(vf, 24, a1, a2, NT)
            csum, rsum = kside[28:29], qside[28:29]
            kp_ref[KEY0 + C * h : KEY0 + C * h + C] = kside[0:16]
            kp_ref[VAL0 + C * h : VAL0 + C * h + C] = vside[0:16]
            qp_ref[QRY0 + C * h : QRY0 + C * h + C] = qside[0:16]
            tk = jnp.zeros((1, JK), F32)
            tq = jnp.zeros((1, IQ), F32)
            for x in range(3):
                kq = kside[16 + 4 * x : 20 + 4 * x]
                qk = qside[16 + 4 * x : 20 + 4 * x]
                kp_ref[KPT0 + 48 * x + 4 * h : KPT0 + 48 * x + 4 * h + 4] = (2.0 * cfk) * (
                    kq - kgh[x] * csum
                )
                qp_ref[QPT0 + 48 * x + 4 * h : QPT0 + 48 * x + 4 * h + 4] = (-2.0 * cfq) * (
                    qgh[x] * rsum - qk
                )
                kp_ref[VPT0 + 96 * x + 8 * h : VPT0 + 96 * x + 8 * h + 8] = vside[
                    16 + 8 * x : 24 + 8 * x
                ]
                qp_ref[OPT0 + 96 * x + 8 * h : OPT0 + 96 * x + 8 * h + 8] = oside[
                    8 * x : 8 * x + 8
                ]
                tk = tk + jnp.sum(kgh[x] * (kgh[x] * csum - 2.0 * kq), axis=0, keepdims=True)
                tq = tq + jnp.sum(qgh[x] * qgh[x], axis=0, keepdims=True)
            part = jnp.sum(tk, axis=1, keepdims=True) + jnp.sum(tq * rsum, axis=1, keepdims=True)
            hs = jnp.where(lane == 48 + h, part, hs)
        hs_ref[...] = hs

    @pl.loop(0, IQ // PB)
    def _(b):
        dlogs = []
        for n in range(PB):
            at = b * PB + n
            rows = jnp.concatenate(
                [da_ref[half, pl.ds(at, 32, stride=IQ), :] for half in range(2)], 1
            ).astype(BF16)
            d_ref[at] = rows
            dlogs.append(rows[:16])
        w_ref[...] += mm(
            jnp.concatenate(dlogs, 1), pair_ref[pl.ds(b * PB, PB)].reshape(PB * JK, CZ), NN
        )

    if True:
        core = lax.axis_index("row_2")
        w0 = w_ref[0:8]
        w1 = w_ref[8:16]
        lane = lax.broadcasted_iota(jnp.int32, (8, 128), 1)
        sub = lax.broadcasted_iota(jnp.int32, (8, 128), 0)
        fold = jnp.where(sub < 4, pltpu.roll(w1, 64, 1), pltpu.roll(w1, 4, 0))
        extra = jnp.where(lane < 64, hs_ref[...], fold)
        keys = [
            [kp_ref[128 * t : 128 * t + 128, 128 * b : 128 * b + 128].T for t in range(7)]
            for b in range(2)
        ]
        def tile(j, t):
            b, r = divmod(j, 16)
            if t == 7:
                return w0
            piece = keys[b][t][8 * r : 8 * r + 8]
            return jnp.where(lane < 48, piece, extra) if t == 6 else piece

        first = core == 0
        for zone in range(NCHIP):
            for t in range(8):
                even, odd = tile(2 * zone, t), tile(2 * zone + 1, t)
                keep_ref[zone, :, 128 * t : 128 * t + 128] = jnp.where(first, even, odd)
                give_ref[zone, :, 128 * t : 128 * t + 128] = jnp.where(first, odd, even)
        for t in range(5):
            block = qp_ref[128 * t : 128 * t + 128]
            turned = jnp.concatenate([block, jnp.zeros((128, 64), F32)], 1).T
            for c in range(NCOL):
                qry_ref[c, :, 128 * t : 128 * t + 128] = turned[8 * c : 8 * c + 8]


def pair_kernel(d_ref, gp_ref, bw_ref, out_ref, gs_ref):
    wide = jnp.concatenate([bw_ref[...].astype(F32) * WL, jnp.zeros((4, CZ), F32)], 0)
    hi, lo = split2(wide)
    gs_ref[...] = gp_ref[...].astype(F32).reshape(H * QB, CZ)
    pad = jnp.zeros((4, CZ), F32)
    for n in range(QB):
        rows = d_ref[n]
        lhs = jnp.concatenate([rows[:16], rows], 0)
        part = jnp.concatenate([gs_ref[pl.ds(n, H, stride=QB), :], pad], 0).astype(BF16)
        rhs = jnp.concatenate([hi, lo, part], 0)
        out_ref[n] = mm(lhs, rhs, TN).astype(BF16)


def mid_kernel(parts_ref, qry_ref, keys_ref, send_ref):
    total = jnp.sum(parts_ref[...], axis=0)
    keys_ref[...] = total
    for c in range(NCOL):
        send_ref[c, :, 0:QW] = qry_ref[c]
        send_ref[c, :, QW : QW + 128] = total[:, 896:1024]
        send_ref[c, :, QW + 128 : QW + 256] = total[:, 768:896]


def own_lanes(ref, offset, rows):
    base = pl.multiple_of(lax.div(offset, 128) * 128, 128)
    off = lax.rem(offset, 128)
    return [lanes_at(ref[y, :, pl.ds(base, 128)], off, 128) for y in range(3)]


def sum1(x):
    return jnp.sum(x, axis=1, keepdims=True)


def frame_cols(rot_ref, tr_ref, at):
    base = pl.multiple_of(lax.div(at, 128) * 128, 128)
    rows = [rot_ref[x, :, pl.ds(base, 128)] for x in range(3)] + [tr_ref[:, pl.ds(base, 128)]]
    block = jnp.concatenate(rows + [jnp.zeros((116, 128), F32)], 0)
    return lanes_at(block, lax.rem(at, 128), 128).T[:8]


def tall(rows):
    x = jnp.concatenate(rows, 0)
    full = -(-x.shape[0] // 128) * 128
    if full > x.shape[0]:
        x = jnp.concatenate([x, jnp.zeros((full - x.shape[0], 128), F32)], 0)
    return jnp.concatenate([x[t : t + 128].T[:8] for t in range(0, full, 128)], 1)


def frame_out(ref, table):
    lane = lax.broadcasted_iota(jnp.int32, (8, 128), 1)
    block = jnp.zeros((8, 128), F32)
    for (x, y), column in table.items():
        block = jnp.where(lane == 4 * x + y, column, block)
    block = jnp.concatenate([block, jnp.zeros((120, 128), F32)], 0).T
    for x in range(3):
        ref[x] = block[4 * x : 4 * x + 4, :8]


def key_kernel(
    keys_ref, kp_ref, vp_ref, qp_ref, rot_ref, tr_ref,
    kgr_ref, vgr_ref, kpg_ref, vpg_ref, kfr_ref, qpo_ref, fr_ref,
):
    flat = keys_ref[...]
    kgr_ref[...] = flat[:, KEY0:VAL0]
    vgr_ref[...] = flat[:, VAL0:KPT0]
    dk = [flat[:, KPT0 + 48 * x : KPT0 + 48 * x + 48] for x in range(3)]
    dv = [flat[:, VPT0 + 96 * x : VPT0 + 96 * x + 96] for x in range(3)]
    offset = row_index() * 8
    local = tall(own_lanes(kp_ref, offset, 48) + own_lanes(vp_ref, offset, 96))
    kp = [local[:, 48 * y : 48 * y + 48] for y in range(3)]
    vp = [local[:, 144 + 96 * y : 240 + 96 * y] for y in range(3)]
    fr = frame_cols(rot_ref, tr_ref, col_index() * JK + offset)
    rot = [[fr[:, 3 * x + y : 3 * x + y + 1] for y in range(3)] for x in range(3)]
    table = {}
    for y in range(3):
        kpg_ref[y] = rot[0][y] * dk[0] + rot[1][y] * dk[1] + rot[2][y] * dk[2]
        vpg_ref[y] = rot[0][y] * dv[0] + rot[1][y] * dv[1] + rot[2][y] * dv[2]
    for x in range(3):
        for y in range(3):
            table[x, y] = sum1(dk[x] * kp[y]) + sum1(dv[x] * vp[y])
        table[x, 3] = sum1(dk[x]) + sum1(dv[x])
    frame_out(kfr_ref, table)
    off = col_index() * 8
    qpo_ref[...] = tall(
        [lanes_at(jnp.concatenate([qp_ref[y], qp_ref[y]], 1), off, 128) for y in range(3)]
    )
    fr_ref[...] = frame_cols(rot_ref, tr_ref, row_index() * IQ + off)


def last_kernel(
    hw_ref, parts_ref, qpo_ref, fr_ref, gpt_ref, qgr_ref, qpg_ref, qfr_ref, wg_ref, hg_ref,
):
    total = jnp.sum(parts_ref[...], axis=0)
    qgr_ref[...] = total[:, QRY0:QPT0]
    dq = [total[:, QPT0 + 48 * x : QPT0 + 48 * x + 48] for x in range(3)]
    opt = [total[:, OPT0 + 96 * x : OPT0 + 96 * x + 96] for x in range(3)]
    fr = fr_ref[...]
    rot = [[fr[:, 3 * x + y : 3 * x + y + 1] for y in range(3)] for x in range(3)]
    at = pl.multiple_of(col_index() * 8, 8)
    gpt = [gpt_ref[y, pl.ds(at, 8), :] for y in range(3)]
    qp = [qpo_ref[:, 48 * y : 48 * y + 48] for y in range(3)]
    gsum = [sum1(g) for g in gpt]
    for y in range(3):
        qpg_ref[y] = rot[0][y] * dq[0] + rot[1][y] * dq[1] + rot[2][y] * dq[2]
    table = {}
    for x in range(3):
        away = opt[x] - fr[:, 9 + x : 10 + x]
        for y in range(3):
            table[x, y] = sum1(dq[x] * qp[y]) + sum1(away * gpt[y])
        back = rot[x][0] * gsum[0] + rot[x][1] * gsum[1] + rot[x][2] * gsum[2]
        table[x, 3] = sum1(dq[x]) - back
    frame_out(qfr_ref, table)
    w0 = total[:, QW : QW + 128]
    extra = total[:, QW + 128 : QW + 256]
    lane4 = lax.broadcasted_iota(jnp.int32, (4, 128), 1)
    wg_ref[0:8] = WL * w0
    wg_ref[8:12] = WL * jnp.where(lane4 < 64, pltpu.roll(extra, 64, 1)[0:4], extra[4:8])
    lane = lax.broadcasted_iota(jnp.int32, (1, 128), 1)
    raw = jnp.zeros((1, 128), F32)
    for h in range(H):
        raw = jnp.where(lane == h, hw_ref[h], raw)
    sig = 1.0 / (1.0 + jnp.exp(-raw))
    sums = pltpu.roll(extra, 128 - 48, 1)[0:1]
    hg_ref[...] = ((-0.5 * WL * WC) * sums * sig)[:, :H]


def struct(shape, dtype=F32):
    return jax.ShapeDtypeStruct(shape, dtype)


def cost(us, nbytes):
    return pl.CostEstimate(flops=int(us * 4e6), bytes_accessed=int(nbytes), transcendentals=0)


def per_device(
    pair_rep, bias_weight, head_weight, queries, key_vectors, values, query_points, key_points,
    value_points, rotations, translations, residue_count, grad_output, grad_points, grad_pair,
):
    steps = IQ // QB
    pair_spec = pl.BlockSpec((QB, JK, CZ), lambda i: (i, 0, 0))
    gp_spec = pl.BlockSpec((H, QB, CZ), lambda i: (0, i, 0))
    gp_heads = grad_pair.transpose(1, 0, 2)
    bw_heads = bias_weight.T
    gpt_rows = grad_points.transpose(0, 2, 1)
    e, p, st, q, go, qg, kg, vg, gg, pair, keys = pl.pallas_call(
        logits_kernel,
        name="logits",
        in_specs=[SMEM_SPEC] + [HBM_SPEC] * 14,
        out_specs=[VMEM_SPEC] * 11,
        out_shape=[
            struct((H, IQ, JK)), struct((H, IQ, JK)), struct((NCOL, 24, 128)),
            struct((H * C, IQ)), struct((H * C, IQ)),
            struct((3, 48, IQ)), struct((3, 48, JK)), struct((3, 96, JK)), struct((3, 96, IQ)),
            struct((IQ, JK, CZ), BF16), struct((H * C, JK)),
        ],
        scratch_shapes=[
            pltpu.VMEM((2, 32 * IQ, 128), F32), pltpu.VMEM((H * IQ, CZ), F32),
            pltpu.SMEM((H,), F32), pltpu.VMEM((H, IQ, CZ), BF16), pltpu.VMEM((H, CZ), BF16),
            pltpu.VMEM((IQ, H * C), F32), pltpu.VMEM((H * C, JK), F32),
            pltpu.VMEM((3, 48, IQ), F32), pltpu.VMEM((3, 48, JK), F32),
            pltpu.VMEM((3, 96, JK), F32), pltpu.VMEM((3, 3, 2048), F32),
            pltpu.VMEM((3, 2048), F32), pltpu.VMEM((IQ, H * C), F32),
            pltpu.VMEM((3, IQ, 96), F32), pltpu.SemaphoreType.DMA((13,)),
            pltpu.SemaphoreType.DMA((IQ // PB,)),
        ],
        compiler_params=pltpu.CompilerParams(vmem_limit_bytes=LIMIT),
        cost_estimate=cost(5, 6e6),
    )(
        residue_count,
        *(
            pltpu.with_memory_space_constraint(x, pltpu.HBM)
            for x in (
                head_weight, pair_rep, gp_heads, bw_heads, queries.T, key_vectors, values,
                query_points, key_points, value_points, rotations, translations, grad_output.T,
                gpt_rows,
            )
        ),
    )
    everyone = lax.all_to_all(st, COL, 0, 0, tiled=True)
    d, keep, give, qry = pl.pallas_call(
        grads_kernel,
        name="grads",
        in_specs=[SMEM_SPEC] + [VMEM_SPEC] * 12,
        out_specs=[VMEM_SPEC] * 4,
        out_shape=[
            struct((IQ, 32, JK), BF16), struct((NCHIP, 8, KW)), struct((NCHIP, 8, KW)),
            struct((NCOL, 8, QW)),
        ],
        scratch_shapes=[
            pltpu.VMEM((2, 32 * IQ, 128), F32), pltpu.VMEM((896, JK), F32),
            pltpu.VMEM((QW, IQ), F32), pltpu.VMEM((16, CZ), F32), pltpu.VMEM((8, 128), F32),
        ],
        compiler_params=pltpu.CompilerParams(vmem_limit_bytes=LIMIT),
        cost_estimate=cost(5, 8e6),
    )(head_weight, e, p, st, everyone, q, keys, go, qg, kg, vg, gg, pair)
    swapped = lax.ppermute(give, "row_2", [(0, 1), (1, 0)])
    parts = lax.all_to_all(keep + swapped, CHIPS, 0, 0, tiled=True)
    pair_grad = pl.pallas_call(
        pair_kernel,
        name="pair",
        grid=(steps,),
        in_specs=[pl.BlockSpec((QB, 32, JK), lambda i: (i, 0, 0)), gp_spec, VMEM_SPEC],
        out_specs=pair_spec,
        out_shape=struct((IQ, JK, CZ), BF16),
        scratch_shapes=[pltpu.VMEM((H * QB, CZ), F32)],
        compiler_params=pltpu.CompilerParams(vmem_limit_bytes=LIMIT),
        cost_estimate=cost(6, 6e6),
    )(d, gp_heads, bw_heads)
    parts, pair_grad = lax.optimization_barrier((parts, pair_grad))
    keysum, send = pl.pallas_call(
        mid_kernel,
        name="mid",
        in_specs=[VMEM_SPEC] * 2,
        out_specs=[VMEM_SPEC] * 2,
        out_shape=[struct((8, KW)), struct((NCOL, 8, QW + 256))],
        compiler_params=pltpu.CompilerParams(vmem_limit_bytes=LIMIT),
        cost_estimate=cost(1, 1e6),
    )(parts, qry)
    last = lax.all_to_all(send, COL, 0, 0, tiled=True)
    key_grad, value_grad, key_point_grad, value_point_grad, key_frame_grad, qpo, fr = (
        pl.pallas_call(
            key_kernel,
            name="keyout",
            in_specs=[VMEM_SPEC] * 6,
            out_specs=[VMEM_SPEC] * 7,
            out_shape=[
                struct((8, 192)), struct((8, 192)), struct((3, 8, 48)), struct((3, 8, 96)),
                struct((3, 4, 8)), struct((8, 256)), struct((8, 128)),
            ],
            compiler_params=pltpu.CompilerParams(vmem_limit_bytes=LIMIT),
        cost_estimate=cost(2, 1e6),
        )(keysum, key_points, value_points, query_points, rotations, translations)
    )
    query_grad, query_point_grad, query_frame_grad, weight_grad, head_grad = pl.pallas_call(
        last_kernel,
        name="last",
        in_specs=[SMEM_SPEC] + [VMEM_SPEC] * 4,
        out_specs=[VMEM_SPEC] * 5,
        out_shape=[
            struct((8, 192)), struct((3, 8, 48)), struct((3, 4, 8)), struct((H, CZ)),
            struct((1, H)),
        ],
        compiler_params=pltpu.CompilerParams(vmem_limit_bytes=LIMIT),
        cost_estimate=cost(2, 1e6),
    )(head_weight, last, qpo, fr, gpt_rows)
    return (
        pair_grad, query_grad.T, query_point_grad.transpose(0, 2, 1), query_frame_grad, key_grad.T,
        value_grad.T, key_point_grad.transpose(0, 2, 1), value_point_grad.transpose(0, 2, 1),
        key_frame_grad, weight_grad.T, head_grad.reshape(H),
    )


def solution(mesh):
    finer = Mesh(mesh.devices.reshape(4, 4, 2, 4, 2), ROW_COL)
    in_specs = (
        P(ROW, COL, None), P(), P(), P(None, ROW), P(None, COL), P(None, COL),
        P(None, None, ROW), P(None, None, COL), P(None, None, COL), P(), P(), P(),
        P(None, ROW), P(None, None, ROW), P(ROW, None, None),
    )
    out_specs = (
        P(ROW, COL, None), P(None, ROW_COL), P(None, None, ROW_COL), P(None, None, ROW_COL),
        P(None, COL_ROW), P(None, COL_ROW), P(None, None, COL_ROW), P(None, None, COL_ROW),
        P(None, None, COL_ROW), P(), P(),
    )
    return jax.shard_map(
        per_device, mesh=finer, in_specs=in_specs, out_specs=out_specs, check_vma=False
    )
```

```python
import functools
import math

import jax
import jax.numpy as jnp
from jax import lax
from jax.experimental import pallas as pl
from jax.experimental.pallas import tpu as pltpu
from jax.sharding import Mesh
from jax.sharding import PartitionSpec as P

ROW = ("row_0", "row_1", "row_2")
COL = ("col_0", "col_1")
ROW_COL = ROW + COL
COL_ROW = COL + ROW
CHIPS = ("row_0", "row_1")

H, C, PQ, PV, CZ = 12, 16, 4, 8, 128
IQ, JK = 64, 256
NCOL, NROW, NCHIP = 8, 32, 16
WL = math.sqrt(1.0 / 3.0)
WC = math.sqrt(2.0 / (9.0 * PQ))
WS = 1.0 / math.sqrt(C)
MASKED = -1000000000.0

KEY0, VAL0, KPT0, VPT0, KEND = 0, 192, 384, 528, 816
QRY0, QPT0, OPT0, QEND = 0, 192, 336, 624
KW, QW = 1024, 640
LIMIT = 20 << 20
QB = 16
PB = 8

F32, BF16 = jnp.float32, jnp.bfloat16
VMEM_SPEC = pl.BlockSpec(memory_space=pltpu.VMEM)
SMEM_SPEC = pl.BlockSpec(memory_space=pltpu.SMEM)
TN = (((0,), (0,)), ((), ()))
NT = (((1,), (1,)), ((), ()))
NN = (((1,), (0,)), ((), ()))


def mm(a, b, dims):
    return lax.dot_general(a, b, dims, preferred_element_type=F32)


def split2(x):
    hi = x.astype(BF16)
    return hi, (x - hi.astype(F32)).astype(BF16)


def split3(x):
    hi = x.astype(BF16)
    rest = x - hi.astype(F32)
    mid = rest.astype(BF16)
    return hi, mid, (rest - mid.astype(F32)).astype(BF16)


def row_index():
    return (lax.axis_index("row_0") * 4 + lax.axis_index("row_1")) * 2 + lax.axis_index("row_2")


def col_index():
    return lax.axis_index("col_0") * 2 + lax.axis_index("col_1")


def soft(hw_ref, h, lanes):
    w = jnp.full((1, lanes), hw_ref[h], F32)
    return jnp.maximum(w, 0.0) + jnp.log1p(jnp.exp(-jnp.abs(w)))


def coef_row(hw_ref, h, lanes):
    return (0.5 * WL * WC) * soft(hw_ref, h, lanes)


def rotate(rot, shift, local):
    out = []
    for x in range(3):
        g = rot[x][0] * local[0] + rot[x][1] * local[1] + rot[x][2] * local[2]
        out.append(g if shift is None else g + shift[x])
    return out


def flip(x):
    rows, lanes = x.shape
    full = -(-lanes // 128) * 128
    if full > lanes:
        x = jnp.concatenate([x, jnp.zeros((rows, full - lanes), F32)], 1)
    x = jnp.concatenate([x, jnp.zeros((128 - rows, full), F32)], 0)
    return jnp.concatenate(
        [x[:, t : t + 128].T for t in range(0, full, 128)], 0
    )[:, :rows]


def col_frames(rot_ref, tr_ref):
    start = pl.multiple_of(col_index() * JK, JK)
    rot = [[rot_ref[x, y : y + 1, pl.ds(start, JK)] for y in range(3)] for x in range(3)]
    tr = [tr_ref[x : x + 1, pl.ds(start, JK)] for x in range(3)]
    return rot, tr


def lanes_at(block, offset, count):
    return pltpu.roll(block, lax.rem(128 - offset, 128), block.ndim - 1)[..., :count]


def row_frames(rot_ref, tr_ref, offset, count):
    at = row_index() * IQ + offset
    base = pl.multiple_of(lax.div(at, 128) * 128, 128)
    off = lax.rem(at, 128)
    rot = []
    for x in range(3):
        block = lanes_at(
            jnp.concatenate([rot_ref[x, :, pl.ds(base, 128)], jnp.zeros((5, 128), F32)], 0),
            off,
            count,
        )
        rot.append([block[y : y + 1] for y in range(3)])
    block = lanes_at(
        jnp.concatenate([tr_ref[:, pl.ds(base, 128)], jnp.zeros((5, 128), F32)], 0), off, count
    )
    return rot, [block[x : x + 1] for x in range(3)]


HBM_SPEC = pl.BlockSpec(memory_space=pltpu.HBM)


def logits_kernel(
    rc_ref, hw_hbm, pair_hbm, gp_hbm, bw_hbm, qt_hbm, k_hbm, v_hbm, qp_hbm, kp_hbm, vp_hbm,
    rot_hbm, tr_hbm, got_hbm, gpt_hbm,
    e_ref, p_ref, st_ref, q_ref, go_ref, qg_ref, kg_ref, vg_ref, gg_ref, pair_ref, k_ref,
    bp_ref, gs_ref, hw_ref, gp_ref, bw_ref, qt_ref, v_ref, qp_ref, kp_ref, vp_ref, rot_ref,
    tr_ref, got_ref, gpt_ref, sems, pair_sems,
):
    def pair_copy(b):
        part = pl.ds(b * PB, PB)
        return pltpu.make_async_copy(pair_hbm.at[part], pair_ref.at[part], pair_sems.at[b])

    moves = [
        (gp_hbm, gp_ref), (bw_hbm, bw_ref), (k_hbm, k_ref), (v_hbm, v_ref), (qt_hbm, qt_ref),
        (got_hbm, got_ref), (qp_hbm, qp_ref), (kp_hbm, kp_ref), (vp_hbm, vp_ref),
        (gpt_hbm, gpt_ref), (rot_hbm, rot_ref), (tr_hbm, tr_ref), (hw_hbm, hw_ref),
    ]
    copies = [pltpu.make_async_copy(a, b, sems.at[n]) for n, (a, b) in enumerate(moves)]
    for c in copies[:2]:
        c.start()
    pair_copy(0).start()
    for c in copies[2:]:
        c.start()
    for b in range(1, IQ // PB):
        pair_copy(b).start()
    for c in copies[:2]:
        c.wait()
    wt = jnp.concatenate([bw_ref[...].astype(F32), jnp.zeros((4, CZ), F32)], 0)
    gs_ref[...] = gp_ref[...].astype(F32).reshape(H * IQ, CZ)

    @pl.loop(0, IQ // PB)
    def _(b):
        pair_copy(b).wait()
        for n in range(PB):
            at = b * PB + n
            lhs = jnp.concatenate([wt, gs_ref[pl.ds(at, H, stride=IQ), :]], 0).astype(BF16)
            res = mm(lhs, pair_ref[at], NT)
            for half in range(2):
                bp_ref[half, pl.ds(at, 16 + H, stride=IQ), :] = res[
                    :, half * 128 : half * 128 + 128
                ]

    for c in copies[2:]:
        c.wait()
    crot, ctr = col_frames(rot_ref, tr_ref)
    rrot, rtr = row_frames(rot_ref, tr_ref, 0, IQ)
    kg = rotate(crot, ctr, [kp_ref[y] for y in range(3)])
    vg = rotate(crot, ctr, [vp_ref[y] for y in range(3)])
    qg = rotate(rrot, rtr, [qp_ref[y] for y in range(3)])
    gg = rotate(rrot, None, [flip(gpt_ref[y])[: H * PV] for y in range(3)])
    q_ref[...] = flip(qt_ref[...])[: H * C]
    go_ref[...] = flip(got_ref[...])[: H * C]
    for x in range(3):
        kg_ref[x], vg_ref[x], qg_ref[x], gg_ref[x] = kg[x], vg[x], qg[x], gg[x]
    real = (
        lax.broadcasted_iota(jnp.int32, (IQ, JK), 1) + col_index() * JK < rc_ref[0]
    )
    lane = lax.broadcasted_iota(jnp.int32, (IQ, 128), 1)
    stats = [jnp.zeros((IQ, 128), F32), jnp.zeros((IQ, 128), F32)]
    row4q = lax.broadcasted_iota(jnp.int32, (4, IQ), 0)
    row4k = lax.broadcasted_iota(jnp.int32, (4, JK), 0)
    for h in range(H):
        cf = coef_row(hw_ref, h, IQ)
        qgh = [qg_ref[x, 4 * h : 4 * h + 4] for x in range(3)]
        kgh = [kg_ref[x, 4 * h : 4 * h + 4] for x in range(3)]
        qn = sum(jnp.sum(t * t, axis=0, keepdims=True) for t in qgh)
        kn = sum(jnp.sum(t * t, axis=0, keepdims=True) for t in kgh)
        qtail = jnp.where(row4q == 0, -cf, jnp.where(row4q == 1, -cf * qn, 0.0))
        ktail = jnp.where(row4k == 0, kn, jnp.where(row4k == 1, 1.0, 0.0))
        qf = jnp.concatenate(
            [q_ref[C * h : C * h + C] * (WL * WS)] + [2.0 * cf * t for t in qgh] + [qtail], 0
        )
        kf = jnp.concatenate([k_ref[C * h : C * h + C]] + kgh + [ktail], 0)
        a1, a2, a3 = split3(qf)
        b1, b2, b3 = split3(kf)
        core = mm(
            jnp.concatenate([a1, a1, a2, a1, a2, a3], 0),
            jnp.concatenate([b1, b2, b1, b3, b2, b1], 0),
            TN,
        )
        gf = jnp.concatenate(
            [go_ref[C * h : C * h + C]] + [gg_ref[x, 8 * h : 8 * h + 8] for x in range(3)]
            + [jnp.zeros((8, IQ), F32)], 0
        )
        vf = jnp.concatenate(
            [v_ref[C * h : C * h + C]] + [vg_ref[x, 8 * h : 8 * h + 8] for x in range(3)]
            + [jnp.zeros((8, JK), F32)], 0
        )
        g1, g2 = split2(gf)
        v1, v2 = split2(vf)
        prod = mm(
            jnp.concatenate([g1, g1, g2], 0), jnp.concatenate([v1, v2, v1], 0), TN
        )

        def planes(base):
            return jnp.concatenate(
                [bp_ref[half, base * IQ : base * IQ + IQ, :] for half in range(2)], 1
            )

        logit = jnp.where(real, core + WL * planes(h), MASKED)
        prod = prod + planes(16 + h)
        peak = jnp.max(logit, axis=1, keepdims=True)
        e = jnp.exp(logit - peak)
        e_ref[h] = e
        p_ref[h] = prod
        total = jnp.sum(e, axis=1, keepdims=True)
        upper = jnp.sum(e * prod, axis=1, keepdims=True)
        g, r = divmod(h, 6)
        acc = jnp.where(lane == r, peak, stats[g])
        acc = jnp.where(lane == 8 + r, total, acc)
        stats[g] = jnp.where(lane == 16 + r, upper, acc)
    packed = jnp.concatenate(stats, 0).T[:24]
    for c in range(NCOL):
        st_ref[c] = packed


def grads_kernel(
    hw_ref, e_ref, p_ref, own_ref, all_ref, q_ref, k_ref, go_ref, qg_ref, kg_ref, vg_ref, gg_ref,
    pair_ref,
    d_ref, keep_ref, give_ref, qry_ref,
    da_ref, kp_ref, qp_ref, w_ref, hs_ref,
):
    if True:
        peaks = all_ref[:, 0:8]
        top = jnp.max(peaks, axis=0)
        grow = jnp.exp(peaks - top[None])
        total = jnp.sum(all_ref[:, 8:16] * grow, axis=0)
        upper = jnp.sum(all_ref[:, 16:24] * grow, axis=0)
        scale = jnp.exp(own_ref[0, 0:8] - top) / total
        delta = upper / total
        cols = jnp.concatenate([scale, delta, jnp.zeros((112, 128), F32)], 0).T
        w_ref[...] = jnp.zeros_like(w_ref)
        for half in range(2):
            da_ref[half, H * IQ : 16 * IQ, :] = jnp.zeros((4 * IQ, 128), F32)
            da_ref[half, 28 * IQ : 32 * IQ, :] = jnp.zeros((4 * IQ, 128), F32)
        row4q = lax.broadcasted_iota(jnp.int32, (4, IQ), 0)
        row4k = lax.broadcasted_iota(jnp.int32, (4, JK), 0)
        lane = lax.broadcasted_iota(jnp.int32, (8, 128), 1)
        hs = jnp.zeros((8, 128), F32)
        for h in range(H):
            g, r = divmod(h, 6)
            sc = cols[IQ * g : IQ * g + IQ, r : r + 1]
            dl = cols[IQ * g : IQ * g + IQ, 8 + r : 9 + r]
            a = e_ref[h] * sc
            d = a * (p_ref[h] - dl)
            for half in range(2):
                piece = slice(half * 128, half * 128 + 128)
                da_ref[half, h * IQ : h * IQ + IQ, :] = d[:, piece]
                da_ref[half, (16 + h) * IQ : (17 + h) * IQ, :] = a[:, piece]
            d1, d2 = split2(d)
            a1, a2 = split2(a)
            cfq = coef_row(hw_ref, h, IQ)
            cfk = coef_row(hw_ref, h, JK)
            qgh = [qg_ref[x, 4 * h : 4 * h + 4] for x in range(3)]
            kgh = [kg_ref[x, 4 * h : 4 * h + 4] for x in range(3)]
            qf = jnp.concatenate(
                [q_ref[C * h : C * h + C] * (WL * WS)] + qgh + [jnp.where(row4q == 0, 1.0, 0.0)], 0
            )
            kf = jnp.concatenate(
                [k_ref[C * h : C * h + C] * (WL * WS)] + kgh + [jnp.where(row4k == 0, 1.0, 0.0)], 0
            )
            gf = jnp.concatenate(
                [go_ref[C * h : C * h + C]] + [gg_ref[x, 8 * h : 8 * h + 8] for x in range(3)], 0
            )
            vf = jnp.concatenate([vg_ref[x, 8 * h : 8 * h + 8] for x in range(3)], 0)

            def three(left, n, right1, right2, dims):
                hi, lo = split2(left)
                both = mm(jnp.concatenate([hi, lo], 0), right1, dims)
                return both[:n] + both[n:] + mm(hi, right2, dims)

            kside = three(qf, 32, d1, d2, NN)
            vside = three(gf, 40, a1, a2, NN)
            qside = three(kf, 32, d1, d2, NT)
            oside = three(vf, 24, a1, a2, NT)
            csum, rsum = kside[28:29], qside[28:29]
            kp_ref[KEY0 + C * h : KEY0 + C * h + C] = kside[0:16]
            kp_ref[VAL0 + C * h : VAL0 + C * h + C] = vside[0:16]
            qp_ref[QRY0 + C * h : QRY0 + C * h + C] = qside[0:16]
            tk = jnp.zeros((1, JK), F32)
            tq = jnp.zeros((1, IQ), F32)
            for x in range(3):
                kq = kside[16 + 4 * x : 20 + 4 * x]
                qk = qside[16 + 4 * x : 20 + 4 * x]
                kp_ref[KPT0 + 48 * x + 4 * h : KPT0 + 48 * x + 4 * h + 4] = (2.0 * cfk) * (
                    kq - kgh[x] * csum
                )
                qp_ref[QPT0 + 48 * x + 4 * h : QPT0 + 48 * x + 4 * h + 4] = (-2.0 * cfq) * (
                    qgh[x] * rsum - qk
                )
                kp_ref[VPT0 + 96 * x + 8 * h : VPT0 + 96 * x + 8 * h + 8] = vside[
                    16 + 8 * x : 24 + 8 * x
                ]
                qp_ref[OPT0 + 96 * x + 8 * h : OPT0 + 96 * x + 8 * h + 8] = oside[
                    8 * x : 8 * x + 8
                ]
                tk = tk + jnp.sum(kgh[x] * (kgh[x] * csum - 2.0 * kq), axis=0, keepdims=True)
                tq = tq + jnp.sum(qgh[x] * qgh[x], axis=0, keepdims=True)
            part = jnp.sum(tk, axis=1, keepdims=True) + jnp.sum(tq * rsum, axis=1, keepdims=True)
            hs = jnp.where(lane == 48 + h, part, hs)
        hs_ref[...] = hs

    @pl.loop(0, IQ // PB)
    def _(b):
        dlogs = []
        for n in range(PB):
            at = b * PB + n
            rows = jnp.concatenate(
                [da_ref[half, pl.ds(at, 32, stride=IQ), :] for half in range(2)], 1
            ).astype(BF16)
            d_ref[at] = rows
            dlogs.append(rows[:16])
        w_ref[...] += mm(
            jnp.concatenate(dlogs, 1), pair_ref[pl.ds(b * PB, PB)].reshape(PB * JK, CZ), NN
        )

    if True:
        core = lax.axis_index("row_2")
        w0 = w_ref[0:8]
        w1 = w_ref[8:16]
        lane = lax.broadcasted_iota(jnp.int32, (8, 128), 1)
        sub = lax.broadcasted_iota(jnp.int32, (8, 128), 0)
        fold = jnp.where(sub < 4, pltpu.roll(w1, 64, 1), pltpu.roll(w1, 4, 0))
        extra = jnp.where(lane < 64, hs_ref[...], fold)
        keys = [
            [kp_ref[128 * t : 128 * t + 128, 128 * b : 128 * b + 128].T for t in range(7)]
            for b in range(2)
        ]
        def tile(j, t):
            b, r = divmod(j, 16)
            if t == 7:
                return w0
            piece = keys[b][t][8 * r : 8 * r + 8]
            return jnp.where(lane < 48, piece, extra) if t == 6 else piece

        first = core == 0
        my_z, my_y = lax.axis_index("row_0"), lax.axis_index("row_1")
        for zone in range(NCHIP):
            z, y = divmod(zone, 4)
            dz = lax.rem(z + 4 - my_z, 4)
            dy = lax.rem(y + 4 - my_y, 4)
            for t in range(8):
                even, odd = tile(2 * zone, t), tile(2 * zone + 1, t)
                keep_ref[dy, dz, :, 128 * t : 128 * t + 128] = jnp.where(first, even, odd)
                give_ref[dy, dz, :, 128 * t : 128 * t + 128] = jnp.where(first, odd, even)
        for t in range(5):
            block = qp_ref[128 * t : 128 * t + 128]
            turned = jnp.concatenate([block, jnp.zeros((128, 64), F32)], 1).T
            for c in range(NCOL):
                qry_ref[c, :, 128 * t : 128 * t + 128] = turned[8 * c : 8 * c + 8]


def pair_kernel(d_ref, gp_ref, bw_ref, out_ref, gs_ref):
    wide = jnp.concatenate([bw_ref[...].astype(F32) * WL, jnp.zeros((4, CZ), F32)], 0)
    hi, lo = split2(wide)
    gs_ref[...] = gp_ref[...].astype(F32).reshape(H * QB, CZ)
    pad = jnp.zeros((4, CZ), F32)
    for n in range(QB):
        rows = d_ref[n]
        lhs = jnp.concatenate([rows[:16], rows], 0)
        part = jnp.concatenate([gs_ref[pl.ds(n, H, stride=QB), :], pad], 0).astype(BF16)
        rhs = jnp.concatenate([hi, lo, part], 0)
        out_ref[n] = mm(lhs, rhs, TN).astype(BF16)


def mid_kernel(a_ref, b_ref, c_ref, d_ref, qry_ref, keys_ref, send_ref):
    total = (a_ref[...] + b_ref[...]) + (c_ref[...] + d_ref[...])
    keys_ref[...] = total
    for c in range(NCOL):
        send_ref[c, :, 0:QW] = qry_ref[c]
        send_ref[c, :, QW : QW + 128] = total[:, 896:1024]
        send_ref[c, :, QW + 128 : QW + 256] = total[:, 768:896]


def own_lanes(ref, offset, rows):
    base = pl.multiple_of(lax.div(offset, 128) * 128, 128)
    off = lax.rem(offset, 128)
    return [lanes_at(ref[y, :, pl.ds(base, 128)], off, 128) for y in range(3)]


def sum1(x):
    return jnp.sum(x, axis=1, keepdims=True)


def frame_cols(rot_ref, tr_ref, at):
    base = pl.multiple_of(lax.div(at, 128) * 128, 128)
    rows = [rot_ref[x, :, pl.ds(base, 128)] for x in range(3)] + [tr_ref[:, pl.ds(base, 128)]]
    block = jnp.concatenate(rows + [jnp.zeros((116, 128), F32)], 0)
    return lanes_at(block, lax.rem(at, 128), 128).T[:8]


def tall(rows):
    x = jnp.concatenate(rows, 0)
    full = -(-x.shape[0] // 128) * 128
    if full > x.shape[0]:
        x = jnp.concatenate([x, jnp.zeros((full - x.shape[0], 128), F32)], 0)
    return jnp.concatenate([x[t : t + 128].T[:8] for t in range(0, full, 128)], 1)


def frame_out(ref, table):
    lane = lax.broadcasted_iota(jnp.int32, (8, 128), 1)
    block = jnp.zeros((8, 128), F32)
    for (x, y), column in table.items():
        block = jnp.where(lane == 4 * x + y, column, block)
    block = jnp.concatenate([block, jnp.zeros((120, 128), F32)], 0).T
    for x in range(3):
        ref[x] = block[4 * x : 4 * x + 4, :8]


def key_kernel(
    keys_ref, kp_ref, vp_ref, qp_ref, rot_ref, tr_ref,
    kgr_ref, vgr_ref, kpg_ref, vpg_ref, kfr_ref, qpo_ref, fr_ref,
):
    flat = keys_ref[...]
    kgr_ref[...] = flat[:, KEY0:VAL0]
    vgr_ref[...] = flat[:, VAL0:KPT0]
    dk = [flat[:, KPT0 + 48 * x : KPT0 + 48 * x + 48] for x in range(3)]
    dv = [flat[:, VPT0 + 96 * x : VPT0 + 96 * x + 96] for x in range(3)]
    offset = row_index() * 8
    local = tall(own_lanes(kp_ref, offset, 48) + own_lanes(vp_ref, offset, 96))
    kp = [local[:, 48 * y : 48 * y + 48] for y in range(3)]
    vp = [local[:, 144 + 96 * y : 240 + 96 * y] for y in range(3)]
    fr = frame_cols(rot_ref, tr_ref, col_index() * JK + offset)
    rot = [[fr[:, 3 * x + y : 3 * x + y + 1] for y in range(3)] for x in range(3)]
    table = {}
    for y in range(3):
        kpg_ref[y] = rot[0][y] * dk[0] + rot[1][y] * dk[1] + rot[2][y] * dk[2]
        vpg_ref[y] = rot[0][y] * dv[0] + rot[1][y] * dv[1] + rot[2][y] * dv[2]
    for x in range(3):
        for y in range(3):
            table[x, y] = sum1(dk[x] * kp[y]) + sum1(dv[x] * vp[y])
        table[x, 3] = sum1(dk[x]) + sum1(dv[x])
    frame_out(kfr_ref, table)
    off = col_index() * 8
    qpo_ref[...] = tall(
        [lanes_at(jnp.concatenate([qp_ref[y], qp_ref[y]], 1), off, 128) for y in range(3)]
    )
    fr_ref[...] = frame_cols(rot_ref, tr_ref, row_index() * IQ + off)


def last_kernel(
    hw_ref, parts_ref, qpo_ref, fr_ref, gpt_ref, qgr_ref, qpg_ref, qfr_ref, wg_ref, hg_ref,
):
    total = jnp.sum(parts_ref[...], axis=0)
    qgr_ref[...] = total[:, QRY0:QPT0]
    dq = [total[:, QPT0 + 48 * x : QPT0 + 48 * x + 48] for x in range(3)]
    opt = [total[:, OPT0 + 96 * x : OPT0 + 96 * x + 96] for x in range(3)]
    fr = fr_ref[...]
    rot = [[fr[:, 3 * x + y : 3 * x + y + 1] for y in range(3)] for x in range(3)]
    at = pl.multiple_of(col_index() * 8, 8)
    gpt = [gpt_ref[y, pl.ds(at, 8), :] for y in range(3)]
    qp = [qpo_ref[:, 48 * y : 48 * y + 48] for y in range(3)]
    gsum = [sum1(g) for g in gpt]
    for y in range(3):
        qpg_ref[y] = rot[0][y] * dq[0] + rot[1][y] * dq[1] + rot[2][y] * dq[2]
    table = {}
    for x in range(3):
        away = opt[x] - fr[:, 9 + x : 10 + x]
        for y in range(3):
            table[x, y] = sum1(dq[x] * qp[y]) + sum1(away * gpt[y])
        back = rot[x][0] * gsum[0] + rot[x][1] * gsum[1] + rot[x][2] * gsum[2]
        table[x, 3] = sum1(dq[x]) - back
    frame_out(qfr_ref, table)
    w0 = total[:, QW : QW + 128]
    extra = total[:, QW + 128 : QW + 256]
    lane4 = lax.broadcasted_iota(jnp.int32, (4, 128), 1)
    wg_ref[0:8] = WL * w0
    wg_ref[8:12] = WL * jnp.where(lane4 < 64, pltpu.roll(extra, 64, 1)[0:4], extra[4:8])
    lane = lax.broadcasted_iota(jnp.int32, (1, 128), 1)
    raw = jnp.zeros((1, 128), F32)
    for h in range(H):
        raw = jnp.where(lane == h, hw_ref[h], raw)
    sig = 1.0 / (1.0 + jnp.exp(-raw))
    sums = pltpu.roll(extra, 128 - 48, 1)[0:1]
    hg_ref[...] = ((-0.5 * WL * WC) * sums * sig)[:, :H]


def fold_kernel(count, *refs):
    ins, outs = refs[:-count], refs[-count:]
    for n, out in enumerate(outs):
        out[...] = sum(r[n] for r in ins[1:]) + ins[0][n]


def fold_call(name, count, shape):
    def call(*parts):
        return pl.pallas_call(
            functools.partial(fold_kernel, count),
            name=name,
            in_specs=[VMEM_SPEC] * len(parts),
            out_specs=[VMEM_SPEC] * count,
            out_shape=[struct(shape)] * count,
            compiler_params=pltpu.CompilerParams(vmem_limit_bytes=LIMIT),
            cost_estimate=cost(1, 1e6),
        )(*parts)

    return call


def onward(block, axis, step):
    return lax.ppermute(block, axis, [(n, (n + step) % 4) for n in range(4)])


def struct(shape, dtype=F32):
    return jax.ShapeDtypeStruct(shape, dtype)


def cost(us, nbytes):
    return pl.CostEstimate(flops=int(us * 4e6), bytes_accessed=int(nbytes), transcendentals=0)


def per_device(
    pair_rep, bias_weight, head_weight, queries, key_vectors, values, query_points, key_points,
    value_points, rotations, translations, residue_count, grad_output, grad_points, grad_pair,
):
    steps = IQ // QB
    pair_spec = pl.BlockSpec((QB, JK, CZ), lambda i: (i, 0, 0))
    gp_spec = pl.BlockSpec((H, QB, CZ), lambda i: (0, i, 0))
    gp_heads = grad_pair.transpose(1, 0, 2)
    bw_heads = bias_weight.T
    gpt_rows = grad_points.transpose(0, 2, 1)
    e, p, st, q, go, qg, kg, vg, gg, pair, keys = pl.pallas_call(
        logits_kernel,
        name="logits",
        in_specs=[SMEM_SPEC] + [HBM_SPEC] * 14,
        out_specs=[VMEM_SPEC] * 11,
        out_shape=[
            struct((H, IQ, JK)), struct((H, IQ, JK)), struct((NCOL, 24, 128)),
            struct((H * C, IQ)), struct((H * C, IQ)),
            struct((3, 48, IQ)), struct((3, 48, JK)), struct((3, 96, JK)), struct((3, 96, IQ)),
            struct((IQ, JK, CZ), BF16), struct((H * C, JK)),
        ],
        scratch_shapes=[
            pltpu.VMEM((2, 32 * IQ, 128), F32), pltpu.VMEM((H * IQ, CZ), F32),
            pltpu.SMEM((H,), F32), pltpu.VMEM((H, IQ, CZ), BF16), pltpu.VMEM((H, CZ), BF16),
            pltpu.VMEM((IQ, H * C), F32), pltpu.VMEM((H * C, JK), F32),
            pltpu.VMEM((3, 48, IQ), F32), pltpu.VMEM((3, 48, JK), F32),
            pltpu.VMEM((3, 96, JK), F32), pltpu.VMEM((3, 3, 2048), F32),
            pltpu.VMEM((3, 2048), F32), pltpu.VMEM((IQ, H * C), F32),
            pltpu.VMEM((3, IQ, 96), F32), pltpu.SemaphoreType.DMA((13,)),
            pltpu.SemaphoreType.DMA((IQ // PB,)),
        ],
        compiler_params=pltpu.CompilerParams(vmem_limit_bytes=LIMIT),
        cost_estimate=cost(5, 6e6),
    )(
        residue_count,
        *(
            pltpu.with_memory_space_constraint(x, pltpu.HBM)
            for x in (
                head_weight, pair_rep, gp_heads, bw_heads, queries.T, key_vectors, values,
                query_points, key_points, value_points, rotations, translations, grad_output.T,
                gpt_rows,
            )
        ),
    )
    everyone = lax.all_to_all(st, COL, 0, 0, tiled=True)
    d, keep, give, qry = pl.pallas_call(
        grads_kernel,
        name="grads",
        in_specs=[SMEM_SPEC] + [VMEM_SPEC] * 12,
        out_specs=[VMEM_SPEC] * 4,
        out_shape=[
            struct((IQ, 32, JK), BF16), struct((4, 4, 8, KW)), struct((4, 4, 8, KW)),
            struct((NCOL, 8, QW)),
        ],
        scratch_shapes=[
            pltpu.VMEM((2, 32 * IQ, 128), F32), pltpu.VMEM((896, JK), F32),
            pltpu.VMEM((QW, IQ), F32), pltpu.VMEM((16, CZ), F32), pltpu.VMEM((8, 128), F32),
        ],
        compiler_params=pltpu.CompilerParams(vmem_limit_bytes=LIMIT),
        cost_estimate=cost(5, 8e6),
    )(head_weight, e, p, st, everyone, q, keys, go, qg, kg, vg, gg, pair)
    swapped = lax.ppermute(give, "row_2", [(0, 1), (1, 0)])
    chip = fold_call("chip", 4, (4, 8, KW))(keep, swapped)
    by_y = [chip[0]] + [onward(chip[n], "row_1", n) for n in range(1, 4)]
    line = fold_call("line", 4, (8, KW))(*by_y)
    parts = [line[0]] + [onward(line[n], "row_0", n) for n in range(1, 4)]
    pair_grad = pl.pallas_call(
        pair_kernel,
        name="pair",
        grid=(steps,),
        in_specs=[pl.BlockSpec((QB, 32, JK), lambda i: (i, 0, 0)), gp_spec, VMEM_SPEC],
        out_specs=pair_spec,
        out_shape=struct((IQ, JK, CZ), BF16),
        scratch_shapes=[pltpu.VMEM((H * QB, CZ), F32)],
        compiler_params=pltpu.CompilerParams(vmem_limit_bytes=LIMIT),
        cost_estimate=cost(6, 6e6),
    )(d, gp_heads, bw_heads)
    keysum, send = pl.pallas_call(
        mid_kernel,
        name="mid",
        in_specs=[VMEM_SPEC] * 5,
        out_specs=[VMEM_SPEC] * 2,
        out_shape=[struct((8, KW)), struct((NCOL, 8, QW + 256))],
        compiler_params=pltpu.CompilerParams(vmem_limit_bytes=LIMIT),
        cost_estimate=cost(1, 1e6),
    )(*parts, qry)
    last = lax.all_to_all(send, COL, 0, 0, tiled=True)
    key_grad, value_grad, key_point_grad, value_point_grad, key_frame_grad, qpo, fr = (
        pl.pallas_call(
            key_kernel,
            name="keyout",
            in_specs=[VMEM_SPEC] * 6,
            out_specs=[VMEM_SPEC] * 7,
            out_shape=[
                struct((8, 192)), struct((8, 192)), struct((3, 8, 48)), struct((3, 8, 96)),
                struct((3, 4, 8)), struct((8, 256)), struct((8, 128)),
            ],
            compiler_params=pltpu.CompilerParams(vmem_limit_bytes=LIMIT),
        cost_estimate=cost(2, 1e6),
        )(keysum, key_points, value_points, query_points, rotations, translations)
    )
    query_grad, query_point_grad, query_frame_grad, weight_grad, head_grad = pl.pallas_call(
        last_kernel,
        name="last",
        in_specs=[SMEM_SPEC] + [VMEM_SPEC] * 4,
        out_specs=[VMEM_SPEC] * 5,
        out_shape=[
            struct((8, 192)), struct((3, 8, 48)), struct((3, 4, 8)), struct((H, CZ)),
            struct((1, H)),
        ],
        compiler_params=pltpu.CompilerParams(vmem_limit_bytes=LIMIT),
        cost_estimate=cost(2, 1e6),
    )(head_weight, last, qpo, fr, gpt_rows)
    return (
        pair_grad, query_grad.T, query_point_grad.transpose(0, 2, 1), query_frame_grad, key_grad.T,
        value_grad.T, key_point_grad.transpose(0, 2, 1), value_point_grad.transpose(0, 2, 1),
        key_frame_grad, weight_grad.T, head_grad.reshape(H),
    )


def solution(mesh):
    finer = Mesh(mesh.devices.reshape(4, 4, 2, 4, 2), ROW_COL)
    in_specs = (
        P(ROW, COL, None), P(), P(), P(None, ROW), P(None, COL), P(None, COL),
        P(None, None, ROW), P(None, None, COL), P(None, None, COL), P(), P(), P(),
        P(None, ROW), P(None, None, ROW), P(ROW, None, None),
    )
    out_specs = (
        P(ROW, COL, None), P(None, ROW_COL), P(None, None, ROW_COL), P(None, None, ROW_COL),
        P(None, COL_ROW), P(None, COL_ROW), P(None, None, COL_ROW), P(None, None, COL_ROW),
        P(None, None, COL_ROW), P(), P(),
    )
    return jax.shard_map(
        per_device, mesh=finer, in_specs=in_specs, out_specs=out_specs, check_vma=False
    )
```

```python
import functools
import math

import jax
import jax.numpy as jnp
from jax import lax
from jax.experimental import pallas as pl
from jax.experimental.pallas import tpu as pltpu
from jax.sharding import Mesh
from jax.sharding import PartitionSpec as P

ROW = ("row_0", "row_1", "row_2")
COL = ("col_0", "col_1")
ROW_COL = ROW + COL
COL_ROW = COL + ROW
CHIPS = ("row_0", "row_1")

H, C, PQ, PV, CZ = 12, 16, 4, 8, 128
IQ, JK = 64, 256
NCOL, NROW, NCHIP = 8, 32, 16
WL = math.sqrt(1.0 / 3.0)
WC = math.sqrt(2.0 / (9.0 * PQ))
WS = 1.0 / math.sqrt(C)
MASKED = -1000000000.0

KEY0, VAL0, KPT0, VPT0, KEND = 0, 192, 384, 528, 816
QRY0, QPT0, OPT0, QEND = 0, 192, 336, 624
KW, QW = 1024, 640
LIMIT = 20 << 20
QB = 16
PB = 16

F32, BF16 = jnp.float32, jnp.bfloat16
VMEM_SPEC = pl.BlockSpec(memory_space=pltpu.VMEM)
SMEM_SPEC = pl.BlockSpec(memory_space=pltpu.SMEM)
TN = (((0,), (0,)), ((), ()))
NT = (((1,), (1,)), ((), ()))
NN = (((1,), (0,)), ((), ()))


def mm(a, b, dims):
    return lax.dot_general(a, b, dims, preferred_element_type=F32)


def split2(x):
    hi = x.astype(BF16)
    return hi, (x - hi.astype(F32)).astype(BF16)


def split3(x):
    hi = x.astype(BF16)
    rest = x - hi.astype(F32)
    mid = rest.astype(BF16)
    return hi, mid, (rest - mid.astype(F32)).astype(BF16)


def row_index():
    return (lax.axis_index("row_0") * 4 + lax.axis_index("row_1")) * 2 + lax.axis_index("row_2")


def col_index():
    return lax.axis_index("col_0") * 2 + lax.axis_index("col_1")


def soft(hw_ref, h, lanes):
    w = jnp.full((1, lanes), hw_ref[h], F32)
    return jnp.maximum(w, 0.0) + jnp.log1p(jnp.exp(-jnp.abs(w)))


def coef_row(hw_ref, h, lanes):
    return (0.5 * WL * WC) * soft(hw_ref, h, lanes)


def rotate(rot, shift, local):
    out = []
    for x in range(3):
        g = rot[x][0] * local[0] + rot[x][1] * local[1] + rot[x][2] * local[2]
        out.append(g if shift is None else g + shift[x])
    return out


def flip(x):
    rows, lanes = x.shape
    full = -(-lanes // 128) * 128
    if full > lanes:
        x = jnp.concatenate([x, jnp.zeros((rows, full - lanes), F32)], 1)
    x = jnp.concatenate([x, jnp.zeros((128 - rows, full), F32)], 0)
    return jnp.concatenate(
        [x[:, t : t + 128].T for t in range(0, full, 128)], 0
    )[:, :rows]


def col_frames(rot_ref, tr_ref):
    start = pl.multiple_of(col_index() * JK, JK)
    rot = [[rot_ref[x, y : y + 1, pl.ds(start, JK)] for y in range(3)] for x in range(3)]
    tr = [tr_ref[x : x + 1, pl.ds(start, JK)] for x in range(3)]
    return rot, tr


def lanes_at(block, offset, count):
    return pltpu.roll(block, lax.rem(128 - offset, 128), block.ndim - 1)[..., :count]


def row_frames(rot_ref, tr_ref, offset, count):
    at = row_index() * IQ + offset
    base = pl.multiple_of(lax.div(at, 128) * 128, 128)
    off = lax.rem(at, 128)
    rot = []
    for x in range(3):
        block = lanes_at(
            jnp.concatenate([rot_ref[x, :, pl.ds(base, 128)], jnp.zeros((5, 128), F32)], 0),
            off,
            count,
        )
        rot.append([block[y : y + 1] for y in range(3)])
    block = lanes_at(
        jnp.concatenate([tr_ref[:, pl.ds(base, 128)], jnp.zeros((5, 128), F32)], 0), off, count
    )
    return rot, [block[x : x + 1] for x in range(3)]


HBM_SPEC = pl.BlockSpec(memory_space=pltpu.HBM)


def logits_kernel(
    rc_ref, hw_hbm, pair_hbm, gp_hbm, bw_hbm, qt_hbm, k_hbm, v_hbm, qp_hbm, kp_hbm, vp_hbm,
    rot_hbm, tr_hbm, got_hbm, gpt_hbm,
    e_ref, p_ref, st_ref, q_ref, go_ref, qg_ref, kg_ref, vg_ref, gg_ref, pair_ref, k_ref, cf_ref, sig_ref,
    bp_ref, gs_ref, hw_ref, gp_ref, bw_ref, qt_ref, v_ref, qp_ref, kp_ref, vp_ref, rot_ref,
    tr_ref, got_ref, gpt_ref, sems, pair_sems,
):
    def pair_copy(b):
        part = pl.ds(b * PB, PB)
        return pltpu.make_async_copy(pair_hbm.at[part], pair_ref.at[part], pair_sems.at[b])

    moves = [
        (gp_hbm, gp_ref), (bw_hbm, bw_ref), (k_hbm, k_ref), (v_hbm, v_ref), (qt_hbm, qt_ref),
        (got_hbm, got_ref), (qp_hbm, qp_ref), (kp_hbm, kp_ref), (vp_hbm, vp_ref),
        (gpt_hbm, gpt_ref), (rot_hbm, rot_ref), (tr_hbm, tr_ref), (hw_hbm, hw_ref),
    ]
    copies = [pltpu.make_async_copy(a, b, sems.at[n]) for n, (a, b) in enumerate(moves)]
    for c in copies[:2]:
        c.start()
    pair_copy(0).start()
    for c in copies[2:]:
        c.start()
    for b in range(1, IQ // PB):
        pair_copy(b).start()
    for c in copies[:2]:
        c.wait()
    wt = jnp.concatenate([bw_ref[...].astype(F32), jnp.zeros((4, CZ), F32)], 0)
    gs_ref[...] = gp_ref[...].astype(F32).reshape(H * IQ, CZ)

    @pl.loop(0, IQ // PB)
    def _(b):
        pair_copy(b).wait()
        for n in range(PB):
            at = b * PB + n
            lhs = jnp.concatenate([wt, gs_ref[pl.ds(at, H, stride=IQ), :]], 0).astype(BF16)
            res = mm(lhs, pair_ref[at], NT)
            for half in range(2):
                bp_ref[half, pl.ds(at, 16 + H, stride=IQ), :] = res[
                    :, half * 128 : half * 128 + 128
                ]

    for c in copies[2:]:
        c.wait()
    crot, ctr = col_frames(rot_ref, tr_ref)
    rrot, rtr = row_frames(rot_ref, tr_ref, 0, IQ)
    kg = rotate(crot, ctr, [kp_ref[y] for y in range(3)])
    vg = rotate(crot, ctr, [vp_ref[y] for y in range(3)])
    qg = rotate(rrot, rtr, [qp_ref[y] for y in range(3)])
    gg = rotate(rrot, None, [flip(gpt_ref[y])[: H * PV] for y in range(3)])
    q_ref[...] = flip(qt_ref[...])[: H * C]
    go_ref[...] = flip(got_ref[...])[: H * C]
    for x in range(3):
        kg_ref[x], vg_ref[x], qg_ref[x], gg_ref[x] = kg[x], vg[x], qg[x], gg[x]
    real = (
        lax.broadcasted_iota(jnp.int32, (IQ, JK), 1) + col_index() * JK < rc_ref[0]
    )
    lane = lax.broadcasted_iota(jnp.int32, (IQ, 128), 1)
    stats = [jnp.zeros((IQ, 128), F32), jnp.zeros((IQ, 128), F32)]
    row4q = lax.broadcasted_iota(jnp.int32, (4, IQ), 0)
    row4k = lax.broadcasted_iota(jnp.int32, (4, JK), 0)
    lane8 = lax.broadcasted_iota(jnp.int32, (8, 128), 1)
    raw = jnp.zeros((8, 128), F32)
    for h in range(H):
        raw = jnp.where(lane8 == h, hw_ref[h], raw)
        cf_ref[h : h + 1] = coef_row(hw_ref, h, 128)
    sig_ref[...] = (-0.5 * WL * WC) / (1.0 + jnp.exp(-raw))
    for h in range(H):
        cf = cf_ref[h : h + 1, :IQ]
        qgh = [qg_ref[x, 4 * h : 4 * h + 4] for x in range(3)]
        kgh = [kg_ref[x, 4 * h : 4 * h + 4] for x in range(3)]
        qn = sum(jnp.sum(t * t, axis=0, keepdims=True) for t in qgh)
        kn = sum(jnp.sum(t * t, axis=0, keepdims=True) for t in kgh)
        qtail = jnp.where(row4q == 0, -cf, jnp.where(row4q == 1, -cf * qn, 0.0))
        ktail = jnp.where(row4k == 0, kn, jnp.where(row4k == 1, 1.0, 0.0))
        qf = jnp.concatenate(
            [q_ref[C * h : C * h + C] * (WL * WS)] + [2.0 * cf * t for t in qgh] + [qtail], 0
        )
        kf = jnp.concatenate([k_ref[C * h : C * h + C]] + kgh + [ktail], 0)
        a1, a2, a3 = split3(qf)
        b1, b2, b3 = split3(kf)
        core = mm(
            jnp.concatenate([a1, a1, a2, a1, a2, a3], 0),
            jnp.concatenate([b1, b2, b1, b3, b2, b1], 0),
            TN,
        )
        gf = jnp.concatenate(
            [go_ref[C * h : C * h + C]] + [gg_ref[x, 8 * h : 8 * h + 8] for x in range(3)]
            + [jnp.zeros((8, IQ), F32)], 0
        )
        vf = jnp.concatenate(
            [v_ref[C * h : C * h + C]] + [vg_ref[x, 8 * h : 8 * h + 8] for x in range(3)]
            + [jnp.zeros((8, JK), F32)], 0
        )
        g1, g2 = split2(gf)
        v1, v2 = split2(vf)
        prod = mm(
            jnp.concatenate([g1, g1, g2], 0), jnp.concatenate([v1, v2, v1], 0), TN
        )

        def planes(base):
            return jnp.concatenate(
                [bp_ref[half, base * IQ : base * IQ + IQ, :] for half in range(2)], 1
            )

        logit = jnp.where(real, core + WL * planes(h), MASKED)
        prod = prod + planes(16 + h)
        peak = jnp.max(logit, axis=1, keepdims=True)
        e = jnp.exp(logit - peak)
        e_ref[h] = e
        p_ref[h] = prod
        total = jnp.sum(e, axis=1, keepdims=True)
        upper = jnp.sum(e * prod, axis=1, keepdims=True)
        g, r = divmod(h, 6)
        acc = jnp.where(lane == r, peak, stats[g])
        acc = jnp.where(lane == 8 + r, total, acc)
        stats[g] = jnp.where(lane == 16 + r, upper, acc)
    packed = jnp.concatenate(stats, 0).T[:24]
    for c in range(NCOL):
        st_ref[c] = packed


def grads_kernel(
    cf_ref, e_ref, p_ref, own_ref, all_ref, q_ref, k_ref, go_ref, qg_ref, kg_ref, vg_ref, gg_ref,
    pair_ref,
    da_ref, keep_ref, give_ref, qry_ref,
    kp_ref, qp_ref, w_ref, hs_ref,
):
    if True:
        peaks = all_ref[:, 0:8]
        top = jnp.max(peaks, axis=0)
        grow = jnp.exp(peaks - top[None])
        total = jnp.sum(all_ref[:, 8:16] * grow, axis=0)
        upper = jnp.sum(all_ref[:, 16:24] * grow, axis=0)
        scale = jnp.exp(own_ref[0, 0:8] - top) / total
        delta = upper / total
        cols = jnp.concatenate([scale, delta, jnp.zeros((112, 128), F32)], 0).T
        w_ref[...] = jnp.zeros_like(w_ref)
        for half in range(2):
            da_ref[half, H * IQ : 16 * IQ, :] = jnp.zeros((4 * IQ, 128), F32)
            da_ref[half, 28 * IQ : 32 * IQ, :] = jnp.zeros((4 * IQ, 128), F32)
        row4q = lax.broadcasted_iota(jnp.int32, (4, IQ), 0)
        row4k = lax.broadcasted_iota(jnp.int32, (4, JK), 0)
        lane = lax.broadcasted_iota(jnp.int32, (8, 128), 1)
        hs = jnp.zeros((8, 128), F32)
        for h in range(H):
            g, r = divmod(h, 6)
            sc = cols[IQ * g : IQ * g + IQ, r : r + 1]
            dl = cols[IQ * g : IQ * g + IQ, 8 + r : 9 + r]
            a = e_ref[h] * sc
            d = a * (p_ref[h] - dl)
            for half in range(2):
                piece = slice(half * 128, half * 128 + 128)
                da_ref[half, h * IQ : h * IQ + IQ, :] = d[:, piece]
                da_ref[half, (16 + h) * IQ : (17 + h) * IQ, :] = a[:, piece]
            d1, d2 = split2(d)
            a1, a2 = split2(a)
            cfq = cf_ref[h : h + 1, :IQ]
            cfk = jnp.concatenate([cf_ref[h : h + 1]] * 2, 1)
            qgh = [qg_ref[x, 4 * h : 4 * h + 4] for x in range(3)]
            kgh = [kg_ref[x, 4 * h : 4 * h + 4] for x in range(3)]
            qf = jnp.concatenate(
                [q_ref[C * h : C * h + C] * (WL * WS)] + qgh + [jnp.where(row4q == 0, 1.0, 0.0)], 0
            )
            kf = jnp.concatenate(
                [k_ref[C * h : C * h + C] * (WL * WS)] + kgh + [jnp.where(row4k == 0, 1.0, 0.0)], 0
            )
            gf = jnp.concatenate(
                [go_ref[C * h : C * h + C]] + [gg_ref[x, 8 * h : 8 * h + 8] for x in range(3)], 0
            )
            vf = jnp.concatenate([vg_ref[x, 8 * h : 8 * h + 8] for x in range(3)], 0)

            def three(left, n, right1, right2, dims):
                hi, lo = split2(left)
                both = mm(jnp.concatenate([hi, lo], 0), right1, dims)
                return both[:n] + both[n:] + mm(hi, right2, dims)

            kside = three(qf, 32, d1, d2, NN)
            vside = three(gf, 40, a1, a2, NN)
            qside = three(kf, 32, d1, d2, NT)
            oside = three(vf, 24, a1, a2, NT)
            csum, rsum = kside[28:29], qside[28:29]
            kp_ref[KEY0 + C * h : KEY0 + C * h + C] = kside[0:16]
            kp_ref[VAL0 + C * h : VAL0 + C * h + C] = vside[0:16]
            qp_ref[QRY0 + C * h : QRY0 + C * h + C] = qside[0:16]
            tk = jnp.zeros((1, JK), F32)
            tq = jnp.zeros((1, IQ), F32)
            for x in range(3):
                kq = kside[16 + 4 * x : 20 + 4 * x]
                qk = qside[16 + 4 * x : 20 + 4 * x]
                kp_ref[KPT0 + 48 * x + 4 * h : KPT0 + 48 * x + 4 * h + 4] = (2.0 * cfk) * (
                    kq - kgh[x] * csum
                )
                qp_ref[QPT0 + 48 * x + 4 * h : QPT0 + 48 * x + 4 * h + 4] = (-2.0 * cfq) * (
                    qgh[x] * rsum - qk
                )
                kp_ref[VPT0 + 96 * x + 8 * h : VPT0 + 96 * x + 8 * h + 8] = vside[
                    16 + 8 * x : 24 + 8 * x
                ]
                qp_ref[OPT0 + 96 * x + 8 * h : OPT0 + 96 * x + 8 * h + 8] = oside[
                    8 * x : 8 * x + 8
                ]
                tk = tk + jnp.sum(kgh[x] * (kgh[x] * csum - 2.0 * kq), axis=0, keepdims=True)
                tq = tq + jnp.sum(qgh[x] * qgh[x], axis=0, keepdims=True)
            part = jnp.sum(tk, axis=1, keepdims=True) + jnp.sum(tq * rsum, axis=1, keepdims=True)
            hs = jnp.where(lane == 48 + h, part, hs)
        hs_ref[...] = hs

    @pl.loop(0, IQ // PB)
    def _(b):
        dlogs = []
        for n in range(PB):
            at = b * PB + n
            dlogs.append(
                jnp.concatenate(
                    [da_ref[half, pl.ds(at, 16, stride=IQ), :] for half in range(2)], 1
                ).astype(BF16)
            )
        w_ref[...] += mm(
            jnp.concatenate(dlogs, 1), pair_ref[pl.ds(b * PB, PB)].reshape(PB * JK, CZ), NN
        )

    if True:
        core = lax.axis_index("row_2")
        w0 = w_ref[0:8]
        w1 = w_ref[8:16]
        lane = lax.broadcasted_iota(jnp.int32, (8, 128), 1)
        sub = lax.broadcasted_iota(jnp.int32, (8, 128), 0)
        fold = jnp.where(sub < 4, pltpu.roll(w1, 64, 1), pltpu.roll(w1, 4, 0))
        extra = jnp.where(lane < 64, hs_ref[...], fold)
        keys = [
            [kp_ref[128 * t : 128 * t + 128, 128 * b : 128 * b + 128].T for t in range(7)]
            for b in range(2)
        ]
        def tile(j, t):
            b, r = divmod(j, 16)
            if t == 7:
                return w0
            piece = keys[b][t][8 * r : 8 * r + 8]
            return jnp.where(lane < 48, piece, extra) if t == 6 else piece

        first = core == 0
        my_z, my_y = lax.axis_index("row_0"), lax.axis_index("row_1")
        for zone in range(NCHIP):
            z, y = divmod(zone, 4)
            dz = lax.rem(z + 4 - my_z, 4)
            dy = lax.rem(y + 4 - my_y, 4)
            for t in range(8):
                even, odd = tile(2 * zone, t), tile(2 * zone + 1, t)
                keep_ref[dy, dz, :, 128 * t : 128 * t + 128] = jnp.where(first, even, odd)
                give_ref[dy, dz, :, 128 * t : 128 * t + 128] = jnp.where(first, odd, even)
        for t in range(5):
            block = qp_ref[128 * t : 128 * t + 128]
            turned = jnp.concatenate([block, jnp.zeros((128, 64), F32)], 1).T
            for c in range(NCOL):
                qry_ref[c, :, 128 * t : 128 * t + 128] = turned[8 * c : 8 * c + 8]


def pair_kernel(da_ref, gp_ref, bw_ref, out_ref, gs_ref):
    wide = jnp.concatenate([bw_ref[...].astype(F32) * WL, jnp.zeros((4, CZ), F32)], 0)
    hi, lo = split2(wide)
    gs_ref[...] = gp_ref[...].astype(F32).reshape(H * QB, CZ)
    pad = jnp.zeros((4, CZ), F32)
    for n in range(QB):
        at = pl.program_id(0) * QB + n
        rows = jnp.concatenate(
            [da_ref[half, pl.ds(at, 32, stride=IQ), :] for half in range(2)], 1
        ).astype(BF16)
        lhs = jnp.concatenate([rows[:16], rows], 0)
        part = jnp.concatenate([gs_ref[pl.ds(n, H, stride=QB), :], pad], 0).astype(BF16)
        rhs = jnp.concatenate([hi, lo, part], 0)
        out_ref[n] = mm(lhs, rhs, TN).astype(BF16)


def mid_kernel(a_ref, b_ref, c_ref, d_ref, qry_ref, keys_ref, send_ref):
    total = (a_ref[...] + b_ref[...]) + (c_ref[...] + d_ref[...])
    keys_ref[...] = total
    for c in range(NCOL):
        send_ref[c, :, 0:QW] = qry_ref[c]
        send_ref[c, :, QW : QW + 128] = total[:, 896:1024]
        send_ref[c, :, QW + 128 : QW + 256] = total[:, 768:896]


def own_lanes(ref, offset, rows):
    base = pl.multiple_of(lax.div(offset, 128) * 128, 128)
    off = lax.rem(offset, 128)
    return [lanes_at(ref[y, :, pl.ds(base, 128)], off, 128) for y in range(3)]


def sum1(x):
    return jnp.sum(x, axis=1, keepdims=True)


def frame_cols(rot_ref, tr_ref, at):
    base = pl.multiple_of(lax.div(at, 128) * 128, 128)
    rows = [rot_ref[x, :, pl.ds(base, 128)] for x in range(3)] + [tr_ref[:, pl.ds(base, 128)]]
    block = jnp.concatenate(rows + [jnp.zeros((116, 128), F32)], 0)
    return lanes_at(block, lax.rem(at, 128), 128).T[:8]


def tall(rows):
    x = jnp.concatenate(rows, 0)
    full = -(-x.shape[0] // 128) * 128
    if full > x.shape[0]:
        x = jnp.concatenate([x, jnp.zeros((full - x.shape[0], 128), F32)], 0)
    return jnp.concatenate([x[t : t + 128].T[:8] for t in range(0, full, 128)], 1)


def frame_out(ref, table):
    lane = lax.broadcasted_iota(jnp.int32, (8, 128), 1)
    block = jnp.zeros((8, 128), F32)
    for (x, y), column in table.items():
        block = jnp.where(lane == 4 * x + y, column, block)
    block = jnp.concatenate([block, jnp.zeros((120, 128), F32)], 0).T
    for x in range(3):
        ref[x] = block[4 * x : 4 * x + 4, :8]


def key_kernel(
    keys_ref, kp_ref, vp_ref, qp_ref, rot_ref, tr_ref,
    kgr_ref, vgr_ref, kpg_ref, vpg_ref, kfr_ref, qpo_ref, fr_ref,
):
    flat = keys_ref[...]
    kgr_ref[...] = flat[:, KEY0:VAL0]
    vgr_ref[...] = flat[:, VAL0:KPT0]
    dk = [flat[:, KPT0 + 48 * x : KPT0 + 48 * x + 48] for x in range(3)]
    dv = [flat[:, VPT0 + 96 * x : VPT0 + 96 * x + 96] for x in range(3)]
    offset = row_index() * 8
    local = tall(own_lanes(kp_ref, offset, 48) + own_lanes(vp_ref, offset, 96))
    kp = [local[:, 48 * y : 48 * y + 48] for y in range(3)]
    vp = [local[:, 144 + 96 * y : 240 + 96 * y] for y in range(3)]
    fr = frame_cols(rot_ref, tr_ref, col_index() * JK + offset)
    rot = [[fr[:, 3 * x + y : 3 * x + y + 1] for y in range(3)] for x in range(3)]
    table = {}
    for y in range(3):
        kpg_ref[y] = rot[0][y] * dk[0] + rot[1][y] * dk[1] + rot[2][y] * dk[2]
        vpg_ref[y] = rot[0][y] * dv[0] + rot[1][y] * dv[1] + rot[2][y] * dv[2]
    for x in range(3):
        for y in range(3):
            table[x, y] = sum1(dk[x] * kp[y]) + sum1(dv[x] * vp[y])
        table[x, 3] = sum1(dk[x]) + sum1(dv[x])
    frame_out(kfr_ref, table)
    off = col_index() * 8
    qpo_ref[...] = tall(
        [lanes_at(jnp.concatenate([qp_ref[y], qp_ref[y]], 1), off, 128) for y in range(3)]
    )
    fr_ref[...] = frame_cols(rot_ref, tr_ref, row_index() * IQ + off)


def last_kernel(
    sig_ref, parts_ref, qpo_ref, fr_ref, gpt_ref, qgr_ref, qpg_ref, qfr_ref, wg_ref, hg_ref,
):
    total = jnp.sum(parts_ref[...], axis=0)
    qgr_ref[...] = total[:, QRY0:QPT0]
    dq = [total[:, QPT0 + 48 * x : QPT0 + 48 * x + 48] for x in range(3)]
    opt = [total[:, OPT0 + 96 * x : OPT0 + 96 * x + 96] for x in range(3)]
    fr = fr_ref[...]
    rot = [[fr[:, 3 * x + y : 3 * x + y + 1] for y in range(3)] for x in range(3)]
    at = pl.multiple_of(col_index() * 8, 8)
    gpt = [gpt_ref[y, pl.ds(at, 8), :] for y in range(3)]
    qp = [qpo_ref[:, 48 * y : 48 * y + 48] for y in range(3)]
    gsum = [sum1(g) for g in gpt]
    for y in range(3):
        qpg_ref[y] = rot[0][y] * dq[0] + rot[1][y] * dq[1] + rot[2][y] * dq[2]
    table = {}
    for x in range(3):
        away = opt[x] - fr[:, 9 + x : 10 + x]
        for y in range(3):
            table[x, y] = sum1(dq[x] * qp[y]) + sum1(away * gpt[y])
        back = rot[x][0] * gsum[0] + rot[x][1] * gsum[1] + rot[x][2] * gsum[2]
        table[x, 3] = sum1(dq[x]) - back
    frame_out(qfr_ref, table)
    w0 = total[:, QW : QW + 128]
    extra = total[:, QW + 128 : QW + 256]
    lane4 = lax.broadcasted_iota(jnp.int32, (4, 128), 1)
    wg_ref[0:8] = WL * w0
    wg_ref[8:12] = WL * jnp.where(lane4 < 64, pltpu.roll(extra, 64, 1)[0:4], extra[4:8])
    sums = pltpu.roll(extra, 128 - 48, 1)[0:1]
    hg_ref[...] = (sums * sig_ref[0:1])[:, :H]


def fold_kernel(count, *refs):
    ins, outs = refs[:-count], refs[-count:]
    for n, out in enumerate(outs):
        out[...] = sum(r[n] for r in ins[1:]) + ins[0][n]


def fold_call(name, count, shape):
    def call(*parts):
        return pl.pallas_call(
            functools.partial(fold_kernel, count),
            name=name,
            in_specs=[VMEM_SPEC] * len(parts),
            out_specs=[VMEM_SPEC] * count,
            out_shape=[struct(shape)] * count,
            compiler_params=pltpu.CompilerParams(vmem_limit_bytes=LIMIT),
            cost_estimate=cost(1, 1e6),
        )(*parts)

    return call


def onward(block, axis, step):
    return lax.ppermute(block, axis, [(n, (n + step) % 4) for n in range(4)])


def struct(shape, dtype=F32):
    return jax.ShapeDtypeStruct(shape, dtype)


def cost(us, nbytes):
    return pl.CostEstimate(flops=int(us * 4e6), bytes_accessed=int(nbytes), transcendentals=0)


def per_device(
    pair_rep, bias_weight, head_weight, queries, key_vectors, values, query_points, key_points,
    value_points, rotations, translations, residue_count, grad_output, grad_points, grad_pair,
):
    steps = IQ // QB
    pair_spec = pl.BlockSpec((QB, JK, CZ), lambda i: (i, 0, 0))
    gp_spec = pl.BlockSpec((H, QB, CZ), lambda i: (0, i, 0))
    gp_heads = grad_pair.transpose(1, 0, 2)
    bw_heads = bias_weight.T
    gpt_rows = grad_points.transpose(0, 2, 1)
    e, p, st, q, go, qg, kg, vg, gg, pair, keys, coef, sig = pl.pallas_call(
        logits_kernel,
        name="logits",
        in_specs=[SMEM_SPEC] + [HBM_SPEC] * 14,
        out_specs=[VMEM_SPEC] * 13,
        out_shape=[
            struct((H, IQ, JK)), struct((H, IQ, JK)), struct((NCOL, 24, 128)),
            struct((H * C, IQ)), struct((H * C, IQ)),
            struct((3, 48, IQ)), struct((3, 48, JK)), struct((3, 96, JK)), struct((3, 96, IQ)),
            struct((IQ, JK, CZ), BF16), struct((H * C, JK)), struct((16, 128)), struct((8, 128)),
        ],
        scratch_shapes=[
            pltpu.VMEM((2, 32 * IQ, 128), F32), pltpu.VMEM((H * IQ, CZ), F32),
            pltpu.SMEM((H,), F32), pltpu.VMEM((H, IQ, CZ), BF16), pltpu.VMEM((H, CZ), BF16),
            pltpu.VMEM((IQ, H * C), F32), pltpu.VMEM((H * C, JK), F32),
            pltpu.VMEM((3, 48, IQ), F32), pltpu.VMEM((3, 48, JK), F32),
            pltpu.VMEM((3, 96, JK), F32), pltpu.VMEM((3, 3, 2048), F32),
            pltpu.VMEM((3, 2048), F32), pltpu.VMEM((IQ, H * C), F32),
            pltpu.VMEM((3, IQ, 96), F32), pltpu.SemaphoreType.DMA((13,)),
            pltpu.SemaphoreType.DMA((IQ // PB,)),
        ],
        compiler_params=pltpu.CompilerParams(vmem_limit_bytes=LIMIT),
        cost_estimate=cost(5, 6e6),
    )(
        residue_count,
        *(
            pltpu.with_memory_space_constraint(x, pltpu.HBM)
            for x in (
                head_weight, pair_rep, gp_heads, bw_heads, queries.T, key_vectors, values,
                query_points, key_points, value_points, rotations, translations, grad_output.T,
                gpt_rows,
            )
        ),
    )
    everyone = lax.all_to_all(st, COL, 0, 0, tiled=True)
    d, keep, give, qry = pl.pallas_call(
        grads_kernel,
        name="grads",
        in_specs=[VMEM_SPEC] * 13,
        out_specs=[VMEM_SPEC] * 4,
        out_shape=[
            struct((2, 32 * IQ, 128)), struct((4, 4, 8, KW)), struct((4, 4, 8, KW)),
            struct((NCOL, 8, QW)),
        ],
        scratch_shapes=[
            pltpu.VMEM((896, JK), F32), pltpu.VMEM((QW, IQ), F32), pltpu.VMEM((16, CZ), F32), pltpu.VMEM((8, 128), F32),
        ],
        compiler_params=pltpu.CompilerParams(vmem_limit_bytes=LIMIT),
        cost_estimate=cost(5, 8e6),
    )(coef, e, p, st, everyone, q, keys, go, qg, kg, vg, gg, pair)
    swapped = lax.ppermute(give, "row_2", [(0, 1), (1, 0)])
    chip = fold_call("chip", 4, (4, 8, KW))(keep, swapped)
    by_y = [chip[0]] + [onward(chip[n], "row_1", n) for n in range(1, 4)]
    line = fold_call("line", 4, (8, KW))(*by_y)
    parts = [line[0]] + [onward(line[n], "row_0", n) for n in range(1, 4)]
    pair_grad = pl.pallas_call(
        pair_kernel,
        name="pair",
        grid=(steps,),
        in_specs=[VMEM_SPEC, gp_spec, VMEM_SPEC],
        out_specs=pair_spec,
        out_shape=struct((IQ, JK, CZ), BF16),
        scratch_shapes=[pltpu.VMEM((H * QB, CZ), F32)],
        compiler_params=pltpu.CompilerParams(vmem_limit_bytes=LIMIT),
        cost_estimate=cost(6, 6e6),
    )(d, gp_heads, bw_heads)
    keysum, send = pl.pallas_call(
        mid_kernel,
        name="mid",
        in_specs=[VMEM_SPEC] * 5,
        out_specs=[VMEM_SPEC] * 2,
        out_shape=[struct((8, KW)), struct((NCOL, 8, QW + 256))],
        compiler_params=pltpu.CompilerParams(vmem_limit_bytes=LIMIT),
        cost_estimate=cost(1, 1e6),
    )(*parts, qry)
    last = lax.all_to_all(send, COL, 0, 0, tiled=True)
    key_grad, value_grad, key_point_grad, value_point_grad, key_frame_grad, qpo, fr = (
        pl.pallas_call(
            key_kernel,
            name="keyout",
            in_specs=[VMEM_SPEC] * 6,
            out_specs=[VMEM_SPEC] * 7,
            out_shape=[
                struct((8, 192)), struct((8, 192)), struct((3, 8, 48)), struct((3, 8, 96)),
                struct((3, 4, 8)), struct((8, 256)), struct((8, 128)),
            ],
            compiler_params=pltpu.CompilerParams(vmem_limit_bytes=LIMIT),
        cost_estimate=cost(2, 1e6),
        )(keysum, key_points, value_points, query_points, rotations, translations)
    )
    query_grad, query_point_grad, query_frame_grad, weight_grad, head_grad = pl.pallas_call(
        last_kernel,
        name="last",
        in_specs=[VMEM_SPEC] * 5,
        out_specs=[VMEM_SPEC] * 5,
        out_shape=[
            struct((8, 192)), struct((3, 8, 48)), struct((3, 4, 8)), struct((H, CZ)),
            struct((1, H)),
        ],
        compiler_params=pltpu.CompilerParams(vmem_limit_bytes=LIMIT),
        cost_estimate=cost(2, 1e6),
    )(sig, last, qpo, fr, gpt_rows)
    return (
        pair_grad, query_grad.T, query_point_grad.transpose(0, 2, 1), query_frame_grad, key_grad.T,
        value_grad.T, key_point_grad.transpose(0, 2, 1), value_point_grad.transpose(0, 2, 1),
        key_frame_grad, weight_grad.T, head_grad.reshape(H),
    )


def solution(mesh):
    finer = Mesh(mesh.devices.reshape(4, 4, 2, 4, 2), ROW_COL)
    in_specs = (
        P(ROW, COL, None), P(), P(), P(None, ROW), P(None, COL), P(None, COL),
        P(None, None, ROW), P(None, None, COL), P(None, None, COL), P(), P(), P(),
        P(None, ROW), P(None, None, ROW), P(ROW, None, None),
    )
    out_specs = (
        P(ROW, COL, None), P(None, ROW_COL), P(None, None, ROW_COL), P(None, None, ROW_COL),
        P(None, COL_ROW), P(None, COL_ROW), P(None, None, COL_ROW), P(None, None, COL_ROW),
        P(None, None, COL_ROW), P(), P(),
    )
    return jax.shard_map(
        per_device, mesh=finer, in_specs=in_specs, out_specs=out_specs, check_vma=False
    )
```

```python
import functools
import math

import jax
import jax.numpy as jnp
from jax import lax
from jax.experimental import pallas as pl
from jax.experimental.pallas import tpu as pltpu
from jax.sharding import Mesh
from jax.sharding import PartitionSpec as P

ROW = ("row_0", "row_1", "row_2")
COL = ("col_0", "col_1")
ROW_COL = ROW + COL
COL_ROW = COL + ROW
CHIPS = ("row_0", "row_1")

H, C, PQ, PV, CZ = 12, 16, 4, 8, 128
IQ, JK = 64, 256
NCOL, NROW, NCHIP = 8, 32, 16
WL = math.sqrt(1.0 / 3.0)
WC = math.sqrt(2.0 / (9.0 * PQ))
WS = 1.0 / math.sqrt(C)
MASKED = -1000000000.0

KEY0, VAL0, KPT0, VPT0, KEND = 0, 192, 384, 528, 816
QRY0, QPT0, OPT0, QEND = 0, 192, 336, 624
KW, QW, LW = 1024, 640, 3712
LIMIT = 20 << 20
QB = 16
PB = 16

F32, BF16 = jnp.float32, jnp.bfloat16
VMEM_SPEC = pl.BlockSpec(memory_space=pltpu.VMEM)
SMEM_SPEC = pl.BlockSpec(memory_space=pltpu.SMEM)
TN = (((0,), (0,)), ((), ()))
NT = (((1,), (1,)), ((), ()))
NN = (((1,), (0,)), ((), ()))


def mm(a, b, dims):
    return lax.dot_general(a, b, dims, preferred_element_type=F32)


def split2(x):
    hi = x.astype(BF16)
    return hi, (x - hi.astype(F32)).astype(BF16)


def split3(x):
    hi = x.astype(BF16)
    rest = x - hi.astype(F32)
    mid = rest.astype(BF16)
    return hi, mid, (rest - mid.astype(F32)).astype(BF16)


def row_index():
    return (lax.axis_index("row_0") * 4 + lax.axis_index("row_1")) * 2 + lax.axis_index("row_2")


def col_index():
    return lax.axis_index("col_0") * 2 + lax.axis_index("col_1")


def soft(hw_ref, h, lanes):
    w = jnp.full((1, lanes), hw_ref[h], F32)
    return jnp.maximum(w, 0.0) + jnp.log1p(jnp.exp(-jnp.abs(w)))


def coef_row(hw_ref, h, lanes):
    return (0.5 * WL * WC) * soft(hw_ref, h, lanes)


def rotate(rot, shift, local):
    out = []
    for x in range(3):
        g = rot[x][0] * local[0] + rot[x][1] * local[1] + rot[x][2] * local[2]
        out.append(g if shift is None else g + shift[x])
    return out


def flip(x):
    rows, lanes = x.shape
    full = -(-lanes // 128) * 128
    if full > lanes:
        x = jnp.concatenate([x, jnp.zeros((rows, full - lanes), F32)], 1)
    x = jnp.concatenate([x, jnp.zeros((128 - rows, full), F32)], 0)
    return jnp.concatenate(
        [x[:, t : t + 128].T for t in range(0, full, 128)], 0
    )[:, :rows]


def col_frames(rot_ref, tr_ref):
    start = pl.multiple_of(col_index() * JK, JK)
    rot = [[rot_ref[x, y : y + 1, pl.ds(start, JK)] for y in range(3)] for x in range(3)]
    tr = [tr_ref[x : x + 1, pl.ds(start, JK)] for x in range(3)]
    return rot, tr


def lanes_at(block, offset, count):
    return pltpu.roll(block, lax.rem(128 - offset, 128), block.ndim - 1)[..., :count]


def row_frames(rot_ref, tr_ref, offset, count):
    at = row_index() * IQ + offset
    base = pl.multiple_of(lax.div(at, 128) * 128, 128)
    off = lax.rem(at, 128)
    rot = []
    for x in range(3):
        block = lanes_at(
            jnp.concatenate([rot_ref[x, :, pl.ds(base, 128)], jnp.zeros((5, 128), F32)], 0),
            off,
            count,
        )
        rot.append([block[y : y + 1] for y in range(3)])
    block = lanes_at(
        jnp.concatenate([tr_ref[:, pl.ds(base, 128)], jnp.zeros((5, 128), F32)], 0), off, count
    )
    return rot, [block[x : x + 1] for x in range(3)]


HBM_SPEC = pl.BlockSpec(memory_space=pltpu.HBM)


def logits_kernel(
    rc_ref, hw_hbm, pair_hbm, gp_hbm, bw_hbm, qt_hbm, k_hbm, v_hbm, qp_hbm, kp_hbm, vp_hbm,
    rot_hbm, tr_hbm, got_hbm, gpt_hbm,
    e_ref, p_ref, st_ref, q_ref, go_ref, qg_ref, kg_ref, vg_ref, gg_ref, pair_ref, k_ref, cf_ref, sig_ref,
    bp_ref, gs_ref, hw_ref, gp_ref, bw_ref, qt_ref, v_ref, qp_ref, kp_ref, vp_ref, rot_ref,
    tr_ref, got_ref, gpt_ref, sems, pair_sems,
):
    def pair_copy(b):
        part = pl.ds(b * PB, PB)
        return pltpu.make_async_copy(pair_hbm.at[part], pair_ref.at[part], pair_sems.at[b])

    moves = [
        (gp_hbm, gp_ref), (bw_hbm, bw_ref), (k_hbm, k_ref), (v_hbm, v_ref), (qt_hbm, qt_ref),
        (got_hbm, got_ref), (qp_hbm, qp_ref), (kp_hbm, kp_ref), (vp_hbm, vp_ref),
        (gpt_hbm, gpt_ref), (rot_hbm, rot_ref), (tr_hbm, tr_ref), (hw_hbm, hw_ref),
    ]
    copies = [pltpu.make_async_copy(a, b, sems.at[n]) for n, (a, b) in enumerate(moves)]
    for c in copies[:2]:
        c.start()
    pair_copy(0).start()
    for c in copies[2:]:
        c.start()
    for b in range(1, IQ // PB):
        pair_copy(b).start()
    for c in copies[:2]:
        c.wait()
    wt = jnp.concatenate([bw_ref[...].astype(F32), jnp.zeros((4, CZ), F32)], 0)
    gs_ref[...] = gp_ref[...].astype(F32).reshape(H * IQ, CZ)

    for b in range(IQ // PB):
        pair_copy(b).wait()
        for n in range(PB):
            at = b * PB + n
            lhs = jnp.concatenate([wt, gs_ref[pl.ds(at, H, stride=IQ), :]], 0).astype(BF16)
            res = mm(lhs, pair_ref[at], NT)
            for half in range(2):
                bp_ref[half, pl.ds(at, 16 + H, stride=IQ), :] = res[
                    :, half * 128 : half * 128 + 128
                ]

    for c in copies[2:]:
        c.wait()
    crot, ctr = col_frames(rot_ref, tr_ref)
    rrot, rtr = row_frames(rot_ref, tr_ref, 0, IQ)
    kg = rotate(crot, ctr, [kp_ref[y] for y in range(3)])
    vg = rotate(crot, ctr, [vp_ref[y] for y in range(3)])
    qg = rotate(rrot, rtr, [qp_ref[y] for y in range(3)])
    gg = rotate(rrot, None, [flip(gpt_ref[y])[: H * PV] for y in range(3)])
    q_ref[...] = flip(qt_ref[...])[: H * C]
    go_ref[...] = flip(got_ref[...])[: H * C]
    for x in range(3):
        kg_ref[x], vg_ref[x], qg_ref[x], gg_ref[x] = kg[x], vg[x], qg[x], gg[x]
    real = (
        lax.broadcasted_iota(jnp.int32, (IQ, JK), 1) + col_index() * JK < rc_ref[0]
    )
    lane = lax.broadcasted_iota(jnp.int32, (IQ, 128), 1)
    stats = [jnp.zeros((IQ, 128), F32), jnp.zeros((IQ, 128), F32)]
    row4q = lax.broadcasted_iota(jnp.int32, (4, IQ), 0)
    row4k = lax.broadcasted_iota(jnp.int32, (4, JK), 0)
    lane8 = lax.broadcasted_iota(jnp.int32, (8, 128), 1)
    raw = jnp.zeros((8, 128), F32)
    for h in range(H):
        raw = jnp.where(lane8 == h, hw_ref[h], raw)
        cf_ref[h : h + 1] = coef_row(hw_ref, h, 128)
    sig_ref[...] = (-0.5 * WL * WC) / (1.0 + jnp.exp(-raw))
    for h in range(H):
        cf = cf_ref[h : h + 1, :IQ]
        qgh = [qg_ref[x, 4 * h : 4 * h + 4] for x in range(3)]
        kgh = [kg_ref[x, 4 * h : 4 * h + 4] for x in range(3)]
        qn = sum(jnp.sum(t * t, axis=0, keepdims=True) for t in qgh)
        kn = sum(jnp.sum(t * t, axis=0, keepdims=True) for t in kgh)
        qtail = jnp.where(row4q == 0, -cf, jnp.where(row4q == 1, -cf * qn, 0.0))
        ktail = jnp.where(row4k == 0, kn, jnp.where(row4k == 1, 1.0, 0.0))
        qf = jnp.concatenate(
            [q_ref[C * h : C * h + C] * (WL * WS)] + [2.0 * cf * t for t in qgh] + [qtail], 0
        )
        kf = jnp.concatenate([k_ref[C * h : C * h + C]] + kgh + [ktail], 0)
        a1, a2, a3 = split3(qf)
        b1, b2, b3 = split3(kf)
        core = mm(
            jnp.concatenate([a1, a1, a2, a1, a2, a3], 0),
            jnp.concatenate([b1, b2, b1, b3, b2, b1], 0),
            TN,
        )
        gf = jnp.concatenate(
            [go_ref[C * h : C * h + C]] + [gg_ref[x, 8 * h : 8 * h + 8] for x in range(3)]
            + [jnp.zeros((8, IQ), F32)], 0
        )
        vf = jnp.concatenate(
            [v_ref[C * h : C * h + C]] + [vg_ref[x, 8 * h : 8 * h + 8] for x in range(3)]
            + [jnp.zeros((8, JK), F32)], 0
        )
        g1, g2 = split2(gf)
        v1, v2 = split2(vf)
        prod = mm(
            jnp.concatenate([g1, g1, g2], 0), jnp.concatenate([v1, v2, v1], 0), TN
        )

        def planes(base):
            return jnp.concatenate(
                [bp_ref[half, base * IQ : base * IQ + IQ, :] for half in range(2)], 1
            )

        logit = jnp.where(real, core + WL * planes(h), MASKED)
        prod = prod + planes(16 + h)
        peak = jnp.max(logit, axis=1, keepdims=True)
        e = jnp.exp(logit - peak)
        e_ref[h] = e
        p_ref[h] = prod
        total = jnp.sum(e, axis=1, keepdims=True)
        upper = jnp.sum(e * prod, axis=1, keepdims=True)
        g, r = divmod(h, 6)
        acc = jnp.where(lane == r, peak, stats[g])
        acc = jnp.where(lane == 8 + r, total, acc)
        stats[g] = jnp.where(lane == 16 + r, upper, acc)
    packed = jnp.concatenate(stats, 0).T[:24]
    for c in range(NCOL):
        st_ref[c] = packed


def grads_kernel(
    cf_ref, e_ref, p_ref, own_ref, all_ref, q_ref, k_ref, go_ref, qg_ref, kg_ref, vg_ref, gg_ref,
    pair_ref,
    da_ref, keep_ref, give_ref, qry_ref,
    kp_ref, qp_ref, w_ref, hs_ref,
):
    if True:
        peaks = all_ref[:, 0:8]
        top = jnp.max(peaks, axis=0)
        grow = jnp.exp(peaks - top[None])
        total = jnp.sum(all_ref[:, 8:16] * grow, axis=0)
        upper = jnp.sum(all_ref[:, 16:24] * grow, axis=0)
        scale = jnp.exp(own_ref[0, 0:8] - top) / total
        delta = upper / total
        cols = jnp.concatenate([scale, delta, jnp.zeros((112, 128), F32)], 0).T
        w_ref[...] = jnp.zeros_like(w_ref)
        for half in range(2):
            da_ref[half, H * IQ : 16 * IQ, :] = jnp.zeros((4 * IQ, 128), F32)
            da_ref[half, 28 * IQ : 32 * IQ, :] = jnp.zeros((4 * IQ, 128), F32)
        row4q = lax.broadcasted_iota(jnp.int32, (4, IQ), 0)
        row4k = lax.broadcasted_iota(jnp.int32, (4, JK), 0)
        lane = lax.broadcasted_iota(jnp.int32, (8, 128), 1)
        hs = jnp.zeros((8, 128), F32)
        for h in range(H):
            g, r = divmod(h, 6)
            sc = cols[IQ * g : IQ * g + IQ, r : r + 1]
            dl = cols[IQ * g : IQ * g + IQ, 8 + r : 9 + r]
            a = e_ref[h] * sc
            d = a * (p_ref[h] - dl)
            for half in range(2):
                piece = slice(half * 128, half * 128 + 128)
                da_ref[half, h * IQ : h * IQ + IQ, :] = d[:, piece]
                da_ref[half, (16 + h) * IQ : (17 + h) * IQ, :] = a[:, piece]
            d1, d2 = split2(d)
            a1, a2 = split2(a)
            cfq = cf_ref[h : h + 1, :IQ]
            cfk = jnp.concatenate([cf_ref[h : h + 1]] * 2, 1)
            qgh = [qg_ref[x, 4 * h : 4 * h + 4] for x in range(3)]
            kgh = [kg_ref[x, 4 * h : 4 * h + 4] for x in range(3)]
            qf = jnp.concatenate(
                [q_ref[C * h : C * h + C] * (WL * WS)] + qgh + [jnp.where(row4q == 0, 1.0, 0.0)], 0
            )
            kf = jnp.concatenate(
                [k_ref[C * h : C * h + C] * (WL * WS)] + kgh + [jnp.where(row4k == 0, 1.0, 0.0)], 0
            )
            gf = jnp.concatenate(
                [go_ref[C * h : C * h + C]] + [gg_ref[x, 8 * h : 8 * h + 8] for x in range(3)], 0
            )
            vf = jnp.concatenate([vg_ref[x, 8 * h : 8 * h + 8] for x in range(3)], 0)

            def three(left, n, right1, right2, dims):
                hi, lo = split2(left)
                both = mm(jnp.concatenate([hi, lo], 0), right1, dims)
                return both[:n] + both[n:] + mm(hi, right2, dims)

            kside = three(qf, 32, d1, d2, NN)
            vside = three(gf, 40, a1, a2, NN)
            qside = three(kf, 32, d1, d2, NT)
            oside = three(vf, 24, a1, a2, NT)
            csum, rsum = kside[28:29], qside[28:29]
            kp_ref[KEY0 + C * h : KEY0 + C * h + C] = kside[0:16]
            kp_ref[VAL0 + C * h : VAL0 + C * h + C] = vside[0:16]
            qp_ref[QRY0 + C * h : QRY0 + C * h + C] = qside[0:16]
            tk = jnp.zeros((1, JK), F32)
            tq = jnp.zeros((1, IQ), F32)
            for x in range(3):
                kq = kside[16 + 4 * x : 20 + 4 * x]
                qk = qside[16 + 4 * x : 20 + 4 * x]
                kp_ref[KPT0 + 48 * x + 4 * h : KPT0 + 48 * x + 4 * h + 4] = (2.0 * cfk) * (
                    kq - kgh[x] * csum
                )
                qp_ref[QPT0 + 48 * x + 4 * h : QPT0 + 48 * x + 4 * h + 4] = (-2.0 * cfq) * (
                    qgh[x] * rsum - qk
                )
                kp_ref[VPT0 + 96 * x + 8 * h : VPT0 + 96 * x + 8 * h + 8] = vside[
                    16 + 8 * x : 24 + 8 * x
                ]
                qp_ref[OPT0 + 96 * x + 8 * h : OPT0 + 96 * x + 8 * h + 8] = oside[
                    8 * x : 8 * x + 8
                ]
                tk = tk + jnp.sum(kgh[x] * (kgh[x] * csum - 2.0 * kq), axis=0, keepdims=True)
                tq = tq + jnp.sum(qgh[x] * qgh[x], axis=0, keepdims=True)
            part = jnp.sum(tk, axis=1, keepdims=True) + jnp.sum(tq * rsum, axis=1, keepdims=True)
            hs = jnp.where(lane == 48 + h, part, hs)
        hs_ref[...] = hs

    for b in range(IQ // PB):
        dlogs = []
        for n in range(PB):
            at = b * PB + n
            dlogs.append(
                jnp.concatenate(
                    [da_ref[half, pl.ds(at, 16, stride=IQ), :] for half in range(2)], 1
                ).astype(BF16)
            )
        w_ref[...] += mm(
            jnp.concatenate(dlogs, 1), pair_ref[pl.ds(b * PB, PB)].reshape(PB * JK, CZ), NN
        )

    if True:
        core = lax.axis_index("row_2")
        w0 = w_ref[0:8]
        w1 = w_ref[8:16]
        lane = lax.broadcasted_iota(jnp.int32, (8, 128), 1)
        sub = lax.broadcasted_iota(jnp.int32, (8, 128), 0)
        fold = jnp.where(sub < 4, pltpu.roll(w1, 64, 1), pltpu.roll(w1, 4, 0))
        extra = jnp.where(lane < 64, hs_ref[...], fold)
        keys = [
            [kp_ref[128 * t : 128 * t + 128, 128 * b : 128 * b + 128].T for t in range(7)]
            for b in range(2)
        ]
        def tile(j, t):
            b, r = divmod(j, 16)
            piece = keys[b][t][8 * r : 8 * r + 8]
            return jnp.where(lane < 48, piece, extra) if t == 6 else piece

        first = core == 0
        my_z, my_y = lax.axis_index("row_0"), lax.axis_index("row_1")
        for zone in range(NCHIP):
            z, y = divmod(zone, 4)
            dz = lax.rem(z + 4 - my_z, 4)
            dy = lax.rem(y + 4 - my_y, 4)
            for t in range(7):
                even, odd = tile(2 * zone, t), tile(2 * zone + 1, t)
                spot = pl.ds(pl.multiple_of(dz * 896 + 128 * t, 128), 128)
                keep_ref[dy, :, spot] = jnp.where(first, even, odd)
                give_ref[dy, :, spot] = jnp.where(first, odd, even)
        for n in range(4):
            keep_ref[n, :, 3584:LW] = w0
            give_ref[n, :, 3584:LW] = w0
        for t in range(5):
            block = qp_ref[128 * t : 128 * t + 128]
            turned = jnp.concatenate([block, jnp.zeros((128, 64), F32)], 1).T
            for c in range(NCOL):
                qry_ref[c, :, 128 * t : 128 * t + 128] = turned[8 * c : 8 * c + 8]


def pair_kernel(da_ref, gp_ref, bw_ref, out_ref, gs_ref):
    wide = jnp.concatenate([bw_ref[...].astype(F32) * WL, jnp.zeros((4, CZ), F32)], 0)
    hi, lo = split2(wide)
    gs_ref[...] = gp_ref[...].astype(F32).reshape(H * QB, CZ)
    pad = jnp.zeros((4, CZ), F32)
    for n in range(QB):
        at = pl.program_id(0) * QB + n
        rows = jnp.concatenate(
            [da_ref[half, pl.ds(at, 32, stride=IQ), :] for half in range(2)], 1
        ).astype(BF16)
        lhs = jnp.concatenate([rows[:16], rows], 0)
        part = jnp.concatenate([gs_ref[pl.ds(n, H, stride=QB), :], pad], 0).astype(BF16)
        rhs = jnp.concatenate([hi, lo, part], 0)
        out_ref[n] = mm(lhs, rhs, TN).astype(BF16)


def mid_kernel(a_ref, b_ref, c_ref, d_ref, qry_ref, keys_ref, send_ref):
    total = (a_ref[...] + b_ref[...]) + (c_ref[...] + d_ref[...])
    keys_ref[...] = total
    for c in range(NCOL):
        send_ref[c, :, 0:QW] = qry_ref[c]
        send_ref[c, :, QW : QW + 128] = total[:, 896:1024]
        send_ref[c, :, QW + 128 : QW + 256] = total[:, 768:896]


def own_lanes(ref, offset, rows):
    base = pl.multiple_of(lax.div(offset, 128) * 128, 128)
    off = lax.rem(offset, 128)
    return [lanes_at(ref[y, :, pl.ds(base, 128)], off, 128) for y in range(3)]


def sum1(x):
    return jnp.sum(x, axis=1, keepdims=True)


def frame_cols(rot_ref, tr_ref, at):
    base = pl.multiple_of(lax.div(at, 128) * 128, 128)
    rows = [rot_ref[x, :, pl.ds(base, 128)] for x in range(3)] + [tr_ref[:, pl.ds(base, 128)]]
    block = jnp.concatenate(rows + [jnp.zeros((116, 128), F32)], 0)
    return lanes_at(block, lax.rem(at, 128), 128).T[:8]


def tall(rows):
    x = jnp.concatenate(rows, 0)
    full = -(-x.shape[0] // 128) * 128
    if full > x.shape[0]:
        x = jnp.concatenate([x, jnp.zeros((full - x.shape[0], 128), F32)], 0)
    return jnp.concatenate([x[t : t + 128].T[:8] for t in range(0, full, 128)], 1)


def frame_out(ref, table):
    lane = lax.broadcasted_iota(jnp.int32, (8, 128), 1)
    block = jnp.zeros((8, 128), F32)
    for (x, y), column in table.items():
        block = jnp.where(lane == 4 * x + y, column, block)
    block = jnp.concatenate([block, jnp.zeros((120, 128), F32)], 0).T
    for x in range(3):
        ref[x] = block[4 * x : 4 * x + 4, :8]


def key_kernel(
    keys_ref, kp_ref, vp_ref, qp_ref, rot_ref, tr_ref,
    kgr_ref, vgr_ref, kpg_ref, vpg_ref, kfr_ref, qpo_ref, fr_ref,
):
    flat = keys_ref[...]
    kgr_ref[...] = flat[:, KEY0:VAL0]
    vgr_ref[...] = flat[:, VAL0:KPT0]
    dk = [flat[:, KPT0 + 48 * x : KPT0 + 48 * x + 48] for x in range(3)]
    dv = [flat[:, VPT0 + 96 * x : VPT0 + 96 * x + 96] for x in range(3)]
    offset = row_index() * 8
    local = tall(own_lanes(kp_ref, offset, 48) + own_lanes(vp_ref, offset, 96))
    kp = [local[:, 48 * y : 48 * y + 48] for y in range(3)]
    vp = [local[:, 144 + 96 * y : 240 + 96 * y] for y in range(3)]
    fr = frame_cols(rot_ref, tr_ref, col_index() * JK + offset)
    rot = [[fr[:, 3 * x + y : 3 * x + y + 1] for y in range(3)] for x in range(3)]
    table = {}
    for y in range(3):
        kpg_ref[y] = rot[0][y] * dk[0] + rot[1][y] * dk[1] + rot[2][y] * dk[2]
        vpg_ref[y] = rot[0][y] * dv[0] + rot[1][y] * dv[1] + rot[2][y] * dv[2]
    for x in range(3):
        for y in range(3):
            table[x, y] = sum1(dk[x] * kp[y]) + sum1(dv[x] * vp[y])
        table[x, 3] = sum1(dk[x]) + sum1(dv[x])
    frame_out(kfr_ref, table)
    off = col_index() * 8
    qpo_ref[...] = tall(
        [lanes_at(jnp.concatenate([qp_ref[y], qp_ref[y]], 1), off, 128) for y in range(3)]
    )
    fr_ref[...] = frame_cols(rot_ref, tr_ref, row_index() * IQ + off)


def last_kernel(
    sig_ref, parts_ref, qpo_ref, fr_ref, gpt_ref, qgr_ref, qpg_ref, qfr_ref, wg_ref, hg_ref,
):
    total = jnp.sum(parts_ref[...], axis=0)
    qgr_ref[...] = total[:, QRY0:QPT0]
    dq = [total[:, QPT0 + 48 * x : QPT0 + 48 * x + 48] for x in range(3)]
    opt = [total[:, OPT0 + 96 * x : OPT0 + 96 * x + 96] for x in range(3)]
    fr = fr_ref[...]
    rot = [[fr[:, 3 * x + y : 3 * x + y + 1] for y in range(3)] for x in range(3)]
    at = pl.multiple_of(col_index() * 8, 8)
    gpt = [gpt_ref[y, pl.ds(at, 8), :] for y in range(3)]
    qp = [qpo_ref[:, 48 * y : 48 * y + 48] for y in range(3)]
    gsum = [sum1(g) for g in gpt]
    for y in range(3):
        qpg_ref[y] = rot[0][y] * dq[0] + rot[1][y] * dq[1] + rot[2][y] * dq[2]
    table = {}
    for x in range(3):
        away = opt[x] - fr[:, 9 + x : 10 + x]
        for y in range(3):
            table[x, y] = sum1(dq[x] * qp[y]) + sum1(away * gpt[y])
        back = rot[x][0] * gsum[0] + rot[x][1] * gsum[1] + rot[x][2] * gsum[2]
        table[x, 3] = sum1(dq[x]) - back
    frame_out(qfr_ref, table)
    w0 = total[:, QW : QW + 128]
    extra = total[:, QW + 128 : QW + 256]
    lane4 = lax.broadcasted_iota(jnp.int32, (4, 128), 1)
    wg_ref[0:8] = WL * w0
    wg_ref[8:12] = WL * jnp.where(lane4 < 64, pltpu.roll(extra, 64, 1)[0:4], extra[4:8])
    sums = pltpu.roll(extra, 128 - 48, 1)[0:1]
    hg_ref[...] = (sums * sig_ref[0:1])[:, :H]


def chip_kernel(keep_ref, got_ref, *outs):
    for n, out in enumerate(outs):
        out[...] = keep_ref[n] + got_ref[n]


def line_kernel(a_ref, b_ref, c_ref, d_ref, *outs):
    total = (a_ref[...] + b_ref[...]) + (c_ref[...] + d_ref[...])
    for n, out in enumerate(outs):
        out[:, 0:896] = total[:, 896 * n : 896 * n + 896]
        out[:, 896:KW] = total[:, 3584:LW]


def fold_call(body, name, shape):
    def call(*parts):
        return pl.pallas_call(
            body,
            name=name,
            in_specs=[VMEM_SPEC] * len(parts),
            out_specs=[VMEM_SPEC] * 4,
            out_shape=[struct(shape)] * 4,
            compiler_params=pltpu.CompilerParams(vmem_limit_bytes=LIMIT),
            cost_estimate=cost(1, 1e6),
        )(*parts)

    return call


def onward(block, axis, step):
    return lax.ppermute(block, axis, [(n, (n + step) % 4) for n in range(4)])


def struct(shape, dtype=F32):
    return jax.ShapeDtypeStruct(shape, dtype)


def cost(us, nbytes):
    return pl.CostEstimate(flops=int(us * 4e6), bytes_accessed=int(nbytes), transcendentals=0)


def per_device(
    pair_rep, bias_weight, head_weight, queries, key_vectors, values, query_points, key_points,
    value_points, rotations, translations, residue_count, grad_output, grad_points, grad_pair,
):
    steps = IQ // QB
    pair_spec = pl.BlockSpec((QB, JK, CZ), lambda i: (i, 0, 0))
    gp_spec = pl.BlockSpec((H, QB, CZ), lambda i: (0, i, 0))
    gp_heads = grad_pair.transpose(1, 0, 2)
    bw_heads = bias_weight.T
    gpt_rows = grad_points.transpose(0, 2, 1)
    e, p, st, q, go, qg, kg, vg, gg, pair, keys, coef, sig = pl.pallas_call(
        logits_kernel,
        name="logits",
        in_specs=[SMEM_SPEC] + [HBM_SPEC] * 14,
        out_specs=[VMEM_SPEC] * 13,
        out_shape=[
            struct((H, IQ, JK)), struct((H, IQ, JK)), struct((NCOL, 24, 128)),
            struct((H * C, IQ)), struct((H * C, IQ)),
            struct((3, 48, IQ)), struct((3, 48, JK)), struct((3, 96, JK)), struct((3, 96, IQ)),
            struct((IQ, JK, CZ), BF16), struct((H * C, JK)), struct((16, 128)), struct((8, 128)),
        ],
        scratch_shapes=[
            pltpu.VMEM((2, 32 * IQ, 128), F32), pltpu.VMEM((H * IQ, CZ), F32),
            pltpu.SMEM((H,), F32), pltpu.VMEM((H, IQ, CZ), BF16), pltpu.VMEM((H, CZ), BF16),
            pltpu.VMEM((IQ, H * C), F32), pltpu.VMEM((H * C, JK), F32),
            pltpu.VMEM((3, 48, IQ), F32), pltpu.VMEM((3, 48, JK), F32),
            pltpu.VMEM((3, 96, JK), F32), pltpu.VMEM((3, 3, 2048), F32),
            pltpu.VMEM((3, 2048), F32), pltpu.VMEM((IQ, H * C), F32),
            pltpu.VMEM((3, IQ, 96), F32), pltpu.SemaphoreType.DMA((13,)),
            pltpu.SemaphoreType.DMA((IQ // PB,)),
        ],
        compiler_params=pltpu.CompilerParams(vmem_limit_bytes=LIMIT),
        cost_estimate=cost(5, 6e6),
    )(
        residue_count,
        *(
            pltpu.with_memory_space_constraint(x, pltpu.HBM)
            for x in (
                head_weight, pair_rep, gp_heads, bw_heads, queries.T, key_vectors, values,
                query_points, key_points, value_points, rotations, translations, grad_output.T,
                gpt_rows,
            )
        ),
    )
    everyone = lax.all_to_all(st, COL, 0, 0, tiled=True)
    d, keep, give, qry = pl.pallas_call(
        grads_kernel,
        name="grads",
        in_specs=[VMEM_SPEC] * 13,
        out_specs=[VMEM_SPEC] * 4,
        out_shape=[
            struct((2, 32 * IQ, 128)), struct((4, 8, LW)), struct((4, 8, LW)),
            struct((NCOL, 8, QW)),
        ],
        scratch_shapes=[
            pltpu.VMEM((896, JK), F32), pltpu.VMEM((QW, IQ), F32), pltpu.VMEM((16, CZ), F32), pltpu.VMEM((8, 128), F32),
        ],
        compiler_params=pltpu.CompilerParams(vmem_limit_bytes=LIMIT),
        cost_estimate=cost(5, 8e6),
    )(coef, e, p, st, everyone, q, keys, go, qg, kg, vg, gg, pair)
    swapped = lax.ppermute(give, "row_2", [(0, 1), (1, 0)])
    chip = fold_call(chip_kernel, "chip", (8, LW))(keep, swapped)
    by_y = [chip[0]] + [onward(chip[n], "row_1", n) for n in range(1, 4)]
    line = fold_call(line_kernel, "line", (8, KW))(*by_y)
    parts = [line[0]] + [onward(line[n], "row_0", n) for n in range(1, 4)]
    pair_grad = pl.pallas_call(
        pair_kernel,
        name="pair",
        grid=(steps,),
        in_specs=[VMEM_SPEC, gp_spec, VMEM_SPEC],
        out_specs=pair_spec,
        out_shape=struct((IQ, JK, CZ), BF16),
        scratch_shapes=[pltpu.VMEM((H * QB, CZ), F32)],
        compiler_params=pltpu.CompilerParams(vmem_limit_bytes=LIMIT),
        cost_estimate=cost(6, 6e6),
    )(d, gp_heads, bw_heads)
    keysum, send = pl.pallas_call(
        mid_kernel,
        name="mid",
        in_specs=[VMEM_SPEC] * 5,
        out_specs=[VMEM_SPEC] * 2,
        out_shape=[struct((8, KW)), struct((NCOL, 8, QW + 256))],
        compiler_params=pltpu.CompilerParams(vmem_limit_bytes=LIMIT),
        cost_estimate=cost(1, 1e6),
    )(*parts, qry)
    last = lax.all_to_all(send, COL, 0, 0, tiled=True)
    key_grad, value_grad, key_point_grad, value_point_grad, key_frame_grad, qpo, fr = (
        pl.pallas_call(
            key_kernel,
            name="keyout",
            in_specs=[VMEM_SPEC] * 6,
            out_specs=[VMEM_SPEC] * 7,
            out_shape=[
                struct((8, 192)), struct((8, 192)), struct((3, 8, 48)), struct((3, 8, 96)),
                struct((3, 4, 8)), struct((8, 256)), struct((8, 128)),
            ],
            compiler_params=pltpu.CompilerParams(vmem_limit_bytes=LIMIT),
        cost_estimate=cost(2, 1e6),
        )(keysum, key_points, value_points, query_points, rotations, translations)
    )
    query_grad, query_point_grad, query_frame_grad, weight_grad, head_grad = pl.pallas_call(
        last_kernel,
        name="last",
        in_specs=[VMEM_SPEC] * 5,
        out_specs=[VMEM_SPEC] * 5,
        out_shape=[
            struct((8, 192)), struct((3, 8, 48)), struct((3, 4, 8)), struct((H, CZ)),
            struct((1, H)),
        ],
        compiler_params=pltpu.CompilerParams(vmem_limit_bytes=LIMIT),
        cost_estimate=cost(2, 1e6),
    )(sig, last, qpo, fr, gpt_rows)
    return (
        pair_grad, query_grad.T, query_point_grad.transpose(0, 2, 1), query_frame_grad, key_grad.T,
        value_grad.T, key_point_grad.transpose(0, 2, 1), value_point_grad.transpose(0, 2, 1),
        key_frame_grad, weight_grad.T, head_grad.reshape(H),
    )


def solution(mesh):
    finer = Mesh(mesh.devices.reshape(4, 4, 2, 4, 2), ROW_COL)
    in_specs = (
        P(ROW, COL, None), P(), P(), P(None, ROW), P(None, COL), P(None, COL),
        P(None, None, ROW), P(None, None, COL), P(None, None, COL), P(), P(), P(),
        P(None, ROW), P(None, None, ROW), P(ROW, None, None),
    )
    out_specs = (
        P(ROW, COL, None), P(None, ROW_COL), P(None, None, ROW_COL), P(None, None, ROW_COL),
        P(None, COL_ROW), P(None, COL_ROW), P(None, None, COL_ROW), P(None, None, COL_ROW),
        P(None, None, COL_ROW), P(), P(),
    )
    return jax.shard_map(
        per_device, mesh=finer, in_specs=in_specs, out_specs=out_specs, check_vma=False
    )
```
